32 devices in a mesh: nest: 2 (over core), row: 4 (over y, x), col: 4 (over z).
Axes of the slice: x: 2, y: 2, z: 4, core: 2. Of those that a mesh axis runs over, the one named last changes fastest.
Arguments:
- strips: float32 [2, 3, 4, 16, 24, 1536], P('nest', None, None, ('row', 'col')), may hold values from -1.5 to 2, as said below
- anchor: int32 [2, 2], replicated, may hold values from 1 to 127
- wet_mask: int32 [2, 512, 512], P('nest', 'row', 'col'), may hold values 0 or 1
- bathy_index: int32 [2, 512, 512], P('nest', 'row', 'col'), may hold values from 0 to 15
- bed_levels: float32 [16], replicated, may hold values from 0 to 1.5
- coarse: float32 [3, 1024, 512], P(None, ('nest', 'row'), 'col'), may hold values from -6 to 6
Outputs:
- fine_fields: float32 [2, 3, 1536, 1536], P('nest', None, 'row', 'col')
- coarse_next: float32 [3, 1024, 512], P(None, ('nest', 'row'), 'col')
The draws below stay inside these ranges and needn't reach their ends.
Inputs may be any that keep to these rules, and one draw needn't show every extreme that they name: `strips`: plane 0 of the second dimension is the water depth, within 0.5 to 2; planes 1 and 2 are momenta within -1.5 to 1.5. anchor[n] holds the row and then the column offset of nest n's first coarse cell within its block of coarse rows.
All inputs are finite; a program needn't handle non-finite values. No bound on the sum of `wet_mask` on one device may be relied on, other than what follows from the above.
Results may differ from the reference program's by a relative error of at most 0.0003.
Values sent between devices are 32-bit elements; how exact they have to be, the bound alone decides.
No kernel may reach another device: no remote copies, remote signals or barrier semaphores. Data moves between devices by JAX's collectives and lax.ppermute only.
A program may use at most 128 MiB of HBM per device.

```python
import jax
import jax.numpy as jnp
from jax import lax

TR = 384
TC = 384
NLEV = 16
STRIPS = 16
BAND = 24
NFR = 1536
NFC = 1536
CR = 128
CC = 128
NCR = 1024
NCC = 512
N_NEST = 2
N_ROW = 4
N_COL = 4


def draw_strips(key, part):
    shape_depth = (N_NEST, 1, N_ROW, STRIPS, BAND, NFC)
    shape_flow = (N_NEST, 2, N_ROW, STRIPS, BAND, NFC)
    key_depth = jax.random.fold_in(key, 11)
    key_flow = jax.random.fold_in(key, 12)
    depth_part = jnp.clip(1.25 + 0.3 * jax.random.normal(key_depth, shape_depth, jnp.float32), 0.5, 2.0)
    flow_part = jnp.clip(0.4 * jax.random.normal(key_flow, shape_flow, jnp.float32), -1.5, 1.5)
    return jnp.concatenate([depth_part, flow_part], axis=1)


def plant(array, own_key, smallest, largest):
    longest = array.shape.index(max(array.shape))
    spots = []
    for shift in (0, 1):
        where = [jax.random.randint(jax.random.fold_in(own_key, axis), (), 0, length) for axis, length in enumerate(array.shape)]
        where[longest] = (where[longest] + shift) % array.shape[longest]
        spots.append(tuple(where))
    return array.at[spots[0]].set(smallest).at[spots[1]].set(largest)


def level_of(own_key, shape, shards, least, top_value):
    gain = 1.0
    for axis_at, parts in shards:
        draws = jax.random.uniform(jax.random.fold_in(jax.random.fold_in(own_key, 6), axis_at), (parts,), jnp.float32, least / len(shards), top_value / len(shards))
        gain = gain * jnp.repeat(jnp.exp(draws), shape[axis_at] // parts).reshape((-1,) + (1,) * (len(shape) - 1 - axis_at))
    return gain


def gaussian(own_key, extent, deviation, bound, cuts=(), held_as=jnp.bfloat16):
    entries = jax.random.normal(own_key, extent, jnp.float32) * deviation
    if len(cuts) > 0:
        entries = level_of(own_key, extent, cuts, -0.22, 0.18) * entries
    return jnp.clip(entries, min=-bound, max=bound).astype(held_as)


def setup_inputs(seed: int = 0) -> dict:
    splits = jax.random.split(jax.random.key(seed), 7)
    strips = draw_strips(jax.random.fold_in(splits[6], 71), 0)
    anchor = plant(jax.random.randint(splits[1], (N_NEST, 2), 1, min(TR, TC) // 3), jax.random.fold_in(splits[1], 1), 1, (min(TR, TC) // 3) - 1).astype(jnp.int32)
    wet_mask = plant((jax.random.randint(splits[2], (N_NEST, NFR // 3, NFC // 3), 0, 5) < 4).astype(jnp.int32), jax.random.fold_in(splits[2], 1), 0, 1)
    bathy_index = plant(jax.random.randint(splits[3], (N_NEST, NFR // 3, NFC // 3), 0, NLEV), jax.random.fold_in(splits[3], 1), 0, NLEV - 1).astype(jnp.int32)
    bed_levels = jnp.clip(jax.random.uniform(splits[4], (NLEV,), jnp.float32, 0.0, 1.5), 0.0, 1.5)
    coarse = gaussian(splits[5], (3, NCR, NCC), 1.0, 6.0, ((1, 8), (2, 4)), jnp.float32)
    return {"strips": strips, "anchor": anchor, "wet_mask": wet_mask, "bathy_index": bathy_index, "bed_levels": bed_levels, "coarse": coarse}


gravity = 1.0
courant = 0.2

def advance(padded, bed_pad, wet_pad):
    depth_now = padded[0]
    flow_u = padded[1]
    flow_v = padded[2]
    depth_safe = jnp.where(wet_pad > 0.5, depth_now, 1.0)
    speed_u = flow_u / depth_safe
    speed_v = flow_v / depth_safe
    celerity = jnp.sqrt(gravity * depth_safe)
    pressure = 0.5 * gravity * depth_safe * depth_safe
    fluxes_x = (flow_u, flow_u * speed_u + pressure, flow_v * speed_u)
    fluxes_y = (flow_v, flow_u * speed_v, flow_v * speed_v + pressure)
    reach_x = jnp.abs(speed_u) + celerity
    reach_y = jnp.abs(speed_v) + celerity
    open_x = wet_pad[1:-1, :-1] * wet_pad[1:-1, 1:]
    open_y = wet_pad[:-1, 1:-1] * wet_pad[1:, 1:-1]
    bound_x = jnp.maximum(reach_x[1:-1, :-1], reach_x[1:-1, 1:])
    bound_y = jnp.maximum(reach_y[:-1, 1:-1], reach_y[1:, 1:-1])
    slope_x = (bed_pad[1:-1, 1:] - bed_pad[1:-1, :-1]) * open_x
    slope_y = (bed_pad[1:, 1:-1] - bed_pad[:-1, 1:-1]) * open_y
    centre = depth_now[1:-1, 1:-1]
    sources = (None, -0.5 * gravity * centre * (slope_x[:, 1:] + slope_x[:, :-1]), -0.5 * gravity * centre * (slope_y[1:] + slope_y[:-1]))
    results = []
    for plane in range(3):
        state = padded[plane]
        flux_col = fluxes_x[plane]
        flux_row = fluxes_y[plane]
        face_x = (0.5 * (flux_col[1:-1, :-1] + flux_col[1:-1, 1:]) - 0.5 * bound_x * (state[1:-1, 1:] - state[1:-1, :-1])) * open_x
        face_y = (0.5 * (flux_row[:-1, 1:-1] + flux_row[1:, 1:-1]) - 0.5 * bound_y * (state[1:, 1:-1] - state[:-1, 1:-1])) * open_y
        value = state[1:-1, 1:-1] - courant * (face_x[:, 1:] - face_x[:, :-1]) - courant * (face_y[1:] - face_y[:-1])
        if plane > 0:
            value = value + courant * sources[plane]
        results.append(value)
    return jnp.stack(results)

def expand(cells):
    return jnp.repeat(jnp.repeat(cells, 3, axis=-2), 3, axis=-1)

def lookup(classes, levels):
    ladder = jnp.arange(levels.shape[0], dtype=jnp.int32)
    matches = classes[None] == ladder[:, None, None]
    return lax.optimization_barrier(jnp.sum(jnp.where(matches, levels[:, None, None], 0.0), axis=0))

def restrict(updated):
    planes, row_count, col_count = updated.shape
    return updated.reshape(planes, row_count // 3, 3, col_count // 3, 3).sum(axis=(2, 4)) / 9.0

def reference(strips, anchor, wet_mask, bathy_index, bed_levels, coarse):
    fine_rows = TR * N_ROW
    fine_cols = TC * N_COL
    fields_all = strips.reshape(N_NEST, 3, fine_rows, fine_cols)
    coarse_rows = NCR
    coarse_cols = NCC
    canvas = jnp.zeros((4, coarse_rows + CR, coarse_cols + CC), jnp.float32)
    outputs = []
    for nest_id in range(N_NEST):
        wetness = expand(wet_mask[nest_id].astype(jnp.float32))
        bed_fine = expand(lookup(bathy_index[nest_id], bed_levels))
        padded = jnp.pad(fields_all[nest_id], ((0, 0), (1, 1), (1, 1)))
        wet_pad = jnp.pad(wetness, 1)
        bed_pad = jnp.pad(bed_fine, 1)
        updated = advance(padded, bed_pad, wet_pad)
        outputs.append(updated)
        restricted = restrict(updated)
        contribution = jnp.concatenate([restricted, jnp.ones((1,) + restricted.shape[1:], jnp.float32)], axis=0)
        start_row = (nest_id * N_ROW * CR + anchor[nest_id, 0]).astype(jnp.int32)
        start_col = anchor[nest_id, 1].astype(jnp.int32)
        placed = lax.dynamic_update_slice(jnp.zeros_like(canvas), contribution, (jnp.int32(0), start_row, start_col))
        canvas = canvas + placed
    received_sum = canvas[:, :coarse_rows, :coarse_cols]
    coarse_next = (coarse + received_sum[:3]) / (1.0 + received_sum[3])
    return (jnp.stack(outputs), coarse_next)
```

```python
import jax
import jax.numpy as jnp
from jax import lax
from jax.experimental import pallas as pl
from jax.experimental.pallas import tpu as pltpu
from jax.sharding import PartitionSpec as P


gravity = 1.0
courant = 0.2
F32 = jnp.float32
HIGH = lax.Precision.HIGHEST


def padded_2(cells, sides, width):
    for axis, dim in sides:
        count = lax.axis_size(axis)
        ends = count - 1
        head = lax.slice_in_dim(cells, 0, width, axis=dim)
        tail = lax.slice_in_dim(cells, cells.shape[dim] - width, cells.shape[dim], axis=dim)
        cells = jnp.concatenate(
            [
                lax.ppermute(tail, axis, [(i, (i + 1) % count) for i in range(ends)]),
                cells,
                lax.ppermute(head, axis, [((i + 1) % count, i) for i in range(ends)]),
            ],
            axis=dim,
        )
    return cells


def passed_along(block, axis, distance):
    devices = range(lax.axis_size(axis))
    route = [(i - distance, i) for i in devices if i - distance in devices]
    return lax.ppermute(block, axis, route)


def advance(padded, bed_pad, wet_pad):
    depth_now = padded[0]
    flow_u = padded[1]
    flow_v = padded[2]
    depth_safe = jnp.where(wet_pad > 0.5, depth_now, 1.0)
    speed_u = flow_u / depth_safe
    speed_v = flow_v / depth_safe
    celerity = jnp.sqrt(gravity * depth_safe)
    pressure = 0.5 * gravity * depth_safe * depth_safe
    fluxes_x = (flow_u, flow_u * speed_u + pressure, flow_v * speed_u)
    fluxes_y = (flow_v, flow_u * speed_v, flow_v * speed_v + pressure)
    reach_x = jnp.abs(speed_u) + celerity
    reach_y = jnp.abs(speed_v) + celerity
    open_x = wet_pad[1:-1, :-1] * wet_pad[1:-1, 1:]
    open_y = wet_pad[:-1, 1:-1] * wet_pad[1:, 1:-1]
    bound_x = jnp.maximum(reach_x[1:-1, :-1], reach_x[1:-1, 1:])
    bound_y = jnp.maximum(reach_y[:-1, 1:-1], reach_y[1:, 1:-1])
    slope_x = (bed_pad[1:-1, 1:] - bed_pad[1:-1, :-1]) * open_x
    slope_y = (bed_pad[1:, 1:-1] - bed_pad[:-1, 1:-1]) * open_y
    centre = depth_now[1:-1, 1:-1]
    sources = (
        None,
        -0.5 * gravity * centre * (slope_x[:, 1:] + slope_x[:, :-1]),
        -0.5 * gravity * centre * (slope_y[1:] + slope_y[:-1]),
    )
    results = []
    for plane in range(3):
        state = padded[plane]
        flux_col = fluxes_x[plane]
        flux_row = fluxes_y[plane]
        face_x = (
            0.5 * (flux_col[1:-1, :-1] + flux_col[1:-1, 1:])
            - 0.5 * bound_x * (state[1:-1, 1:] - state[1:-1, :-1])
        ) * open_x
        face_y = (
            0.5 * (flux_row[:-1, 1:-1] + flux_row[1:, 1:-1])
            - 0.5 * bound_y * (state[1:, 1:-1] - state[:-1, 1:-1])
        ) * open_y
        value = (
            state[1:-1, 1:-1]
            - courant * (face_x[:, 1:] - face_x[:, :-1])
            - courant * (face_y[1:] - face_y[:-1])
        )
        if plane > 0:
            value = value + courant * sources[plane]
        results.append(value)
    return jnp.stack(results)


def expand(cells):
    return jnp.repeat(jnp.repeat(cells, 3, axis=-2), 3, axis=-1)


def lookup(classes, levels):
    ladder = jnp.arange(levels.shape[0], dtype=jnp.int32)
    matches = classes[None] == ladder[:, None, None]
    return jnp.sum(jnp.where(matches, levels[:, None, None], 0.0), axis=0)


def restrict(updated):
    planes, row_count, col_count = updated.shape
    return updated.reshape(planes, row_count // 3, 3, col_count // 3, 3).sum(axis=(2, 4)) / 9.0


def local_general(strips, anchor, wet_mask, bathy_index, bed_levels, coarse):
    tile_blocks = strips.shape[2]
    band_rows = strips.shape[4]
    full_cols = strips.shape[5]
    columns = lax.axis_size("col")
    tile_cols = full_cols // columns
    layered = (
        strips[0, :, :, 0]
        .reshape(3, tile_blocks, band_rows, columns, tile_cols)
        .transpose(0, 1, 3, 2, 4)
    )
    flattened = layered.reshape(3, tile_blocks * columns, band_rows, tile_cols)
    arrived = lax.all_to_all(flattened, ("row", "col"), split_axis=1, concat_axis=1, tiled=True)
    fields = arrived.reshape(3, tile_blocks * columns * band_rows, tile_cols)
    bed_fine = expand(lookup(bathy_index[0], bed_levels))
    wetness = expand(wet_mask[0].astype(F32))
    stacked = jnp.concatenate([fields, bed_fine[None], wetness[None]], axis=0)
    padded_all = padded_2(stacked, (("row", 1), ("col", 2)), 1)
    updated = advance(padded_all[:3], padded_all[3], padded_all[4])
    restricted = restrict(updated)
    coarse_rows = restricted.shape[1]
    coarse_cols = restricted.shape[2]
    contribution = jnp.concatenate(
        [restricted, jnp.ones((1, coarse_rows, coarse_cols), F32)], axis=0
    )
    nest_index = lax.axis_index("nest")
    corner = lax.dynamic_index_in_dim(anchor, nest_index, 0, keepdims=False)
    canvas = lax.dynamic_update_slice(
        jnp.zeros((4, 2 * coarse_rows, 2 * coarse_cols), F32),
        contribution,
        (jnp.int32(0), corner[0], corner[1]),
    )
    spilled = passed_along(canvas[:, :, coarse_cols:], "col", 1)
    merged = canvas[:, :, :coarse_cols] + spilled
    lowered = passed_along(merged[:, coarse_rows:], ("nest", "row"), 1)
    received_sum = merged[:, :coarse_rows] + lowered
    coarse_next = (coarse + received_sum[:3]) / (1.0 + received_sum[3])
    return (updated[None], coarse_next)


def half_rows(row):
    return pltpu.roll(row, 64, 1), row


def from_half_rows(block, at, lane):
    upper = block[at : at + 1]
    return jnp.where(lane < 64, pltpu.roll(upper, 64, 1), block[at + 1 : at + 2])


def pack_body(dims, where_ref, strips_ref, wet_ref, class_ref, *outs):
    blocks, band, columns, lane_blocks = dims
    owners = blocks * columns
    tile_cols = lane_blocks * 128
    me = where_ref[0]
    my_row = me // columns
    my_col = me % columns
    lane = lax.broadcasted_iota(jnp.int32, (8, 128), 1)
    sub = lax.broadcasted_iota(jnp.int32, (8, 128), 0)
    lane1 = lax.broadcasted_iota(jnp.int32, (1, 128), 1)
    size = wet_ref.shape[1]
    diag = lax.broadcasted_iota(jnp.int32, (size, 128), 0) == lax.broadcasted_iota(
        jnp.int32, (size, 128), 1
    )
    edges = []
    for ref in (wet_ref, class_ref):
        cells = ref[0].astype(F32)
        north = cells[0:1]
        south = cells[size - 1 : size]
        west = jnp.sum(jnp.where(diag, cells[:, 0:1], 0.0), axis=0, keepdims=True)
        east = jnp.sum(jnp.where(diag, cells[:, 127:128], 0.0), axis=0, keepdims=True)
        edges.append((north, south, west, east))
    first = me == 0
    for d in range(owners):
        out = outs[d]
        to = me ^ d
        j = to // columns
        c = to % columns
        base = pl.multiple_of(c * tile_cols, 128)
        for k in range(3):
            for q in range(lane_blocks):
                at = (k * lane_blocks + q) * band
                out[at : at + band] = strips_ref[0, k, j, 0, :, pl.ds(pl.multiple_of(base + q * 128, 128), 128)]
        at = 3 * lane_blocks * band
        west_at = pl.multiple_of(jnp.maximum(base - 128, 0), 128)
        east_at = pl.multiple_of(jnp.where(c == columns - 1, base, base + tile_cols), 128)
        mixed = jnp.zeros((8, 128), F32)
        for g in range(band // 8):
            for k in range(3):
                i = g * 3 + k
                west = strips_ref[0, k, j, 0, g * 8 : g * 8 + 8, pl.ds(west_at, 128)]
                east = strips_ref[0, k, j, 0, g * 8 : g * 8 + 8, pl.ds(east_at, 128)]
                both = pltpu.roll(jnp.where(lane == 127, west, east), 2 * i + 1, 1)
                mixed = jnp.where((lane == 2 * i) | (lane == 2 * i + 1), both, mixed)
        jj = jnp.clip(jnp.where(first, j + 1, j - 1), 0, blocks - 1)
        rows = []
        for k in range(3):
            for q in range(lane_blocks):
                spot = pl.ds(pl.multiple_of(base + q * 128, 128), 128)
                head = strips_ref[0, k, jj, 0, 0:8, spot][0:1]
                tail = strips_ref[0, k, jj, 0, band - 8 : band, spot][7:8]
                rows.append(jnp.where(first, head, tail))
        halo = jnp.zeros((8, 128), F32)
        for i in range(8):
            halo = jnp.where(sub == i, rows[i], halo)
        out[at : at + 8] = halo
        tucked = [rows[8]]
        for north, south, west, east in edges:
            row = jnp.where(
                c == my_col,
                jnp.where(j > my_row, south, north),
                jnp.where(c > my_col, east, west),
            )
            tucked.append(row)
        for n, row in enumerate(tucked):
            low, high = half_rows(row)
            mixed = jnp.where((sub == 2 * n) & (lane >= 64), low, mixed)
            mixed = jnp.where((sub == 2 * n + 1) & (lane >= 64), high, mixed)
        out[at + 8 : at + 16] = mixed


def spread(rows, cols, width, offset=None):
    i = lax.broadcasted_iota(jnp.int32, (rows, cols), 0)
    m = lax.broadcasted_iota(jnp.int32, (rows, cols), 1)
    if offset is not None:
        m = m - offset
        m = jnp.where(m < 0, m + cols, m)
    low = m * width
    return jnp.where((i >= low) & (i < low + width), 1.0, 0.0)


def spread_t(rows, cols, width, offset=None):
    m = lax.broadcasted_iota(jnp.int32, (rows, cols), 0)
    i = lax.broadcasted_iota(jnp.int32, (rows, cols), 1)
    if offset is not None:
        m = m - offset
        m = jnp.where(m < 0, m + rows, m)
    low = m * width
    return jnp.where((i >= low) & (i < low + width), 1.0, 0.0)


def mul(a, b):
    return jnp.dot(a, b, precision=HIGH, preferred_element_type=F32)


def level_of(classes, levels_ref):
    out = jnp.zeros_like(classes)
    for n in range(levels_ref.shape[0]):
        out = jnp.where(classes == n, levels_ref[n], out)
    return out


def prep_body(levels_ref, wet_ref, class_ref, wet_out, bed_out):
    rows, cols = wet_out.shape
    size, width = wet_ref.shape[1], wet_ref.shape[2]
    wet = wet_ref[0].astype(F32)
    bed = level_of(class_ref[0].astype(F32), levels_ref)
    across = spread_t(width, cols, 3)
    down = spread(rows, size, 3)
    wet_out[...] = mul(down, mul(wet, across))
    bed_out[...] = mul(down, mul(bed, across))


def main_body(dims, where_ref, anchor_ref, levels_ref, wet_hbm, bed_hbm, *rest):
    blocks, band, columns, lane_blocks = dims
    owners = blocks * columns
    msgs = rest[:owners]
    fine_out, rolled_out = rest[owners : owners + 2]
    field, wet, bed, extra, made, sems, sem_wb, sem_out = rest[owners + 2 :]
    rows = owners * band
    cols = lane_blocks * 128
    wide = cols + 128
    me = where_ref[0]
    nest = where_ref[1]
    my_row = me // columns
    my_col = me % columns
    body_rows = 3 * lane_blocks * band

    wb = [
        pltpu.make_async_copy(wet_hbm, wet.at[pl.ds(8, rows)], sem_wb.at[0]),
        pltpu.make_async_copy(bed_hbm, bed.at[pl.ds(8, rows)], sem_wb.at[1]),
    ]
    for c in wb:
        c.start()
    copies = []
    for d in range(owners):
        p = me ^ d
        top = pl.multiple_of(8 + p * band, 8)
        for k in range(3):
            for q in range(lane_blocks):
                n = k * lane_blocks + q
                copies.append(
                    pltpu.make_async_copy(
                        msgs[d].at[pl.ds(n * band, band)],
                        field.at[k, pl.ds(top, band), pl.ds(q * 128, 128)],
                        sems.at[d],
                    )
                )
        copies.append(
            pltpu.make_async_copy(
                msgs[d].at[pl.ds(body_rows, 16)], extra.at[p], sems.at[d]
            )
        )
    for c in copies:
        c.start()
    for c in wb:
        c.wait()
    for c in copies:
        c.wait()

    lane1 = lax.broadcasted_iota(jnp.int32, (1, 128), 1)
    for p in range(owners):
        mixed = extra[p, 8:16]
        for g in range(band // 8):
            for k in range(3):
                i = g * 3 + k
                at = 8 + p * band + g * 8
                field[k, at : at + 8, cols:wide] = pltpu.roll(mixed, 127 - 2 * i, 1)
    for source, at in ((owners - 1, 0), (0, 8 + rows)):
        last = from_half_rows(extra[source, 8:16], 0, lane1)
        for k in range(3):
            for q in range(lane_blocks):
                n = k * lane_blocks + q
                row = last if n == 8 else extra[source, n : n + 1]
                field[k, at : at + 8, q * 128 : q * 128 + 128] = jnp.broadcast_to(row, (8, 128))
            field[k, at : at + 8, cols:wide] = jnp.zeros((8, 128), F32)

    def edge(source, inside):
        block = extra[jnp.clip(source, 0, owners - 1), 8:16]
        keep = jnp.where(inside, 1.0, 0.0)
        wet_row = from_half_rows(block, 2, lane1) * keep
        bed_row = level_of(from_half_rows(block, 4, lane1), levels_ref) * keep
        return wet_row, bed_row

    north = edge(me - columns, my_row > 0)
    south = edge(me + columns, my_row < blocks - 1)
    west = edge(me - 1, my_col > 0)
    east = edge(me + 1, my_col < columns - 1)
    across = spread_t(128, wide, 3)
    down = spread(rows, 128, 3)
    sub128 = lax.broadcasted_iota(jnp.int32, (128, 128), 0)
    for n, ref in ((0, wet), (1, bed)):
        for row, at in ((north[n], 0), (south[n], 8 + rows)):
            ref[at : at + 8] = mul(jnp.broadcast_to(row, (8, 128)), across)
        pair = jnp.where(sub128 == 0, east[n], jnp.where(sub128 == 127, west[n], 0.0))
        ref[8 : 8 + rows, cols:wide] = lax.dot_general(
            down, pair, (((1,), (1,)), ((), ())), precision=HIGH, preferred_element_type=F32
        )

    sub = lax.broadcasted_iota(jnp.int32, (8, cols), 0)

    def cells(at):
        at = pl.multiple_of(at, 8)
        h = field[0, pl.ds(at, 8)]
        hu = field[1, pl.ds(at, 8)]
        hv = field[2, pl.ds(at, 8)]
        w = wet[pl.ds(at, 8)]
        z = bed[pl.ds(at, 8)]
        hs = jnp.where(w > 0.5, h, 1.0)
        inv = 1.0 / hs
        u = hu * inv
        v = hv * inv
        c = jnp.sqrt(gravity * hs)
        p = 0.5 * gravity * hs * hs
        f2 = hu * u + p
        m = hv * u
        g3 = hv * v + p
        a = jnp.abs(u) + c
        b = jnp.abs(v) + c
        return h, hu, hv, w, z, f2, m, g3, a, b

    def face(near, far, fluxes_near, fluxes_far, reach_near, reach_far):
        h, hu, hv, w, z = near
        h2, hu2, hv2, w2, z2 = far
        opened = w * w2
        half = 0.5 * opened
        bound = half * jnp.maximum(reach_near, reach_far)
        out = []
        for f, f2, s, s2 in zip(fluxes_near, fluxes_far, (h, hu, hv), (h2, hu2, hv2)):
            out.append(half * (f + f2) - bound * (s2 - s))
        out.append(opened * (z2 - z))
        return out

    def south_face(now, nxt):
        def pick(i):
            a = now[i][:, :cols]
            b = nxt[i][:, :cols]
            return pltpu.roll(jnp.where(sub == 0, b, a), 7, 0)

        h, hu, hv, w, z, f2, m, g3, a, b = [x[:, :cols] for x in now]
        h2, hu2, hv2, w2, z2, m2, g32, b2 = [pick(i) for i in (0, 1, 2, 3, 4, 6, 7, 9)]
        return face(
            (h, hu, hv, w, z), (h2, hu2, hv2, w2, z2), (hv, m, g3), (hv2, m2, g32), b, b2
        )

    before = cells(0)
    start = cells(8)
    above = south_face(before, start)

    def step(t, carry):
        now, above = carry
        at = 8 + t * 8
        nxt = cells(at + 8)
        below = south_face(now, nxt)
        h, hu, hv, w, z, f2, m, g3, a, b = now
        r = [pltpu.roll(x, wide - 1, 1) for x in (h, hu, hv, w, z, f2, m, a)]
        fx = face((h, hu, hv, w, z), tuple(r[:5]), (hu, f2, m), (r[1], r[5], r[6]), a, r[7])
        left = [pltpu.roll(x, 1, 1)[:, :cols] for x in fx]
        right = [x[:, :cols] for x in fx]
        up = [pltpu.roll(jnp.where(sub == 7, y, x), 1, 0) for x, y in zip(below, above)]
        hc = (0.5 * gravity * courant) * h[:, :cols]
        o0 = h[:, :cols] - courant * (right[0] - left[0]) - courant * (below[0] - up[0])
        o1 = (
            hu[:, :cols]
            - courant * (right[1] - left[1])
            - courant * (below[1] - up[1])
            - hc * (right[3] + left[3])
        )
        o2 = (
            hv[:, :cols]
            - courant * (right[2] - left[2])
            - courant * (below[2] - up[2])
            - hc * (below[3] + up[3])
        )
        spot = pl.ds(pl.multiple_of(t * 8, 8), 8)
        made[0, spot] = o0
        made[1, spot] = o1
        made[2, spot] = o2
        return nxt, below

    lax.fori_loop(0, rows // 8, step, (start, above))

    done = pltpu.make_async_copy(made, fine_out.at[0], sem_out)
    done.start()
    coarse_rows = rows // 3
    coarse_cols = cols // 3
    a0 = anchor_ref[nest, 0]
    a1 = anchor_ref[nest, 1]
    gather_rows = spread_t(coarse_rows, rows, 3, a0)
    gather_cols = spread(cols, coarse_cols, 3, a1)
    for k in range(3):
        rolled_out[k] = mul(mul(gather_rows, made[k]), gather_cols) / 9.0
    done.wait()


def local_packed(strips, anchor, wet_mask, bathy_index, bed_levels, coarse):
    blocks, band, full_cols = strips.shape[2], strips.shape[4], strips.shape[5]
    columns = lax.axis_size("col")
    owners = blocks * columns
    cols = full_cols // columns
    lane_blocks = cols // 128
    rows = owners * band
    wide = cols + 128
    dims = (blocks, band, columns, lane_blocks)
    height = 3 * lane_blocks * band + 16
    me = lax.axis_index(("row", "col")).astype(jnp.int32)
    nest = lax.axis_index("nest").astype(jnp.int32)
    spot = jnp.stack([me, nest])
    smem = pl.BlockSpec(memory_space=pltpu.SMEM)
    vmem = pl.BlockSpec(memory_space=pltpu.VMEM)
    hbm = pl.BlockSpec(memory_space=pl.ANY)

    messages = pl.pallas_call(
        lambda *refs: pack_body(dims, *refs),
        in_specs=[smem, vmem, vmem, vmem],
        out_specs=[vmem] * owners,
        out_shape=[jax.ShapeDtypeStruct((height, 128), F32)] * owners,
        name="pack",
    )(spot, strips, wet_mask, bathy_index)

    crossing = [d for d in range(1, owners) if (d % columns) * 2 >= columns]
    others = [d for d in range(1, owners) if d not in crossing]
    arrived = {0: messages[0]}
    for d in crossing + others:
        arrived[d] = lax.ppermute(
            messages[d], ("row", "col"), [(i, i ^ d) for i in range(owners)]
        )

    wet_fine, bed_fine = pl.pallas_call(
        prep_body,
        in_specs=[smem, vmem, vmem],
        out_specs=[vmem, vmem],
        out_shape=[jax.ShapeDtypeStruct((rows, wide), F32)] * 2,
        name="prep",
    )(bed_levels, wet_mask, bathy_index)

    coarse_rows = rows // 3
    coarse_cols = cols // 3
    fine, rolled = pl.pallas_call(
        lambda *refs: main_body(dims, *refs),
        in_specs=[smem, smem, smem, hbm, hbm] + [hbm] * owners,
        out_specs=[hbm, vmem],
        out_shape=[
            jax.ShapeDtypeStruct((1, 3, rows, cols), F32),
            jax.ShapeDtypeStruct((3, coarse_rows, coarse_cols), F32),
        ],
        scratch_shapes=[
            pltpu.VMEM((3, rows + 16, wide), F32),
            pltpu.VMEM((rows + 16, wide), F32),
            pltpu.VMEM((rows + 16, wide), F32),
            pltpu.VMEM((owners, 16, 128), F32),
            pltpu.VMEM((3, rows, cols), F32),
            pltpu.SemaphoreType.DMA((owners,)),
            pltpu.SemaphoreType.DMA((2,)),
            pltpu.SemaphoreType.DMA,
        ],
        name="main",
    )(spot, anchor, bed_levels, wet_fine, bed_fine, *[arrived[d] for d in range(owners)])

    lines = lax.axis_size("nest") * lax.axis_size("row")
    rights = [(c, c + 1) for c in range(columns - 1)]
    downs = [(l, l + 1) for l in range(lines - 1)]
    both = [(l * columns + c, l2 * columns + c2) for l, l2 in downs for c, c2 in rights]
    diagonal = lax.ppermute(rolled, ("nest", "row", "col"), both)
    from_left = lax.ppermute(rolled, "col", rights)
    from_up = lax.ppermute(rolled, ("nest", "row"), downs)

    row_at = lax.axis_index("row")
    col_at = lax.axis_index("col")
    mine = anchor[nest]
    up_nest = jnp.where(row_at == 0, jnp.maximum(nest - 1, 0), nest)
    theirs = anchor[up_nest]
    has_left = col_at > 0
    has_up = (row_at > 0) | (nest > 0)
    i = lax.broadcasted_iota(jnp.int32, (coarse_rows, coarse_cols), 0)
    m = lax.broadcasted_iota(jnp.int32, (coarse_rows, coarse_cols), 1)
    own_rows = i >= mine[0]
    up_rows = (i < theirs[0]) & has_up
    own = jnp.where(own_rows, jnp.where(m >= mine[1], rolled, from_left), 0.0)
    upper = jnp.where(up_rows, jnp.where(m >= theirs[1], from_up, diagonal), 0.0)
    count = (
        1.0
        + jnp.where(own_rows & ((m >= mine[1]) | has_left), 1.0, 0.0)
        + jnp.where(up_rows & ((m >= theirs[1]) | has_left), 1.0, 0.0)
    )
    coarse_next = (coarse + own + upper) / count
    return (fine, coarse_next)


def local(strips, anchor, wet_mask, bathy_index, bed_levels, coarse):
    columns = lax.axis_size("col")
    owners = strips.shape[2] * columns
    cols = strips.shape[5] // columns
    band = strips.shape[4]
    fits = (
        owners & (owners - 1) == 0
        and 2 <= owners <= 16
        and strips.shape[2] == lax.axis_size("row")
        and band == 24
        and cols == 384
        and owners * band == 384
        and wet_mask.shape[1:] == (128, 128)
    )
    run = local_packed if fits else local_general
    return run(strips, anchor, wet_mask, bathy_index, bed_levels, coarse)


def solution(mesh):
    return jax.shard_map(
        local,
        mesh=mesh,
        in_specs=(
            P("nest", None, None, ("row", "col"), None, None),
            P(),
            P("nest", "row", "col"),
            P("nest", "row", "col"),
            P(),
            P(None, ("nest", "row"), "col"),
        ),
        out_specs=(P("nest", None, "row", "col"), P(None, ("nest", "row"), "col")),
        check_vma=False,
    )
```

```python
import jax
import jax.numpy as jnp
from jax import lax
from jax.experimental import pallas as pl
from jax.experimental.pallas import tpu as pltpu
from jax.sharding import PartitionSpec as P


gravity = 1.0
courant = 0.2
F32 = jnp.float32


def padded_2(cells, sides, width):
    for axis, dim in sides:
        count = lax.axis_size(axis)
        ends = count - 1
        head = lax.slice_in_dim(cells, 0, width, axis=dim)
        tail = lax.slice_in_dim(cells, cells.shape[dim] - width, cells.shape[dim], axis=dim)
        cells = jnp.concatenate(
            [
                lax.ppermute(tail, axis, [(i, (i + 1) % count) for i in range(ends)]),
                cells,
                lax.ppermute(head, axis, [((i + 1) % count, i) for i in range(ends)]),
            ],
            axis=dim,
        )
    return cells


def passed_along(block, axis, distance):
    devices = range(lax.axis_size(axis))
    route = [(i - distance, i) for i in devices if i - distance in devices]
    return lax.ppermute(block, axis, route)


def advance(padded, bed_pad, wet_pad):
    depth_now = padded[0]
    flow_u = padded[1]
    flow_v = padded[2]
    depth_safe = jnp.where(wet_pad > 0.5, depth_now, 1.0)
    speed_u = flow_u / depth_safe
    speed_v = flow_v / depth_safe
    celerity = jnp.sqrt(gravity * depth_safe)
    pressure = 0.5 * gravity * depth_safe * depth_safe
    fluxes_x = (flow_u, flow_u * speed_u + pressure, flow_v * speed_u)
    fluxes_y = (flow_v, flow_u * speed_v, flow_v * speed_v + pressure)
    reach_x = jnp.abs(speed_u) + celerity
    reach_y = jnp.abs(speed_v) + celerity
    open_x = wet_pad[1:-1, :-1] * wet_pad[1:-1, 1:]
    open_y = wet_pad[:-1, 1:-1] * wet_pad[1:, 1:-1]
    bound_x = jnp.maximum(reach_x[1:-1, :-1], reach_x[1:-1, 1:])
    bound_y = jnp.maximum(reach_y[:-1, 1:-1], reach_y[1:, 1:-1])
    slope_x = (bed_pad[1:-1, 1:] - bed_pad[1:-1, :-1]) * open_x
    slope_y = (bed_pad[1:, 1:-1] - bed_pad[:-1, 1:-1]) * open_y
    centre = depth_now[1:-1, 1:-1]
    sources = (
        None,
        -0.5 * gravity * centre * (slope_x[:, 1:] + slope_x[:, :-1]),
        -0.5 * gravity * centre * (slope_y[1:] + slope_y[:-1]),
    )
    results = []
    for plane in range(3):
        state = padded[plane]
        flux_col = fluxes_x[plane]
        flux_row = fluxes_y[plane]
        face_x = (
            0.5 * (flux_col[1:-1, :-1] + flux_col[1:-1, 1:])
            - 0.5 * bound_x * (state[1:-1, 1:] - state[1:-1, :-1])
        ) * open_x
        face_y = (
            0.5 * (flux_row[:-1, 1:-1] + flux_row[1:, 1:-1])
            - 0.5 * bound_y * (state[1:, 1:-1] - state[:-1, 1:-1])
        ) * open_y
        value = (
            state[1:-1, 1:-1]
            - courant * (face_x[:, 1:] - face_x[:, :-1])
            - courant * (face_y[1:] - face_y[:-1])
        )
        if plane > 0:
            value = value + courant * sources[plane]
        results.append(value)
    return jnp.stack(results)


def expand(cells):
    return jnp.repeat(jnp.repeat(cells, 3, axis=-2), 3, axis=-1)


def lookup(classes, levels):
    ladder = jnp.arange(levels.shape[0], dtype=jnp.int32)
    matches = classes[None] == ladder[:, None, None]
    return jnp.sum(jnp.where(matches, levels[:, None, None], 0.0), axis=0)


def restrict(updated):
    planes, row_count, col_count = updated.shape
    return updated.reshape(planes, row_count // 3, 3, col_count // 3, 3).sum(axis=(2, 4)) / 9.0


def local_general(strips, anchor, wet_mask, bathy_index, bed_levels, coarse):
    tile_blocks = strips.shape[2]
    band_rows = strips.shape[4]
    full_cols = strips.shape[5]
    columns = lax.axis_size("col")
    tile_cols = full_cols // columns
    layered = (
        strips[0, :, :, 0]
        .reshape(3, tile_blocks, band_rows, columns, tile_cols)
        .transpose(0, 1, 3, 2, 4)
    )
    flattened = layered.reshape(3, tile_blocks * columns, band_rows, tile_cols)
    arrived = lax.all_to_all(flattened, ("row", "col"), split_axis=1, concat_axis=1, tiled=True)
    fields = arrived.reshape(3, tile_blocks * columns * band_rows, tile_cols)
    bed_fine = expand(lookup(bathy_index[0], bed_levels))
    wetness = expand(wet_mask[0].astype(F32))
    stacked = jnp.concatenate([fields, bed_fine[None], wetness[None]], axis=0)
    padded_all = padded_2(stacked, (("row", 1), ("col", 2)), 1)
    updated = advance(padded_all[:3], padded_all[3], padded_all[4])
    restricted = restrict(updated)
    coarse_rows = restricted.shape[1]
    coarse_cols = restricted.shape[2]
    contribution = jnp.concatenate(
        [restricted, jnp.ones((1, coarse_rows, coarse_cols), F32)], axis=0
    )
    nest_index = lax.axis_index("nest")
    corner = lax.dynamic_index_in_dim(anchor, nest_index, 0, keepdims=False)
    canvas = lax.dynamic_update_slice(
        jnp.zeros((4, 2 * coarse_rows, 2 * coarse_cols), F32),
        contribution,
        (jnp.int32(0), corner[0], corner[1]),
    )
    spilled = passed_along(canvas[:, :, coarse_cols:], "col", 1)
    merged = canvas[:, :, :coarse_cols] + spilled
    lowered = passed_along(merged[:, coarse_rows:], ("nest", "row"), 1)
    received_sum = merged[:, :coarse_rows] + lowered
    coarse_next = (coarse + received_sum[:3]) / (1.0 + received_sum[3])
    return (updated[None], coarse_next)


def half_rows(row):
    return pltpu.roll(row, 64, 1), row


def from_half_rows(block, at, lane):
    upper = block[at : at + 1]
    return jnp.where(lane < 64, pltpu.roll(upper, 64, 1), block[at + 1 : at + 2])


def pack_body(dims, where_ref, strips_ref, wet_ref, class_ref, *outs):
    blocks, band, columns, lane_blocks = dims
    owners = blocks * columns
    tile_cols = lane_blocks * 128
    me = where_ref[0]
    my_row = me // columns
    my_col = me % columns
    lane = lax.broadcasted_iota(jnp.int32, (8, 128), 1)
    sub = lax.broadcasted_iota(jnp.int32, (8, 128), 0)
    lane1 = lax.broadcasted_iota(jnp.int32, (1, 128), 1)
    size = wet_ref.shape[1]
    diag = lax.broadcasted_iota(jnp.int32, (size, 128), 0) == lax.broadcasted_iota(
        jnp.int32, (size, 128), 1
    )
    edges = []
    for ref in (wet_ref, class_ref):
        cells = ref[0].astype(F32)
        north = cells[0:1]
        south = cells[size - 1 : size]
        west = jnp.sum(jnp.where(diag, cells[:, 0:1], 0.0), axis=0, keepdims=True)
        east = jnp.sum(jnp.where(diag, cells[:, 127:128], 0.0), axis=0, keepdims=True)
        edges.append((north, south, west, east))
    first = me == 0
    for d in range(owners):
        out = outs[d]
        to = me ^ d
        j = to // columns
        c = to % columns
        base = pl.multiple_of(c * tile_cols, 128)
        for k in range(3):
            for q in range(lane_blocks):
                at = (k * lane_blocks + q) * band
                out[at : at + band] = strips_ref[0, k, j, 0, :, pl.ds(pl.multiple_of(base + q * 128, 128), 128)]
        at = 3 * lane_blocks * band
        west_at = pl.multiple_of(jnp.maximum(base - 128, 0), 128)
        east_at = pl.multiple_of(jnp.where(c == columns - 1, base, base + tile_cols), 128)
        mixed = jnp.zeros((8, 128), F32)
        for g in range(band // 8):
            for k in range(3):
                i = g * 3 + k
                west = strips_ref[0, k, j, 0, g * 8 : g * 8 + 8, pl.ds(west_at, 128)]
                east = strips_ref[0, k, j, 0, g * 8 : g * 8 + 8, pl.ds(east_at, 128)]
                both = pltpu.roll(jnp.where(lane == 127, west, east), 2 * i + 1, 1)
                mixed = jnp.where((lane == 2 * i) | (lane == 2 * i + 1), both, mixed)
        jj = jnp.clip(jnp.where(first, j + 1, j - 1), 0, blocks - 1)
        rows = []
        for k in range(3):
            for q in range(lane_blocks):
                spot = pl.ds(pl.multiple_of(base + q * 128, 128), 128)
                head = strips_ref[0, k, jj, 0, 0:8, spot][0:1]
                tail = strips_ref[0, k, jj, 0, band - 8 : band, spot][7:8]
                rows.append(jnp.where(first, head, tail))
        halo = jnp.zeros((8, 128), F32)
        for i in range(8):
            halo = jnp.where(sub == i, rows[i], halo)
        out[at : at + 8] = halo
        tucked = [rows[8]]
        for north, south, west, east in edges:
            row = jnp.where(
                c == my_col,
                jnp.where(j > my_row, south, north),
                jnp.where(c > my_col, east, west),
            )
            tucked.append(row)
        for n, row in enumerate(tucked):
            low, high = half_rows(row)
            mixed = jnp.where((sub == 2 * n) & (lane >= 64), low, mixed)
            mixed = jnp.where((sub == 2 * n + 1) & (lane >= 64), high, mixed)
        out[at + 8 : at + 16] = mixed


def spread(rows, cols, width, offset=None):
    i = lax.broadcasted_iota(jnp.int32, (rows, cols), 0)
    m = lax.broadcasted_iota(jnp.int32, (rows, cols), 1)
    if offset is not None:
        m = m - offset
        m = jnp.where(m < 0, m + cols, m)
    low = m * width
    return jnp.where((i >= low) & (i < low + width), 1.0, 0.0)


def spread_t(rows, cols, width, offset=None):
    m = lax.broadcasted_iota(jnp.int32, (rows, cols), 0)
    i = lax.broadcasted_iota(jnp.int32, (rows, cols), 1)
    if offset is not None:
        m = m - offset
        m = jnp.where(m < 0, m + rows, m)
    low = m * width
    return jnp.where((i >= low) & (i < low + width), 1.0, 0.0)


def level_of(classes, levels_ref):
    out = jnp.zeros_like(classes)
    for n in range(levels_ref.shape[0]):
        out = jnp.where(classes == n, levels_ref[n], out)
    return out


def prep_body(levels_ref, wet_ref, class_ref, wet_out, bed_out):
    rows, cols = wet_out.shape
    size, width = wet_ref.shape[1], wet_ref.shape[2]
    wet = wet_ref[0].astype(F32)
    bed = level_of(class_ref[0].astype(F32), levels_ref)
    across = spread_t(width, cols, 3)
    down = spread(rows, size, 3)
    wet_out[...] = mul_left(down, mul_right(wet, across, 1), 1)
    bed_out[...] = mul_left(down, mul_right(bed, across, 3), 3)


def split(x, parts):
    out = []
    for n in range(parts):
        piece = x.astype(jnp.bfloat16)
        out.append(piece)
        if n + 1 < parts:
            x = x - piece.astype(F32)
    return out


def mul_left(matrix, x, parts):
    matrix = matrix.astype(jnp.bfloat16)
    return sum(jnp.dot(matrix, piece, preferred_element_type=F32) for piece in split(x, parts))


def mul_right(x, matrix, parts):
    matrix = matrix.astype(jnp.bfloat16)
    return sum(jnp.dot(piece, matrix, preferred_element_type=F32) for piece in split(x, parts))


def mul_left_t(matrix, x, parts):
    matrix = matrix.astype(jnp.bfloat16)
    return sum(
        lax.dot_general(matrix, piece, (((1,), (1,)), ((), ())), preferred_element_type=F32)
        for piece in split(x, parts)
    )


def main_body(dims, order, where_ref, anchor_ref, levels_ref, wet_in, bed_in, *rest):
    blocks, band, columns, lane_blocks = dims
    owners = blocks * columns
    msgs = rest[:owners]
    fine_out, rolled_out = rest[owners : owners + 2]
    field, wet, bed, extra, made, sem_out = rest[owners + 2 :]
    rows = owners * band
    cols = lane_blocks * 128
    wide = cols + 128
    me = where_ref[0]
    nest = where_ref[1]
    my_row = me // columns
    my_col = me % columns
    body_rows = 3 * lane_blocks * band

    lane1 = lax.broadcasted_iota(jnp.int32, (1, 128), 1)
    wet[8 : 8 + rows] = wet_in[...]
    bed[8 : 8 + rows] = bed_in[...]
    for message, d in zip(msgs, order):
        p = me ^ d
        top = pl.multiple_of(8 + p * band, 8)
        mixed = message[body_rows + 8 : body_rows + 16]
        for k in range(3):
            for q in range(lane_blocks):
                n = k * lane_blocks + q
                field[k, pl.ds(top, band), q * 128 : q * 128 + 128] = message[
                    n * band : n * band + band
                ]
            for g in range(band // 8):
                i = g * 3 + k
                at = pl.multiple_of(top + g * 8, 8)
                field[k, pl.ds(at, 8), cols:wide] = pltpu.roll(mixed, 127 - 2 * i, 1)
        extra[p] = message[body_rows : body_rows + 16]

    for source, at in ((owners - 1, 0), (0, 8 + rows)):
        last = from_half_rows(extra[source, 8:16], 0, lane1)
        for k in range(3):
            for q in range(lane_blocks):
                n = k * lane_blocks + q
                row = last if n == 8 else extra[source, n : n + 1]
                field[k, at : at + 8, q * 128 : q * 128 + 128] = jnp.broadcast_to(row, (8, 128))
            field[k, at : at + 8, cols:wide] = jnp.zeros((8, 128), F32)

    def edge(source, inside):
        block = extra[jnp.clip(source, 0, owners - 1), 8:16]
        keep = jnp.where(inside, 1.0, 0.0)
        wet_row = from_half_rows(block, 2, lane1) * keep
        bed_row = level_of(from_half_rows(block, 4, lane1), levels_ref) * keep
        return wet_row, bed_row

    north = edge(me - columns, my_row > 0)
    south = edge(me + columns, my_row < blocks - 1)
    west = edge(me - 1, my_col > 0)
    east = edge(me + 1, my_col < columns - 1)
    sub128 = lax.broadcasted_iota(jnp.int32, (128, 128), 0)
    sub8 = lax.broadcasted_iota(jnp.int32, (8, 128), 0)
    stack = jnp.zeros((8, 128), F32)
    for n, row in enumerate((north[0], north[1], south[0], south[1])):
        stack = jnp.where(sub8 == n, row, stack)
    ends = mul_right(stack, spread_t(128, wide, 3), 3)
    for n, (ref, at) in enumerate(((wet, 0), (bed, 0), (wet, 8 + rows), (bed, 8 + rows))):
        ref[at : at + 8] = jnp.broadcast_to(ends[n : n + 1], (8, wide))
    pair = jnp.zeros((128, 128), F32)
    for n, row in ((0, east[0]), (127, west[0]), (64, east[1]), (63, west[1])):
        pair = jnp.where(sub128 == n, row, pair)
    sides = mul_left_t(spread(rows, 128, 3), pair, 3)
    wet[8 : 8 + rows, cols:wide] = sides
    bed[8 : 8 + rows, cols:wide] = pltpu.roll(sides, 64, 1)

    sub = lax.broadcasted_iota(jnp.int32, (8, cols), 0)

    def cells(at):
        at = pl.multiple_of(at, 8)
        h = field[0, pl.ds(at, 8)]
        hu = field[1, pl.ds(at, 8)]
        hv = field[2, pl.ds(at, 8)]
        w = wet[pl.ds(at, 8)]
        z = bed[pl.ds(at, 8)]
        hs = jnp.where(w > 0.5, h, 1.0)
        inv = 1.0 / hs
        u = hu * inv
        v = hv * inv
        c = jnp.sqrt(gravity * hs)
        p = 0.5 * gravity * hs * hs
        f2 = hu * u + p
        m = hv * u
        g3 = hv * v + p
        a = jnp.abs(u) + c
        b = jnp.abs(v) + c
        return h, hu, hv, w, z, f2, m, g3, a, b

    def face(near, far, fluxes_near, fluxes_far, reach_near, reach_far):
        h, hu, hv, w, z = near
        h2, hu2, hv2, w2, z2 = far
        opened = w * w2
        half = (0.5 * courant) * opened
        bound = half * jnp.maximum(reach_near, reach_far)
        out = []
        for f, f2, s, s2 in zip(fluxes_near, fluxes_far, (h, hu, hv), (h2, hu2, hv2)):
            out.append(half * (f + f2) - bound * (s2 - s))
        out.append(half * (z2 - z))
        return out

    def south_face(now, nxt):
        def pick(i):
            a = now[i][:, :cols]
            b = nxt[i][:, :cols]
            return pltpu.roll(jnp.where(sub == 0, b, a), 7, 0)

        h, hu, hv, w, z, f2, m, g3, a, b = [x[:, :cols] for x in now]
        h2, hu2, hv2, w2, z2, m2, g32, b2 = [pick(i) for i in (0, 1, 2, 3, 4, 6, 7, 9)]
        return face(
            (h, hu, hv, w, z), (h2, hu2, hv2, w2, z2), (hv, m, g3), (hv2, m2, g32), b, b2
        )

    start = cells(8)
    above = south_face(cells(0), start)

    def step(t, carry):
        now, above = carry
        at = 8 + t * 8
        nxt = cells(at + 8)
        below = south_face(now, nxt)
        h, hu, hv, w, z, f2, m, g3, a, b = now
        r = [pltpu.roll(x, wide - 1, 1) for x in (h, hu, hv, w, z, f2, m, a)]
        fx = face((h, hu, hv, w, z), tuple(r[:5]), (hu, f2, m), (r[1], r[5], r[6]), a, r[7])
        left = [pltpu.roll(x, 1, 1)[:, :cols] for x in fx]
        right = [x[:, :cols] for x in fx]
        up = [pltpu.roll(jnp.where(sub == 7, y, x), 1, 0) for x, y in zip(below, above)]
        hc = gravity * h[:, :cols]
        o0 = h[:, :cols] - (right[0] - left[0]) - (below[0] - up[0])
        o1 = hu[:, :cols] - (right[1] - left[1]) - (below[1] - up[1]) - hc * (right[3] + left[3])
        o2 = hv[:, :cols] - (right[2] - left[2]) - (below[2] - up[2]) - hc * (below[3] + up[3])
        spot = pl.ds(pl.multiple_of(t * 8, 8), 8)
        for k, o in enumerate((o0, o1, o2)):
            for q in range(lane_blocks):
                made[k, q, spot] = o[:, q * 128 : q * 128 + 128]
        return nxt, below

    lax.fori_loop(0, rows // 8, step, (start, above), unroll=2)

    done = [
        pltpu.make_async_copy(
            made.at[:, q], fine_out.at[0, :, :, pl.ds(q * 128, 128)], sem_out.at[q]
        )
        for q in range(lane_blocks)
    ]
    for c in done:
        c.start()
    coarse_rows = rows // 3
    coarse_cols = cols // 3
    a0 = anchor_ref[nest, 0]
    a1 = anchor_ref[nest, 1]
    gather_cols = spread(cols, coarse_cols, 3, a1)
    for k in range(3):
        total = jnp.concatenate(
            [
                sum(made[k, q, pl.ds(n, coarse_rows, stride=3), :] for n in range(3))
                for q in range(lane_blocks)
            ],
            axis=1,
        )
        mean = mul_right(total, gather_cols, 2) * (1.0 / 9.0)
        rolled_out[k] = pltpu.roll(mean, a0, 0)
    for c in done:
        c.wait()


def main_call(dims, order, spot, anchor, bed_levels, wet_fine, bed_fine, messages):
    blocks, band, columns, lane_blocks = dims
    owners = blocks * columns
    rows = owners * band
    cols = lane_blocks * 128
    wide = cols + 128
    smem = pl.BlockSpec(memory_space=pltpu.SMEM)
    vmem = pl.BlockSpec(memory_space=pltpu.VMEM)
    return pl.pallas_call(
        lambda *refs: main_body(dims, order, *refs),
        in_specs=[smem, smem, smem, vmem, vmem] + [vmem] * owners,
        out_specs=[pl.BlockSpec(memory_space=pl.ANY), vmem],
        out_shape=[
            jax.ShapeDtypeStruct((1, 3, rows, cols), F32),
            jax.ShapeDtypeStruct((3, rows // 3, cols // 3), F32),
        ],
        scratch_shapes=[
            pltpu.VMEM((3, rows + 16, wide), F32),
            pltpu.VMEM((rows + 16, wide), F32),
            pltpu.VMEM((rows + 16, wide), F32),
            pltpu.VMEM((owners, 16, 128), F32),
            pltpu.VMEM((3, lane_blocks, rows, 128), F32),
            pltpu.SemaphoreType.DMA((lane_blocks,)),
        ],
        name="main",
    )(spot, anchor, bed_levels, wet_fine, bed_fine, *messages)


def local_packed(strips, anchor, wet_mask, bathy_index, bed_levels, coarse):
    blocks, band, full_cols = strips.shape[2], strips.shape[4], strips.shape[5]
    columns = lax.axis_size("col")
    owners = blocks * columns
    cols = full_cols // columns
    lane_blocks = cols // 128
    rows = owners * band
    wide = cols + 128
    dims = (blocks, band, columns, lane_blocks)
    height = 3 * lane_blocks * band + 16
    me = lax.axis_index(("row", "col")).astype(jnp.int32)
    nest = lax.axis_index("nest").astype(jnp.int32)
    spot = jnp.stack([me, nest])
    smem = pl.BlockSpec(memory_space=pltpu.SMEM)
    vmem = pl.BlockSpec(memory_space=pltpu.VMEM)

    messages = pl.pallas_call(
        lambda *refs: pack_body(dims, *refs),
        in_specs=[smem, vmem, vmem, vmem],
        out_specs=[vmem] * owners,
        out_shape=[jax.ShapeDtypeStruct((height, 128), F32)] * owners,
        name="pack",
    )(spot, strips, wet_mask, bathy_index)

    def rank(d):
        r, c = d // columns, d % columns
        return (c * 2 < columns, (r + c) % 2, r, c)

    wanted = sorted(range(1, owners), key=rank)
    turns = sorted(range(owners - 1), key=str)
    order = [0] * owners
    for turn, d in zip(turns, wanted):
        order[turn + 1] = d
    arrived = [
        lax.ppermute(messages[d], ("row", "col"), [(i, i ^ d) for i in range(owners)])
        if d
        else messages[0]
        for d in order
    ]

    wet_fine, bed_fine = pl.pallas_call(
        prep_body,
        in_specs=[smem, vmem, vmem],
        out_specs=[vmem, vmem],
        out_shape=[jax.ShapeDtypeStruct((rows, wide), F32)] * 2,
        name="prep",
    )(bed_levels, wet_mask, bathy_index)

    coarse_rows = rows // 3
    coarse_cols = cols // 3
    fine, rolled = main_call(
        dims, order, spot, anchor, bed_levels, wet_fine, bed_fine, arrived
    )

    lines = lax.axis_size("nest") * lax.axis_size("row")
    rights = [(c, c + 1) for c in range(columns - 1)]
    downs = [(l, l + 1) for l in range(lines - 1)]
    both = [(l * columns + c, l2 * columns + c2) for l, l2 in downs for c, c2 in rights]
    diagonal = lax.ppermute(rolled, ("nest", "row", "col"), both)
    from_left = lax.ppermute(rolled, "col", rights)
    from_up = lax.ppermute(rolled, ("nest", "row"), downs)

    row_at = lax.axis_index("row")
    col_at = lax.axis_index("col")
    mine = anchor[nest]
    up_nest = jnp.where(row_at == 0, jnp.maximum(nest - 1, 0), nest)
    theirs = anchor[up_nest]
    has_left = col_at > 0
    has_up = (row_at > 0) | (nest > 0)
    i = lax.broadcasted_iota(jnp.int32, (coarse_rows, coarse_cols), 0)
    m = lax.broadcasted_iota(jnp.int32, (coarse_rows, coarse_cols), 1)
    own_rows = i >= mine[0]
    up_rows = (i < theirs[0]) & has_up
    own = jnp.where(own_rows, jnp.where(m >= mine[1], rolled, from_left), 0.0)
    upper = jnp.where(up_rows, jnp.where(m >= theirs[1], from_up, diagonal), 0.0)
    count = (
        1.0
        + jnp.where(own_rows & ((m >= mine[1]) | has_left), 1.0, 0.0)
        + jnp.where(up_rows & ((m >= theirs[1]) | has_left), 1.0, 0.0)
    )
    coarse_next = (coarse + own + upper) / count
    return (fine, coarse_next)


def local(strips, anchor, wet_mask, bathy_index, bed_levels, coarse):
    columns = lax.axis_size("col")
    owners = strips.shape[2] * columns
    cols = strips.shape[5] // columns
    band = strips.shape[4]
    fits = (
        owners & (owners - 1) == 0
        and 2 <= owners <= 16
        and strips.shape[2] == lax.axis_size("row")
        and band == 24
        and cols == 384
        and owners * band == 384
        and wet_mask.shape[1:] == (128, 128)
    )
    run = local_packed if fits else local_general
    return run(strips, anchor, wet_mask, bathy_index, bed_levels, coarse)


def solution(mesh):
    return jax.shard_map(
        local,
        mesh=mesh,
        in_specs=(
            P("nest", None, None, ("row", "col"), None, None),
            P(),
            P("nest", "row", "col"),
            P("nest", "row", "col"),
            P(),
            P(None, ("nest", "row"), "col"),
        ),
        out_specs=(P("nest", None, "row", "col"), P(None, ("nest", "row"), "col")),
        check_vma=False,
    )
```

```python
import jax
import jax.numpy as jnp
from jax import lax
from jax.experimental import pallas as pl
from jax.experimental.pallas import tpu as pltpu
from jax.sharding import PartitionSpec as P


gravity = 1.0
courant = 0.2
F32 = jnp.float32


def padded_2(cells, sides, width):
    for axis, dim in sides:
        count = lax.axis_size(axis)
        ends = count - 1
        head = lax.slice_in_dim(cells, 0, width, axis=dim)
        tail = lax.slice_in_dim(cells, cells.shape[dim] - width, cells.shape[dim], axis=dim)
        cells = jnp.concatenate(
            [
                lax.ppermute(tail, axis, [(i, (i + 1) % count) for i in range(ends)]),
                cells,
                lax.ppermute(head, axis, [((i + 1) % count, i) for i in range(ends)]),
            ],
            axis=dim,
        )
    return cells


def passed_along(block, axis, distance):
    devices = range(lax.axis_size(axis))
    route = [(i - distance, i) for i in devices if i - distance in devices]
    return lax.ppermute(block, axis, route)


def advance(padded, bed_pad, wet_pad):
    depth_now = padded[0]
    flow_u = padded[1]
    flow_v = padded[2]
    depth_safe = jnp.where(wet_pad > 0.5, depth_now, 1.0)
    speed_u = flow_u / depth_safe
    speed_v = flow_v / depth_safe
    celerity = jnp.sqrt(gravity * depth_safe)
    pressure = 0.5 * gravity * depth_safe * depth_safe
    fluxes_x = (flow_u, flow_u * speed_u + pressure, flow_v * speed_u)
    fluxes_y = (flow_v, flow_u * speed_v, flow_v * speed_v + pressure)
    reach_x = jnp.abs(speed_u) + celerity
    reach_y = jnp.abs(speed_v) + celerity
    open_x = wet_pad[1:-1, :-1] * wet_pad[1:-1, 1:]
    open_y = wet_pad[:-1, 1:-1] * wet_pad[1:, 1:-1]
    bound_x = jnp.maximum(reach_x[1:-1, :-1], reach_x[1:-1, 1:])
    bound_y = jnp.maximum(reach_y[:-1, 1:-1], reach_y[1:, 1:-1])
    slope_x = (bed_pad[1:-1, 1:] - bed_pad[1:-1, :-1]) * open_x
    slope_y = (bed_pad[1:, 1:-1] - bed_pad[:-1, 1:-1]) * open_y
    centre = depth_now[1:-1, 1:-1]
    sources = (
        None,
        -0.5 * gravity * centre * (slope_x[:, 1:] + slope_x[:, :-1]),
        -0.5 * gravity * centre * (slope_y[1:] + slope_y[:-1]),
    )
    results = []
    for plane in range(3):
        state = padded[plane]
        flux_col = fluxes_x[plane]
        flux_row = fluxes_y[plane]
        face_x = (
            0.5 * (flux_col[1:-1, :-1] + flux_col[1:-1, 1:])
            - 0.5 * bound_x * (state[1:-1, 1:] - state[1:-1, :-1])
        ) * open_x
        face_y = (
            0.5 * (flux_row[:-1, 1:-1] + flux_row[1:, 1:-1])
            - 0.5 * bound_y * (state[1:, 1:-1] - state[:-1, 1:-1])
        ) * open_y
        value = (
            state[1:-1, 1:-1]
            - courant * (face_x[:, 1:] - face_x[:, :-1])
            - courant * (face_y[1:] - face_y[:-1])
        )
        if plane > 0:
            value = value + courant * sources[plane]
        results.append(value)
    return jnp.stack(results)


def expand(cells):
    return jnp.repeat(jnp.repeat(cells, 3, axis=-2), 3, axis=-1)


def lookup(classes, levels):
    ladder = jnp.arange(levels.shape[0], dtype=jnp.int32)
    matches = classes[None] == ladder[:, None, None]
    return jnp.sum(jnp.where(matches, levels[:, None, None], 0.0), axis=0)


def restrict(updated):
    planes, row_count, col_count = updated.shape
    return updated.reshape(planes, row_count // 3, 3, col_count // 3, 3).sum(axis=(2, 4)) / 9.0


def local_general(strips, anchor, wet_mask, bathy_index, bed_levels, coarse):
    tile_blocks = strips.shape[2]
    band_rows = strips.shape[4]
    full_cols = strips.shape[5]
    columns = lax.axis_size("col")
    tile_cols = full_cols // columns
    layered = (
        strips[0, :, :, 0]
        .reshape(3, tile_blocks, band_rows, columns, tile_cols)
        .transpose(0, 1, 3, 2, 4)
    )
    flattened = layered.reshape(3, tile_blocks * columns, band_rows, tile_cols)
    arrived = lax.all_to_all(flattened, ("row", "col"), split_axis=1, concat_axis=1, tiled=True)
    fields = arrived.reshape(3, tile_blocks * columns * band_rows, tile_cols)
    bed_fine = expand(lookup(bathy_index[0], bed_levels))
    wetness = expand(wet_mask[0].astype(F32))
    stacked = jnp.concatenate([fields, bed_fine[None], wetness[None]], axis=0)
    padded_all = padded_2(stacked, (("row", 1), ("col", 2)), 1)
    updated = advance(padded_all[:3], padded_all[3], padded_all[4])
    restricted = restrict(updated)
    coarse_rows = restricted.shape[1]
    coarse_cols = restricted.shape[2]
    contribution = jnp.concatenate(
        [restricted, jnp.ones((1, coarse_rows, coarse_cols), F32)], axis=0
    )
    nest_index = lax.axis_index("nest")
    corner = lax.dynamic_index_in_dim(anchor, nest_index, 0, keepdims=False)
    canvas = lax.dynamic_update_slice(
        jnp.zeros((4, 2 * coarse_rows, 2 * coarse_cols), F32),
        contribution,
        (jnp.int32(0), corner[0], corner[1]),
    )
    spilled = passed_along(canvas[:, :, coarse_cols:], "col", 1)
    merged = canvas[:, :, :coarse_cols] + spilled
    lowered = passed_along(merged[:, coarse_rows:], ("nest", "row"), 1)
    received_sum = merged[:, :coarse_rows] + lowered
    coarse_next = (coarse + received_sum[:3]) / (1.0 + received_sum[3])
    return (updated[None], coarse_next)


def half_rows(row):
    return pltpu.roll(row, 64, 1), row


def from_half_rows(block, at, lane):
    upper = block[at : at + 1]
    return jnp.where(lane < 64, pltpu.roll(upper, 64, 1), block[at + 1 : at + 2])


def pack_body(dims, ds, strips_hbm, wet_ref, class_ref, *rest):
    blocks, band, columns, lane_blocks = dims
    outs = rest[: len(ds)]
    strips, sems = rest[len(ds) :]
    tile_cols = lane_blocks * 128
    me = lax.axis_index(("row", "col")).astype(jnp.int32)
    my_row = me // columns
    my_col = me % columns
    copies = []
    for r in range(blocks):
        j = my_row ^ (r ^ (ds[0] // columns))
        copies.append(
            pltpu.make_async_copy(strips_hbm.at[0, :, j, 0], strips.at[:, j], sems.at[r])
        )
    for c in copies:
        c.start()
    lane = lax.broadcasted_iota(jnp.int32, (8, 128), 1)
    sub = lax.broadcasted_iota(jnp.int32, (8, 128), 0)
    size = wet_ref.shape[1]
    diag = lax.broadcasted_iota(jnp.int32, (size, 128), 0) == lax.broadcasted_iota(
        jnp.int32, (size, 128), 1
    )
    edges = []
    for ref in (wet_ref, class_ref):
        cells = ref[0].astype(F32)
        north = cells[0:1]
        south = cells[size - 1 : size]
        west = jnp.sum(jnp.where(diag, cells[:, 0:1], 0.0), axis=0, keepdims=True)
        east = jnp.sum(jnp.where(diag, cells[:, 127:128], 0.0), axis=0, keepdims=True)
        edges.append((north, south, west, east))
    first = me == 0
    for c in copies:
        c.wait()
    for out, d in zip(outs, ds):
        to = me ^ d
        j = to // columns
        c = to % columns
        base = pl.multiple_of(c * tile_cols, 128)
        for k in range(3):
            for q in range(lane_blocks):
                at = (k * lane_blocks + q) * band
                out[at : at + band] = strips[k, j, :, pl.ds(pl.multiple_of(base + q * 128, 128), 128)]
        at = 3 * lane_blocks * band
        west_at = pl.multiple_of(jnp.maximum(base - 128, 0), 128)
        east_at = pl.multiple_of(jnp.where(c == columns - 1, base, base + tile_cols), 128)
        mixed = jnp.zeros((8, 128), F32)
        for g in range(band // 8):
            for k in range(3):
                i = g * 3 + k
                west = strips[k, j, g * 8 : g * 8 + 8, pl.ds(west_at, 128)]
                east = strips[k, j, g * 8 : g * 8 + 8, pl.ds(east_at, 128)]
                both = pltpu.roll(jnp.where(lane == 127, west, east), 2 * i + 1, 1)
                mixed = jnp.where((lane == 2 * i) | (lane == 2 * i + 1), both, mixed)
        jj = jnp.clip(jnp.where(first, j + 1, j - 1), 0, blocks - 1)
        rows = []
        for k in range(3):
            for q in range(lane_blocks):
                spot = pl.ds(pl.multiple_of(base + q * 128, 128), 128)
                head = strips[k, jj, 0:8, spot][0:1]
                tail = strips[k, jj, band - 8 : band, spot][7:8]
                rows.append(jnp.where(first, head, tail))
        halo = jnp.zeros((8, 128), F32)
        for i in range(8):
            halo = jnp.where(sub == i, rows[i], halo)
        out[at : at + 8] = halo
        tucked = [rows[8]]
        for north, south, west, east in edges:
            row = jnp.where(
                c == my_col,
                jnp.where(j > my_row, south, north),
                jnp.where(c > my_col, east, west),
            )
            tucked.append(row)
        for n, row in enumerate(tucked):
            low, high = half_rows(row)
            mixed = jnp.where((sub == 2 * n) & (lane >= 64), low, mixed)
            mixed = jnp.where((sub == 2 * n + 1) & (lane >= 64), high, mixed)
        out[at + 8 : at + 16] = mixed


def spread(rows, cols, width, offset=None):
    i = lax.broadcasted_iota(jnp.int32, (rows, cols), 0)
    m = lax.broadcasted_iota(jnp.int32, (rows, cols), 1)
    if offset is not None:
        m = m - offset
        m = jnp.where(m < 0, m + cols, m)
    low = m * width
    return jnp.where((i >= low) & (i < low + width), 1.0, 0.0)


def spread_t(rows, cols, width, offset=None):
    m = lax.broadcasted_iota(jnp.int32, (rows, cols), 0)
    i = lax.broadcasted_iota(jnp.int32, (rows, cols), 1)
    if offset is not None:
        m = m - offset
        m = jnp.where(m < 0, m + rows, m)
    low = m * width
    return jnp.where((i >= low) & (i < low + width), 1.0, 0.0)


def level_of(classes, levels_ref):
    out = jnp.zeros_like(classes)
    for n in range(levels_ref.shape[0]):
        out = jnp.where(classes == n, levels_ref[n], out)
    return out


def prep_body(levels_ref, wet_ref, class_ref, wet_out, bed_out):
    rows, cols = wet_out.shape
    size, width = wet_ref.shape[1], wet_ref.shape[2]
    wet = wet_ref[0].astype(F32)
    bed = level_of(class_ref[0].astype(F32), levels_ref)
    across = spread_t(width, cols, 3)
    down = spread(rows, size, 3)
    wet_out[...] = mul_left(down, mul_right(wet, across, 1), 1)
    bed_out[...] = mul_left(down, mul_right(bed, across, 3), 3)


def split(x, parts):
    out = []
    for n in range(parts):
        piece = x.astype(jnp.bfloat16)
        out.append(piece)
        if n + 1 < parts:
            x = x - piece.astype(F32)
    return out


def mul_left(matrix, x, parts):
    matrix = matrix.astype(jnp.bfloat16)
    return sum(jnp.dot(matrix, piece, preferred_element_type=F32) for piece in split(x, parts))


def mul_right(x, matrix, parts):
    matrix = matrix.astype(jnp.bfloat16)
    return sum(jnp.dot(piece, matrix, preferred_element_type=F32) for piece in split(x, parts))


def mul_left_t(matrix, x, parts):
    matrix = matrix.astype(jnp.bfloat16)
    return sum(
        lax.dot_general(matrix, piece, (((1,), (1,)), ((), ())), preferred_element_type=F32)
        for piece in split(x, parts)
    )


def unpack(dims, me, first_row, messages, ds, field, extra):
    blocks, band, columns, lane_blocks = dims
    cols = lane_blocks * 128
    wide = cols + 128
    body_rows = 3 * lane_blocks * band
    for message, d in zip(messages, ds):
        p = me ^ d
        top = pl.multiple_of(8 + p * band - first_row, 8)
        mixed = message[body_rows + 8 : body_rows + 16]
        for k in range(3):
            for q in range(lane_blocks):
                n = k * lane_blocks + q
                field[k, pl.ds(top, band), q * 128 : q * 128 + 128] = message[
                    n * band : n * band + band
                ]
            for g in range(band // 8):
                i = g * 3 + k
                at = pl.multiple_of(top + g * 8, 8)
                field[k, pl.ds(at, 8), cols:wide] = pltpu.roll(mixed, 127 - 2 * i, 1)
        extra[p] = message[body_rows : body_rows + 16]


def edge_rows(dims, extra, levels_ref, source, inside):
    blocks, band, columns, lane_blocks = dims
    lane = lax.broadcasted_iota(jnp.int32, (1, 128), 1)
    block = extra[jnp.where(inside, source, 0), 8:16]
    wet_row = from_half_rows(block, 2, lane)
    bed_row = level_of(from_half_rows(block, 4, lane), levels_ref)
    return jnp.where(inside, wet_row, 0.0), jnp.where(inside, bed_row, 0.0)


def side_cells(dims, me, first_row, extra, levels_ref, wet, bed, rows):
    blocks, band, columns, lane_blocks = dims
    cols = lane_blocks * 128
    wide = cols + 128
    my_col = me % columns
    west = edge_rows(dims, extra, levels_ref, me - 1, my_col > 0)
    east = edge_rows(dims, extra, levels_ref, me + 1, my_col < columns - 1)
    sub = lax.broadcasted_iota(jnp.int32, (128, 128), 0)
    pair = jnp.zeros((128, 128), F32)
    for n, row in ((0, east[0]), (127, west[0]), (64, east[1]), (63, west[1])):
        pair = jnp.where(sub == n, row, pair)
    i = lax.broadcasted_iota(jnp.int32, (rows, 128), 0) + first_row
    low = lax.broadcasted_iota(jnp.int32, (rows, 128), 1) * 3
    sides = mul_left_t(jnp.where((i >= low) & (i < low + 3), 1.0, 0.0), pair, 3)
    wet[8 : 8 + rows, cols:wide] = sides
    bed[8 : 8 + rows, cols:wide] = pltpu.roll(sides, 64, 1)


def sweep(dims, field, wet, bed, made, start, count, unroll):
    blocks, band, columns, lane_blocks = dims
    cols = lane_blocks * 128
    wide = cols + 128
    sub = lax.broadcasted_iota(jnp.int32, (8, cols), 0)

    def cells(group):
        at = pl.multiple_of(8 + group * 8, 8)
        h = field[0, pl.ds(at, 8)]
        hu = field[1, pl.ds(at, 8)]
        hv = field[2, pl.ds(at, 8)]
        w = wet[pl.ds(at, 8)]
        z = bed[pl.ds(at, 8)]
        hs = jnp.where(w > 0.5, h, 1.0)
        inv = 1.0 / hs
        u = hu * inv
        v = hv * inv
        c = jnp.sqrt(gravity * hs)
        p = 0.5 * gravity * hs * hs
        f2 = hu * u + p
        m = hv * u
        g3 = hv * v + p
        a = jnp.abs(u) + c
        b = jnp.abs(v) + c
        return h, hu, hv, w, z, f2, m, g3, a, b

    def face(near, far, fluxes_near, fluxes_far, reach_near, reach_far):
        h, hu, hv, w, z = near
        h2, hu2, hv2, w2, z2 = far
        opened = w * w2
        half = (0.5 * courant) * opened
        bound = half * jnp.maximum(reach_near, reach_far)
        out = []
        for f, f2, s, s2 in zip(fluxes_near, fluxes_far, (h, hu, hv), (h2, hu2, hv2)):
            out.append(half * (f + f2) - bound * (s2 - s))
        out.append(half * (z2 - z))
        return out

    def south_face(now, nxt):
        def pick(i):
            a = now[i][:, :cols]
            b = nxt[i][:, :cols]
            return pltpu.roll(jnp.where(sub == 0, b, a), 7, 0)

        h, hu, hv, w, z, f2, m, g3, a, b = [x[:, :cols] for x in now]
        h2, hu2, hv2, w2, z2, m2, g32, b2 = [pick(i) for i in (0, 1, 2, 3, 4, 6, 7, 9)]
        return face(
            (h, hu, hv, w, z), (h2, hu2, hv2, w2, z2), (hv, m, g3), (hv2, m2, g32), b, b2
        )

    def step(t, carry):
        now, above = carry
        group = start + t
        nxt = cells(group + 1)
        below = south_face(now, nxt)
        h, hu, hv, w, z, f2, m, g3, a, b = now
        r = [pltpu.roll(x, wide - 1, 1) for x in (h, hu, hv, w, z, f2, m, a)]
        fx = face((h, hu, hv, w, z), tuple(r[:5]), (hu, f2, m), (r[1], r[5], r[6]), a, r[7])
        left = [pltpu.roll(x, 1, 1)[:, :cols] for x in fx]
        right = [x[:, :cols] for x in fx]
        up = [pltpu.roll(jnp.where(sub == 7, y, x), 1, 0) for x, y in zip(below, above)]
        hc = gravity * h[:, :cols]
        o0 = h[:, :cols] - (right[0] - left[0]) - (below[0] - up[0])
        o1 = hu[:, :cols] - (right[1] - left[1]) - (below[1] - up[1]) - hc * (right[3] + left[3])
        o2 = hv[:, :cols] - (right[2] - left[2]) - (below[2] - up[2]) - hc * (below[3] + up[3])
        spot = pl.ds(pl.multiple_of(group * 8, 8), 8)
        for k, o in enumerate((o0, o1, o2)):
            for q in range(lane_blocks):
                made[k, q, spot] = o[:, q * 128 : q * 128 + 128]
        return nxt, below

    now = cells(start)
    carry = (now, south_face(cells(start - 1), now))
    if count == 1:
        step(0, carry)
    else:
        lax.fori_loop(0, count, step, carry, unroll=unroll)


def half_body(dims, ds, where_ref, levels_ref, wet_in, bed_in, *rest):
    blocks, band, columns, lane_blocks = dims
    owners = blocks * columns
    messages = rest[: len(ds)]
    made, field, wet, bed, extra = rest[len(ds) :]
    rows = owners * band // 2
    me = where_ref[0]
    first_row = pl.multiple_of((me * 2 // owners) * rows, 8)
    wet[8 : 8 + rows] = wet_in[pl.ds(first_row, rows)]
    bed[8 : 8 + rows] = bed_in[pl.ds(first_row, rows)]
    unpack(dims, me, first_row, messages, ds, field, extra)
    side_cells(dims, me, first_row, extra, levels_ref, wet, bed, rows)
    for k in range(3):
        for q in range(lane_blocks):
            made[k, q, 0:8] = jnp.zeros((8, 128), F32)
            made[k, q, rows - 8 : rows] = jnp.zeros((8, 128), F32)
    sweep(dims, field, wet, bed, made, 1, rows // 8 - 2, 2)


def main_body(dims, ds, where_ref, anchor_ref, levels_ref, wet_in, bed_in, half_in, *rest):
    blocks, band, columns, lane_blocks = dims
    owners = blocks * columns
    messages = rest[:owners]
    fine_out, rolled_out = rest[owners : owners + 2]
    field, wet, bed, extra, made, sem_in, sem_out = rest[owners + 2 :]
    rows = owners * band
    cols = lane_blocks * 128
    wide = cols + 128
    me = where_ref[0]
    nest = where_ref[1]
    my_row = me // columns
    done_half = me * 2 // owners
    early = pltpu.make_async_copy(
        half_in, made.at[:, :, pl.ds(pl.multiple_of(done_half * (rows // 2), 8), rows // 2)], sem_in
    )
    early.start()
    lane1 = lax.broadcasted_iota(jnp.int32, (1, 128), 1)
    wet[8 : 8 + rows] = wet_in[...]
    bed[8 : 8 + rows] = bed_in[...]
    unpack(dims, me, 0, messages, ds, field, extra)

    for source, at in ((owners - 1, 0), (0, 8 + rows)):
        last = from_half_rows(extra[source, 8:16], 0, lane1)
        for k in range(3):
            for q in range(lane_blocks):
                n = k * lane_blocks + q
                row = last if n == 8 else extra[source, n : n + 1]
                field[k, at : at + 8, q * 128 : q * 128 + 128] = jnp.broadcast_to(row, (8, 128))
            field[k, at : at + 8, cols:wide] = jnp.zeros((8, 128), F32)
    north = edge_rows(dims, extra, levels_ref, me - columns, my_row > 0)
    south = edge_rows(dims, extra, levels_ref, me + columns, my_row < blocks - 1)
    sub8 = lax.broadcasted_iota(jnp.int32, (8, 128), 0)
    stack = jnp.zeros((8, 128), F32)
    for n, row in enumerate((north[0], north[1], south[0], south[1])):
        stack = jnp.where(sub8 == n, row, stack)
    ends = mul_right(stack, spread_t(128, wide, 3), 3)
    for n, (ref, at) in enumerate(((wet, 0), (bed, 0), (wet, 8 + rows), (bed, 8 + rows))):
        ref[at : at + 8] = jnp.broadcast_to(ends[n : n + 1], (8, wide))
    side_cells(dims, me, 0, extra, levels_ref, wet, bed, rows)

    groups = rows // 8
    early.wait()
    sweep(dims, field, wet, bed, made, (1 - done_half) * (groups // 2 - 1), groups // 2 + 1, 5)
    sweep(dims, field, wet, bed, made, done_half * (groups - 1), 1, 1)

    done = [
        pltpu.make_async_copy(
            made.at[:, q], fine_out.at[0, :, :, pl.ds(q * 128, 128)], sem_out.at[q]
        )
        for q in range(lane_blocks)
    ]
    for c in done:
        c.start()
    coarse_rows = rows // 3
    coarse_cols = cols // 3
    a0 = anchor_ref[nest, 0]
    a1 = anchor_ref[nest, 1]
    gather_cols = spread(cols, coarse_cols, 3, a1)
    for k in range(3):
        total = jnp.concatenate(
            [
                sum(made[k, q, pl.ds(n, coarse_rows, stride=3), :] for n in range(3))
                for q in range(lane_blocks)
            ],
            axis=1,
        )
        mean = mul_right(total, gather_cols, 2) * (1.0 / 9.0)
        rolled_out[k] = pltpu.roll(mean, a0, 0)
    for c in done:
        c.wait()


SMEM = pl.BlockSpec(memory_space=pltpu.SMEM)
VMEM = pl.BlockSpec(memory_space=pltpu.VMEM)
HBM = pl.BlockSpec(memory_space=pl.ANY)


def half_call(dims, ds, spot, bed_levels, wet_fine, bed_fine, messages):
    blocks, band, columns, lane_blocks = dims
    owners = blocks * columns
    rows = owners * band // 2
    wide = lane_blocks * 128 + 128
    return pl.pallas_call(
        lambda *refs: half_body(dims, ds, *refs),
        in_specs=[SMEM, SMEM, VMEM, VMEM] + [VMEM] * len(ds),
        out_specs=VMEM,
        out_shape=jax.ShapeDtypeStruct((3, lane_blocks, rows, 128), F32),
        scratch_shapes=[
            pltpu.VMEM((3, rows + 16, wide), F32),
            pltpu.VMEM((rows + 16, wide), F32),
            pltpu.VMEM((rows + 16, wide), F32),
            pltpu.VMEM((owners, 16, 128), F32),
        ],
        name="half",
    )(spot, bed_levels, wet_fine, bed_fine, *messages)


def main_call(dims, ds, spot, anchor, bed_levels, wet_fine, bed_fine, half, messages):
    blocks, band, columns, lane_blocks = dims
    owners = blocks * columns
    rows = owners * band
    cols = lane_blocks * 128
    wide = cols + 128
    return pl.pallas_call(
        lambda *refs: main_body(dims, ds, *refs),
        in_specs=[SMEM, SMEM, SMEM, VMEM, VMEM, HBM] + [VMEM] * owners,
        out_specs=[HBM, VMEM],
        out_shape=[
            jax.ShapeDtypeStruct((1, 3, rows, cols), F32),
            jax.ShapeDtypeStruct((3, rows // 3, cols // 3), F32),
        ],
        scratch_shapes=[
            pltpu.VMEM((3, rows + 16, wide), F32),
            pltpu.VMEM((rows + 16, wide), F32),
            pltpu.VMEM((rows + 16, wide), F32),
            pltpu.VMEM((owners, 16, 128), F32),
            pltpu.VMEM((3, lane_blocks, rows, 128), F32),
            pltpu.SemaphoreType.DMA,
            pltpu.SemaphoreType.DMA((lane_blocks,)),
        ],
        name="main",
    )(spot, anchor, bed_levels, wet_fine, bed_fine, half, *messages)


def local_packed(strips, anchor, wet_mask, bathy_index, bed_levels, coarse):
    blocks, band, full_cols = strips.shape[2], strips.shape[4], strips.shape[5]
    columns = lax.axis_size("col")
    owners = blocks * columns
    cols = full_cols // columns
    lane_blocks = cols // 128
    rows = owners * band
    wide = cols + 128
    dims = (blocks, band, columns, lane_blocks)
    height = 3 * lane_blocks * band + 16
    me = lax.axis_index(("row", "col")).astype(jnp.int32)
    nest = lax.axis_index("nest").astype(jnp.int32)
    spot = jnp.stack([me, nest])
    half_owners = owners // 2
    messages = []
    for ds in (range(half_owners), range(half_owners, owners)):
        messages += pl.pallas_call(
            lambda *refs, ds=ds: pack_body(dims, ds, *refs),
            in_specs=[HBM, VMEM, VMEM],
            out_specs=[VMEM] * half_owners,
            out_shape=[jax.ShapeDtypeStruct((height, 128), F32)] * half_owners,
            scratch_shapes=[
                pltpu.VMEM((3, blocks, band, full_cols), F32),
                pltpu.SemaphoreType.DMA((blocks,)),
            ],
            name="pack",
        )(strips, wet_mask, bathy_index)

    def rank(d):
        r, c = d // columns, d % columns
        return (d >= half_owners, c * 2 < columns, r, c)

    wanted = sorted(range(1, owners), key=rank)
    arrived = {
        d: lax.ppermute(messages[d], ("row", "col"), [(i, i ^ d) for i in range(owners)])
        for d in wanted
    }
    arrived[0] = messages[0]
    arrived = {d: pltpu.with_memory_space_constraint(x, pltpu.VMEM) for d, x in arrived.items()}

    wet_fine, bed_fine = pl.pallas_call(
        prep_body,
        in_specs=[SMEM, VMEM, VMEM],
        out_specs=[VMEM, VMEM],
        out_shape=[jax.ShapeDtypeStruct((rows, wide), F32)] * 2,
        name="prep",
    )(bed_levels, wet_mask, bathy_index)

    coarse_rows = rows // 3
    coarse_cols = cols // 3
    turns = sorted(range(half_owners - 1, owners - 1), key=str)
    late = [0] * half_owners
    for turn, d in zip(turns, wanted[half_owners - 1 :]):
        late[turn - half_owners + 1] = d
    early = [0] + wanted[: half_owners - 1]
    order = early + late
    half = half_call(
        dims, early, spot, bed_levels, wet_fine, bed_fine, [arrived[d] for d in early]
    )
    fine, rolled = main_call(
        dims,
        order,
        spot,
        anchor,
        bed_levels,
        wet_fine,
        bed_fine,
        half,
        [arrived[d] for d in order],
    )

    lines = lax.axis_size("nest") * lax.axis_size("row")
    rights = [(c, c + 1) for c in range(columns - 1)]
    downs = [(l, l + 1) for l in range(lines - 1)]
    both = [(l * columns + c, l2 * columns + c2) for l, l2 in downs for c, c2 in rights]
    diagonal = lax.ppermute(rolled, ("nest", "row", "col"), both)
    from_left = lax.ppermute(rolled, "col", rights)
    from_up = lax.ppermute(rolled, ("nest", "row"), downs)

    row_at = lax.axis_index("row")
    col_at = lax.axis_index("col")
    mine = anchor[nest]
    up_nest = jnp.where(row_at == 0, jnp.maximum(nest - 1, 0), nest)
    theirs = anchor[up_nest]
    has_left = col_at > 0
    has_up = (row_at > 0) | (nest > 0)
    i = lax.broadcasted_iota(jnp.int32, (coarse_rows, coarse_cols), 0)
    m = lax.broadcasted_iota(jnp.int32, (coarse_rows, coarse_cols), 1)
    own_rows = i >= mine[0]
    up_rows = (i < theirs[0]) & has_up
    own = jnp.where(own_rows, jnp.where(m >= mine[1], rolled, from_left), 0.0)
    upper = jnp.where(up_rows, jnp.where(m >= theirs[1], from_up, diagonal), 0.0)
    count = (
        1.0
        + jnp.where(own_rows & ((m >= mine[1]) | has_left), 1.0, 0.0)
        + jnp.where(up_rows & ((m >= theirs[1]) | has_left), 1.0, 0.0)
    )
    coarse_next = (coarse + own + upper) / count
    return (fine, coarse_next)


def local(strips, anchor, wet_mask, bathy_index, bed_levels, coarse):
    columns = lax.axis_size("col")
    owners = strips.shape[2] * columns
    cols = strips.shape[5] // columns
    band = strips.shape[4]
    fits = (
        owners & (owners - 1) == 0
        and 2 <= owners <= 16
        and strips.shape[2] == lax.axis_size("row")
        and band == 24
        and cols == 384
        and owners * band == 384
        and wet_mask.shape[1:] == (128, 128)
    )
    run = local_packed if fits else local_general
    return run(strips, anchor, wet_mask, bathy_index, bed_levels, coarse)


def solution(mesh):
    return jax.shard_map(
        local,
        mesh=mesh,
        in_specs=(
            P("nest", None, None, ("row", "col"), None, None),
            P(),
            P("nest", "row", "col"),
            P("nest", "row", "col"),
            P(),
            P(None, ("nest", "row"), "col"),
        ),
        out_specs=(P("nest", None, "row", "col"), P(None, ("nest", "row"), "col")),
        check_vma=False,
    )
```

```python
import jax
import jax.numpy as jnp
from jax import lax
from jax.experimental import pallas as pl
from jax.experimental.pallas import tpu as pltpu
from jax.sharding import PartitionSpec as P


gravity = 1.0
courant = 0.2
F32 = jnp.float32


def padded_2(cells, sides, width):
    for axis, dim in sides:
        count = lax.axis_size(axis)
        ends = count - 1
        head = lax.slice_in_dim(cells, 0, width, axis=dim)
        tail = lax.slice_in_dim(cells, cells.shape[dim] - width, cells.shape[dim], axis=dim)
        cells = jnp.concatenate(
            [
                lax.ppermute(tail, axis, [(i, (i + 1) % count) for i in range(ends)]),
                cells,
                lax.ppermute(head, axis, [((i + 1) % count, i) for i in range(ends)]),
            ],
            axis=dim,
        )
    return cells


def passed_along(block, axis, distance):
    devices = range(lax.axis_size(axis))
    route = [(i - distance, i) for i in devices if i - distance in devices]
    return lax.ppermute(block, axis, route)


def advance(padded, bed_pad, wet_pad):
    depth_now = padded[0]
    flow_u = padded[1]
    flow_v = padded[2]
    depth_safe = jnp.where(wet_pad > 0.5, depth_now, 1.0)
    speed_u = flow_u / depth_safe
    speed_v = flow_v / depth_safe
    celerity = jnp.sqrt(gravity * depth_safe)
    pressure = 0.5 * gravity * depth_safe * depth_safe
    fluxes_x = (flow_u, flow_u * speed_u + pressure, flow_v * speed_u)
    fluxes_y = (flow_v, flow_u * speed_v, flow_v * speed_v + pressure)
    reach_x = jnp.abs(speed_u) + celerity
    reach_y = jnp.abs(speed_v) + celerity
    open_x = wet_pad[1:-1, :-1] * wet_pad[1:-1, 1:]
    open_y = wet_pad[:-1, 1:-1] * wet_pad[1:, 1:-1]
    bound_x = jnp.maximum(reach_x[1:-1, :-1], reach_x[1:-1, 1:])
    bound_y = jnp.maximum(reach_y[:-1, 1:-1], reach_y[1:, 1:-1])
    slope_x = (bed_pad[1:-1, 1:] - bed_pad[1:-1, :-1]) * open_x
    slope_y = (bed_pad[1:, 1:-1] - bed_pad[:-1, 1:-1]) * open_y
    centre = depth_now[1:-1, 1:-1]
    sources = (
        None,
        -0.5 * gravity * centre * (slope_x[:, 1:] + slope_x[:, :-1]),
        -0.5 * gravity * centre * (slope_y[1:] + slope_y[:-1]),
    )
    results = []
    for plane in range(3):
        state = padded[plane]
        flux_col = fluxes_x[plane]
        flux_row = fluxes_y[plane]
        face_x = (
            0.5 * (flux_col[1:-1, :-1] + flux_col[1:-1, 1:])
            - 0.5 * bound_x * (state[1:-1, 1:] - state[1:-1, :-1])
        ) * open_x
        face_y = (
            0.5 * (flux_row[:-1, 1:-1] + flux_row[1:, 1:-1])
            - 0.5 * bound_y * (state[1:, 1:-1] - state[:-1, 1:-1])
        ) * open_y
        value = (
            state[1:-1, 1:-1]
            - courant * (face_x[:, 1:] - face_x[:, :-1])
            - courant * (face_y[1:] - face_y[:-1])
        )
        if plane > 0:
            value = value + courant * sources[plane]
        results.append(value)
    return jnp.stack(results)


def expand(cells):
    return jnp.repeat(jnp.repeat(cells, 3, axis=-2), 3, axis=-1)


def lookup(classes, levels):
    ladder = jnp.arange(levels.shape[0], dtype=jnp.int32)
    matches = classes[None] == ladder[:, None, None]
    return jnp.sum(jnp.where(matches, levels[:, None, None], 0.0), axis=0)


def restrict(updated):
    planes, row_count, col_count = updated.shape
    return updated.reshape(planes, row_count // 3, 3, col_count // 3, 3).sum(axis=(2, 4)) / 9.0


def local_general(strips, anchor, wet_mask, bathy_index, bed_levels, coarse):
    tile_blocks = strips.shape[2]
    band_rows = strips.shape[4]
    full_cols = strips.shape[5]
    columns = lax.axis_size("col")
    tile_cols = full_cols // columns
    layered = (
        strips[0, :, :, 0]
        .reshape(3, tile_blocks, band_rows, columns, tile_cols)
        .transpose(0, 1, 3, 2, 4)
    )
    flattened = layered.reshape(3, tile_blocks * columns, band_rows, tile_cols)
    arrived = lax.all_to_all(flattened, ("row", "col"), split_axis=1, concat_axis=1, tiled=True)
    fields = arrived.reshape(3, tile_blocks * columns * band_rows, tile_cols)
    bed_fine = expand(lookup(bathy_index[0], bed_levels))
    wetness = expand(wet_mask[0].astype(F32))
    stacked = jnp.concatenate([fields, bed_fine[None], wetness[None]], axis=0)
    padded_all = padded_2(stacked, (("row", 1), ("col", 2)), 1)
    updated = advance(padded_all[:3], padded_all[3], padded_all[4])
    restricted = restrict(updated)
    coarse_rows = restricted.shape[1]
    coarse_cols = restricted.shape[2]
    contribution = jnp.concatenate(
        [restricted, jnp.ones((1, coarse_rows, coarse_cols), F32)], axis=0
    )
    nest_index = lax.axis_index("nest")
    corner = lax.dynamic_index_in_dim(anchor, nest_index, 0, keepdims=False)
    canvas = lax.dynamic_update_slice(
        jnp.zeros((4, 2 * coarse_rows, 2 * coarse_cols), F32),
        contribution,
        (jnp.int32(0), corner[0], corner[1]),
    )
    spilled = passed_along(canvas[:, :, coarse_cols:], "col", 1)
    merged = canvas[:, :, :coarse_cols] + spilled
    lowered = passed_along(merged[:, coarse_rows:], ("nest", "row"), 1)
    received_sum = merged[:, :coarse_rows] + lowered
    coarse_next = (coarse + received_sum[:3]) / (1.0 + received_sum[3])
    return (updated[None], coarse_next)


def half_rows(row):
    return pltpu.roll(row, 64, 1), row


def from_half_rows(block, at, lane):
    upper = block[at : at + 1]
    return jnp.where(lane < 64, pltpu.roll(upper, 64, 1), block[at + 1 : at + 2])


def pack_body(dims, ds, after, strips_hbm, wet_hbm, class_hbm, levels_hbm, *rest):
    blocks, band, columns, lane_blocks = dims
    rest = rest[after:]
    outs = rest[: len(ds)]
    strips, wet_ref, class_ref, levels_ref, sems, small = rest[len(ds) :]
    tile_cols = lane_blocks * 128
    me = lax.axis_index(("row", "col")).astype(jnp.int32)
    my_row = me // columns
    my_col = me % columns
    loads = [
        pltpu.make_async_copy(wet_hbm, wet_ref, small.at[0]),
        pltpu.make_async_copy(class_hbm, class_ref, small.at[1]),
        pltpu.make_async_copy(levels_hbm, levels_ref, small.at[2]),
    ]
    for c in loads:
        c.start()
    copies = []
    for r in range(blocks):
        j = my_row ^ (r ^ (ds[0] // columns))
        copies.append(
            pltpu.make_async_copy(strips_hbm.at[0, :, j, 0], strips.at[:, j], sems.at[r])
        )
    for c in copies:
        c.start()
    lane = lax.broadcasted_iota(jnp.int32, (8, 128), 1)
    sub = lax.broadcasted_iota(jnp.int32, (8, 128), 0)
    size = wet_ref.shape[1]
    diag = lax.broadcasted_iota(jnp.int32, (size, 128), 0) == lax.broadcasted_iota(
        jnp.int32, (size, 128), 1
    )
    for c in loads:
        c.wait()
    edges = []
    for ref in (wet_ref, class_ref):
        cells = ref[0].astype(F32)
        north = cells[0:1]
        south = cells[size - 1 : size]
        west = jnp.sum(jnp.where(diag, cells[:, 0:1], 0.0), axis=0, keepdims=True)
        east = jnp.sum(jnp.where(diag, cells[:, 127:128], 0.0), axis=0, keepdims=True)
        four = (north, south, west, east)
        if ref is class_ref:
            four = tuple(level_of(row, levels_ref) for row in four)
        edges.append(four)
    first = me == 0
    for c in copies:
        c.wait()
    for out, d in zip(outs, ds):
        to = me ^ d
        j = to // columns
        c = to % columns
        base = pl.multiple_of(c * tile_cols, 128)
        for k in range(3):
            for q in range(lane_blocks):
                at = (k * lane_blocks + q) * band
                out[at : at + band] = strips[k, j, :, pl.ds(pl.multiple_of(base + q * 128, 128), 128)]
        at = 3 * lane_blocks * band
        west_at = pl.multiple_of(jnp.maximum(base - 128, 0), 128)
        east_at = pl.multiple_of(jnp.where(c == columns - 1, base, base + tile_cols), 128)
        mixed = jnp.zeros((8, 128), F32)
        for g in range(band // 8):
            for k in range(3):
                i = g * 3 + k
                west = strips[k, j, g * 8 : g * 8 + 8, pl.ds(west_at, 128)]
                east = strips[k, j, g * 8 : g * 8 + 8, pl.ds(east_at, 128)]
                both = pltpu.roll(jnp.where(lane == 127, west, east), 2 * i + 1, 1)
                mixed = jnp.where((lane == 2 * i) | (lane == 2 * i + 1), both, mixed)
        jj = jnp.clip(jnp.where(first, j + 1, j - 1), 0, blocks - 1)
        rows = []
        for k in range(3):
            for q in range(lane_blocks):
                spot = pl.ds(pl.multiple_of(base + q * 128, 128), 128)
                head = strips[k, jj, 0:8, spot][0:1]
                tail = strips[k, jj, band - 8 : band, spot][7:8]
                rows.append(jnp.where(first, head, tail))
        halo = jnp.zeros((8, 128), F32)
        for i in range(8):
            halo = jnp.where(sub == i, rows[i], halo)
        out[at : at + 8] = halo
        tucked = [rows[8]]
        for north, south, west, east in edges:
            row = jnp.where(
                c == my_col,
                jnp.where(j > my_row, south, north),
                jnp.where(c > my_col, east, west),
            )
            tucked.append(row)
        for n, row in enumerate(tucked):
            low, high = half_rows(row)
            mixed = jnp.where((sub == 2 * n) & (lane >= 64), low, mixed)
            mixed = jnp.where((sub == 2 * n + 1) & (lane >= 64), high, mixed)
        out[at + 8 : at + 16] = mixed


def spread(rows, cols, width, offset=None):
    i = lax.broadcasted_iota(jnp.int32, (rows, cols), 0)
    m = lax.broadcasted_iota(jnp.int32, (rows, cols), 1)
    if offset is not None:
        m = m - offset
        m = jnp.where(m < 0, m + cols, m)
    low = m * width
    return jnp.where((i >= low) & (i < low + width), 1.0, 0.0)


def spread_t(rows, cols, width, offset=None):
    m = lax.broadcasted_iota(jnp.int32, (rows, cols), 0)
    i = lax.broadcasted_iota(jnp.int32, (rows, cols), 1)
    if offset is not None:
        m = m - offset
        m = jnp.where(m < 0, m + rows, m)
    low = m * width
    return jnp.where((i >= low) & (i < low + width), 1.0, 0.0)


def level_of(classes, levels_ref):
    out = jnp.zeros_like(classes)
    for n in range(levels_ref.shape[0]):
        out = jnp.where(classes == n, levels_ref[n], out)
    return out


def prep_body(columns, levels_ref, anchor_ref, wet_ref, class_ref, wet_out, bed_out, weights):
    rows, cols = wet_out.shape
    size, width = wet_ref.shape[1], wet_ref.shape[2]
    wet = wet_ref[0].astype(F32)
    bed = level_of(class_ref[0].astype(F32), levels_ref)
    across = spread_t(width, cols, 3)
    down = spread(rows, size, 3)
    wet_out[...] = mul_left(down, mul_right(wet, across, 1), 1)
    bed_out[...] = mul_left(down, mul_right(bed, across, 3), 3)
    nest = lax.axis_index("nest").astype(jnp.int32)
    row_at = lax.axis_index("row").astype(jnp.int32)
    col_at = lax.axis_index("col").astype(jnp.int32)
    up_nest = jnp.where(row_at == 0, jnp.maximum(nest - 1, 0), nest)
    i = lax.broadcasted_iota(jnp.int32, weights.shape[1:], 0)
    m = lax.broadcasted_iota(jnp.int32, weights.shape[1:], 1)
    has_left = jnp.where(col_at > 0, 1.0, 0.0)
    has_up = jnp.where((row_at > 0) | (nest > 0), 1.0, 0.0)
    own_rows = jnp.where(i >= anchor_ref[nest, 0], 1.0, 0.0)
    up_rows = jnp.where(i < anchor_ref[up_nest, 0], has_up, 0.0)
    own_cols = m >= anchor_ref[nest, 1]
    up_cols = m >= anchor_ref[up_nest, 1]
    shares = (
        jnp.where(own_cols, own_rows, 0.0),
        jnp.where(own_cols, 0.0, own_rows * has_left),
        jnp.where(up_cols, up_rows, 0.0),
        jnp.where(up_cols, 0.0, up_rows * has_left),
    )
    scale = 1.0 / (1.0 + shares[0] + shares[1] + shares[2] + shares[3])
    weights[0] = scale
    for n, share in enumerate(shares):
        weights[n + 1] = share * scale


def split(x, parts):
    out = []
    for n in range(parts):
        piece = x.astype(jnp.bfloat16)
        out.append(piece)
        if n + 1 < parts:
            x = x - piece.astype(F32)
    return out


def mul_left(matrix, x, parts):
    matrix = matrix.astype(jnp.bfloat16)
    return sum(jnp.dot(matrix, piece, preferred_element_type=F32) for piece in split(x, parts))


def mul_right(x, matrix, parts):
    matrix = matrix.astype(jnp.bfloat16)
    return sum(jnp.dot(piece, matrix, preferred_element_type=F32) for piece in split(x, parts))


def mul_left_t(matrix, x, parts):
    matrix = matrix.astype(jnp.bfloat16)
    return sum(
        lax.dot_general(matrix, piece, (((1,), (1,)), ((), ())), preferred_element_type=F32)
        for piece in split(x, parts)
    )


def unpack(dims, me, first_row, messages, ds, field, extra):
    blocks, band, columns, lane_blocks = dims
    cols = lane_blocks * 128
    wide = cols + 128
    body_rows = 3 * lane_blocks * band
    for message, d in zip(messages, ds):
        p = me ^ d
        top = pl.multiple_of(8 + p * band - first_row, 8)
        mixed = message[body_rows + 8 : body_rows + 16]
        for k in range(3):
            for q in range(lane_blocks):
                n = k * lane_blocks + q
                field[k, pl.ds(top, band), q * 128 : q * 128 + 128] = message[
                    n * band : n * band + band
                ]
            for g in range(band // 8):
                i = g * 3 + k
                at = pl.multiple_of(top + g * 8, 8)
                field[k, pl.ds(at, 8), cols:wide] = pltpu.roll(mixed, 127 - 2 * i, 1)
        extra[p] = message[body_rows : body_rows + 16]


def edge_rows(dims, extra, source, inside):
    blocks, band, columns, lane_blocks = dims
    lane = lax.broadcasted_iota(jnp.int32, (1, 128), 1)
    block = extra[jnp.where(inside, source, 0), 8:16]
    wet_row = from_half_rows(block, 2, lane)
    bed_row = from_half_rows(block, 4, lane)
    return jnp.where(inside, wet_row, 0.0), jnp.where(inside, bed_row, 0.0)


def side_cells(dims, me, first_row, extra, wet, bed, rows):
    blocks, band, columns, lane_blocks = dims
    cols = lane_blocks * 128
    wide = cols + 128
    my_col = me % columns
    west = edge_rows(dims, extra, me - 1, my_col > 0)
    east = edge_rows(dims, extra, me + 1, my_col < columns - 1)
    sub = lax.broadcasted_iota(jnp.int32, (128, 128), 0)
    pair = jnp.zeros((128, 128), F32)
    for n, row in ((0, east[0]), (127, west[0]), (64, east[1]), (63, west[1])):
        pair = jnp.where(sub == n, row, pair)
    i = lax.broadcasted_iota(jnp.int32, (rows, 128), 0) + first_row
    low = lax.broadcasted_iota(jnp.int32, (rows, 128), 1) * 3
    sides = mul_left_t(jnp.where((i >= low) & (i < low + 3), 1.0, 0.0), pair, 3)
    wet[8 : 8 + rows, cols:wide] = sides
    bed[8 : 8 + rows, cols:wide] = pltpu.roll(sides, 64, 1)


def sweep(dims, field, wet, bed, made, start, count, unroll):
    blocks, band, columns, lane_blocks = dims
    cols = lane_blocks * 128
    wide = cols + 128
    sub = lax.broadcasted_iota(jnp.int32, (8, cols), 0)

    def cells(group):
        at = pl.multiple_of(8 + group * 8, 8)
        h = field[0, pl.ds(at, 8)]
        hu = field[1, pl.ds(at, 8)]
        hv = field[2, pl.ds(at, 8)]
        w = wet[pl.ds(at, 8)]
        z = bed[pl.ds(at, 8)]
        hs = jnp.where(w > 0.5, h, 1.0)
        root = lax.rsqrt(hs)
        inv = root * root
        u = hu * inv
        v = hv * inv
        c = (gravity**0.5) * (hs * root)
        p = 0.5 * gravity * hs * hs
        f2 = hu * u + p
        m = hv * u
        g3 = hv * v + p
        a = jnp.abs(u) + c
        b = jnp.abs(v) + c
        return h, hu, hv, w, z, f2, m, g3, a, b

    def face(near, far, fluxes_near, fluxes_far, reach_near, reach_far):
        h, hu, hv, w, z = near
        h2, hu2, hv2, w2, z2 = far
        opened = w * w2
        half = (0.5 * courant) * opened
        bound = half * jnp.maximum(reach_near, reach_far)
        out = []
        for f, f2, s, s2 in zip(fluxes_near, fluxes_far, (h, hu, hv), (h2, hu2, hv2)):
            out.append(half * (f + f2) - bound * (s2 - s))
        out.append(half * (z2 - z))
        return out

    def south_face(now, nxt):
        def pick(i):
            a = now[i][:, :cols]
            b = nxt[i][:, :cols]
            return pltpu.roll(jnp.where(sub == 0, b, a), 7, 0)

        h, hu, hv, w, z, f2, m, g3, a, b = [x[:, :cols] for x in now]
        h2, hu2, hv2, w2, z2, m2, g32, b2 = [pick(i) for i in (0, 1, 2, 3, 4, 6, 7, 9)]
        return face(
            (h, hu, hv, w, z), (h2, hu2, hv2, w2, z2), (hv, m, g3), (hv2, m2, g32), b, b2
        )

    def step(t, carry):
        now, above = carry
        group = start + t
        nxt = cells(group + 1)
        below = south_face(now, nxt)
        h, hu, hv, w, z, f2, m, g3, a, b = now
        r = [pltpu.roll(x, wide - 1, 1) for x in (h, hu, hv, w, z, f2, m, a)]
        fx = face((h, hu, hv, w, z), tuple(r[:5]), (hu, f2, m), (r[1], r[5], r[6]), a, r[7])
        left = [pltpu.roll(x, 1, 1)[:, :cols] for x in fx]
        right = [x[:, :cols] for x in fx]
        up = [pltpu.roll(jnp.where(sub == 7, y, x), 1, 0) for x, y in zip(below, above)]
        hc = gravity * h[:, :cols]
        o0 = h[:, :cols] - (right[0] - left[0]) - (below[0] - up[0])
        o1 = hu[:, :cols] - (right[1] - left[1]) - (below[1] - up[1]) - hc * (right[3] + left[3])
        o2 = hv[:, :cols] - (right[2] - left[2]) - (below[2] - up[2]) - hc * (below[3] + up[3])
        spot = pl.ds(pl.multiple_of(group * 8, 8), 8)
        for k, o in enumerate((o0, o1, o2)):
            for q in range(lane_blocks):
                made[k, q, spot] = o[:, q * 128 : q * 128 + 128]
        return nxt, below

    now = cells(start)
    carry = (now, south_face(cells(start - 1), now))
    if count == 1:
        step(0, carry)
    else:
        lax.fori_loop(0, count, step, carry, unroll=unroll)


def half_body(dims, ds, wet_in, bed_in, *rest):
    blocks, band, columns, lane_blocks = dims
    owners = blocks * columns
    messages = rest[: len(ds)]
    made, field, wet, bed, extra = rest[len(ds) :]
    rows = owners * band // 2
    me = lax.axis_index(("row", "col")).astype(jnp.int32)
    first_row = pl.multiple_of((me * 2 // owners) * rows, 8)
    wet[8 : 8 + rows] = wet_in[pl.ds(first_row, rows)]
    bed[8 : 8 + rows] = bed_in[pl.ds(first_row, rows)]
    unpack(dims, me, first_row, messages, ds, field, extra)
    side_cells(dims, me, first_row, extra, wet, bed, rows)
    for k in range(3):
        for q in range(lane_blocks):
            made[k, q, 0:8] = jnp.zeros((8, 128), F32)
            made[k, q, rows - 8 : rows] = jnp.zeros((8, 128), F32)
    sweep(dims, field, wet, bed, made, 1, rows // 8 - 2, 2)


def main_body(dims, ds, anchor_hbm, wet_in, bed_in, half_in, *rest):
    blocks, band, columns, lane_blocks = dims
    owners = blocks * columns
    messages = rest[:owners]
    fine_out, rolled_out = rest[owners : owners + 2]
    field, wet, bed, extra, made, anchor_ref, sem_in, sem_out = rest[owners + 2 :]
    rows = owners * band
    cols = lane_blocks * 128
    wide = cols + 128
    me = lax.axis_index(("row", "col")).astype(jnp.int32)
    nest = lax.axis_index("nest").astype(jnp.int32)
    my_row = me // columns
    done_half = me * 2 // owners
    half_rows_at = pl.multiple_of(done_half * (rows // 2), 8)
    corners = pltpu.make_async_copy(anchor_hbm, anchor_ref, sem_in)
    corners.start()

    def fine_copy(source, count, at, n):
        return pltpu.make_async_copy(
            source, fine_out.at[0, :, pl.ds(at, count), pl.ds((n % lane_blocks) * 128, 128)], sem_out.at[n]
        )

    inner = rows // 2 - 16
    done = [
        fine_copy(half_in.at[:, q, pl.ds(8, inner)], inner, pl.multiple_of(half_rows_at + 8, 8), q)
        for q in range(lane_blocks)
    ]
    for c in done:
        c.start()
    for k in range(3):
        for q in range(lane_blocks):
            made[k, q, pl.ds(half_rows_at, rows // 2)] = half_in[k, q]
    lane1 = lax.broadcasted_iota(jnp.int32, (1, 128), 1)
    wet[8 : 8 + rows] = wet_in[...]
    bed[8 : 8 + rows] = bed_in[...]
    unpack(dims, me, 0, messages, ds, field, extra)

    for source, at in ((owners - 1, 0), (0, 8 + rows)):
        last = from_half_rows(extra[source, 8:16], 0, lane1)
        for k in range(3):
            for q in range(lane_blocks):
                n = k * lane_blocks + q
                row = last if n == 8 else extra[source, n : n + 1]
                field[k, at : at + 8, q * 128 : q * 128 + 128] = jnp.broadcast_to(row, (8, 128))
            field[k, at : at + 8, cols:wide] = jnp.zeros((8, 128), F32)
    north = edge_rows(dims, extra, me - columns, my_row > 0)
    south = edge_rows(dims, extra, me + columns, my_row < blocks - 1)
    sub8 = lax.broadcasted_iota(jnp.int32, (8, 128), 0)
    stack = jnp.zeros((8, 128), F32)
    for n, row in enumerate((north[0], north[1], south[0], south[1])):
        stack = jnp.where(sub8 == n, row, stack)
    ends = mul_right(stack, spread_t(128, wide, 3), 3)
    for n, (ref, at) in enumerate(((wet, 0), (bed, 0), (wet, 8 + rows), (bed, 8 + rows))):
        ref[at : at + 8] = jnp.broadcast_to(ends[n : n + 1], (8, wide))
    side_cells(dims, me, 0, extra, wet, bed, rows)

    groups = rows // 8
    one = done_half * (groups - 1)
    sweep(dims, field, wet, bed, made, one, 1, 1)
    many = (1 - done_half) * (groups // 2 - 1)
    sweep(dims, field, wet, bed, made, many, groups // 2 + 1, 5)
    late = []
    for n, (group, count) in enumerate(((one, 8), (many, rows // 2 + 8)), 1):
        at = pl.multiple_of(group * 8, 8)
        for q in range(lane_blocks):
            late.append(fine_copy(made.at[:, q, pl.ds(at, count)], count, at, n * lane_blocks + q))
    for c in late:
        c.start()
    corners.wait()
    coarse_rows = rows // 3
    coarse_cols = cols // 3
    a0 = anchor_ref[nest, 0]
    a1 = anchor_ref[nest, 1]
    gather_cols = spread(cols, coarse_cols, 3, a1)
    for k in range(3):
        total = jnp.concatenate(
            [
                sum(made[k, q, pl.ds(n, coarse_rows, stride=3), :] for n in range(3))
                for q in range(lane_blocks)
            ],
            axis=1,
        )
        mean = mul_right(total, gather_cols, 2) * (1.0 / 9.0)
        rolled_out[k] = pltpu.roll(mean, a0, 0)
    for c in done + late:
        c.wait()


def finish_body(coarse, weights, up, left, diagonal, own, out):
    for k in range(3):
        out[k] = (
            coarse[k] * weights[0]
            + own[k] * weights[1]
            + left[k] * weights[2]
            + up[k] * weights[3]
            + diagonal[k] * weights[4]
        )


def in_vmem(x):
    return pltpu.with_memory_space_constraint(x, pltpu.VMEM)


def in_hbm(x):
    return pltpu.with_memory_space_constraint(x, pltpu.HBM)


SMEM = pl.BlockSpec(memory_space=pltpu.SMEM)
VMEM = pl.BlockSpec(memory_space=pltpu.VMEM)
HBM = pl.BlockSpec(memory_space=pltpu.HBM)


def half_call(dims, ds, wet_fine, bed_fine, messages):
    blocks, band, columns, lane_blocks = dims
    owners = blocks * columns
    rows = owners * band // 2
    wide = lane_blocks * 128 + 128
    return pl.pallas_call(
        lambda *refs: half_body(dims, ds, *refs),
        in_specs=[VMEM, VMEM] + [VMEM] * len(ds),
        out_specs=VMEM,
        out_shape=pltpu.VMEM((3, lane_blocks, rows, 128), F32),
        scratch_shapes=[
            pltpu.VMEM((3, rows + 16, wide), F32),
            pltpu.VMEM((rows + 16, wide), F32),
            pltpu.VMEM((rows + 16, wide), F32),
            pltpu.VMEM((owners, 16, 128), F32),
        ],
        name="half", compiler_params=pltpu.CompilerParams(vmem_limit_bytes=12 << 20),
    )(wet_fine, bed_fine, *messages)


def main_call(dims, ds, anchor, wet_fine, bed_fine, half, messages):
    blocks, band, columns, lane_blocks = dims
    owners = blocks * columns
    rows = owners * band
    cols = lane_blocks * 128
    wide = cols + 128
    return pl.pallas_call(
        lambda *refs: main_body(dims, ds, *refs),
        in_specs=[HBM, VMEM, VMEM, VMEM] + [VMEM] * owners,
        out_specs=[HBM, VMEM],
        out_shape=[
            jax.ShapeDtypeStruct((1, 3, rows, cols), F32),
            pltpu.VMEM((3, rows // 3, cols // 3), F32),
        ],
        scratch_shapes=[
            pltpu.VMEM((3, rows + 16, wide), F32),
            pltpu.VMEM((rows + 16, wide), F32),
            pltpu.VMEM((rows + 16, wide), F32),
            pltpu.VMEM((owners, 16, 128), F32),
            pltpu.VMEM((3, lane_blocks, rows, 128), F32),
            pltpu.SMEM((2, 2), jnp.int32),
            pltpu.SemaphoreType.DMA,
            pltpu.SemaphoreType.DMA((3 * lane_blocks,)),
        ],
        name="main", compiler_params=pltpu.CompilerParams(vmem_limit_bytes=20 << 20),
    )(anchor, wet_fine, bed_fine, half, *messages)


def local_packed(strips, anchor, wet_mask, bathy_index, bed_levels, coarse):
    blocks, band, full_cols = strips.shape[2], strips.shape[4], strips.shape[5]
    columns = lax.axis_size("col")
    owners = blocks * columns
    cols = full_cols // columns
    lane_blocks = cols // 128
    rows = owners * band
    wide = cols + 128
    dims = (blocks, band, columns, lane_blocks)
    height = 3 * lane_blocks * band + 16
    half_owners = owners // 2
    messages = []
    for ds in (range(half_owners), range(half_owners, owners)):
        made = pl.pallas_call(
            lambda *refs, ds=ds, after=len(messages[:1]): pack_body(dims, ds, after, *refs),
            in_specs=[HBM] * 4 + [VMEM] * len(messages[:1]),
            out_specs=[VMEM] * half_owners,
            out_shape=[pltpu.VMEM((height, 128), F32)] * half_owners,
            scratch_shapes=[
                pltpu.VMEM((3, blocks, band, full_cols), F32),
                pltpu.VMEM(wet_mask.shape, jnp.int32),
                pltpu.VMEM(bathy_index.shape, jnp.int32),
                pltpu.SMEM(bed_levels.shape, F32),
                pltpu.SemaphoreType.DMA((blocks,)),
                pltpu.SemaphoreType.DMA((3,)),
            ],
            name="pack", compiler_params=pltpu.CompilerParams(vmem_limit_bytes=10 << 20),
        )(
            in_hbm(strips),
            in_hbm(wet_mask),
            in_hbm(bathy_index),
            in_hbm(bed_levels),
            *messages[:1],
        )
        messages += [in_vmem(x) for x in made]

    def rank(d):
        r, c = d // columns, d % columns
        return (d >= half_owners, c * 2 < columns, r, c)

    wanted = sorted(range(1, owners), key=rank)
    arrived = {
        d: lax.ppermute(messages[d], ("row", "col"), [(i, i ^ d) for i in range(owners)])
        for d in wanted
    }
    arrived[0] = messages[0]
    arrived = {d: in_vmem(x) if d else x for d, x in arrived.items()}

    coarse_rows = rows // 3
    coarse_cols = cols // 3
    wet_fine, bed_fine, weights = pl.pallas_call(
        lambda *refs: prep_body(columns, *refs),
        in_specs=[SMEM, SMEM, VMEM, VMEM],
        out_specs=[VMEM] * 3,
        out_shape=[pltpu.VMEM((rows, wide), F32)] * 2
        + [pltpu.VMEM((5, coarse_rows, coarse_cols), F32)],
        name="prep", compiler_params=pltpu.CompilerParams(vmem_limit_bytes=12 << 20),
    )(bed_levels, anchor, wet_mask, bathy_index)

    early = [0] + wanted[: half_owners - 1]
    order = [0] + wanted
    wet_fine, bed_fine, weights = in_vmem(wet_fine), in_vmem(bed_fine), in_vmem(weights)
    half = half_call(dims, early, wet_fine, bed_fine, [arrived[d] for d in early])
    half = in_vmem(half)
    fine, rolled = main_call(
        dims, order, anchor, wet_fine, bed_fine, half, [arrived[d] for d in order]
    )
    rolled = in_vmem(rolled)

    lines = lax.axis_size("nest") * lax.axis_size("row")
    rights = [(c, c + 1) for c in range(columns - 1)]
    downs = [(l, l + 1) for l in range(lines - 1)]
    both = [(l * columns + c, l2 * columns + c2) for l, l2 in downs for c, c2 in rights]
    diagonal = lax.ppermute(rolled, ("nest", "row", "col"), both)
    from_left = lax.ppermute(rolled, "col", rights)
    from_up = lax.ppermute(rolled, ("nest", "row"), downs)

    coarse_next = pl.pallas_call(
        finish_body,
        in_specs=[VMEM] * 6,
        out_specs=VMEM,
        out_shape=jax.ShapeDtypeStruct(coarse.shape, F32),
        name="finish", compiler_params=pltpu.CompilerParams(vmem_limit_bytes=4 << 20),
    )(
        in_vmem(coarse),
        weights,
        in_vmem(from_up),
        in_vmem(from_left),
        in_vmem(diagonal),
        rolled,
    )
    return (fine, coarse_next)


def local(strips, anchor, wet_mask, bathy_index, bed_levels, coarse):
    columns = lax.axis_size("col")
    owners = strips.shape[2] * columns
    cols = strips.shape[5] // columns
    band = strips.shape[4]
    fits = (
        owners & (owners - 1) == 0
        and 2 <= owners <= 16
        and strips.shape[2] == lax.axis_size("row")
        and band == 24
        and cols == 384
        and owners * band == 384
        and wet_mask.shape[1:] == (128, 128)
    )
    run = local_packed if fits else local_general
    return run(strips, anchor, wet_mask, bathy_index, bed_levels, coarse)


def solution(mesh):
    return jax.shard_map(
        local,
        mesh=mesh,
        in_specs=(
            P("nest", None, None, ("row", "col"), None, None),
            P(),
            P("nest", "row", "col"),
            P("nest", "row", "col"),
            P(),
            P(None, ("nest", "row"), "col"),
        ),
        out_specs=(P("nest", None, "row", "col"), P(None, ("nest", "row"), "col")),
        check_vma=False,
    )
```

```python
import jax
import jax.numpy as jnp
from jax import lax
from jax.experimental import pallas as pl
from jax.experimental.pallas import tpu as pltpu
from jax.sharding import PartitionSpec as P


gravity = 1.0
courant = 0.2
F32 = jnp.float32


def padded_2(cells, sides, width):
    for axis, dim in sides:
        count = lax.axis_size(axis)
        ends = count - 1
        head = lax.slice_in_dim(cells, 0, width, axis=dim)
        tail = lax.slice_in_dim(cells, cells.shape[dim] - width, cells.shape[dim], axis=dim)
        cells = jnp.concatenate(
            [
                lax.ppermute(tail, axis, [(i, (i + 1) % count) for i in range(ends)]),
                cells,
                lax.ppermute(head, axis, [((i + 1) % count, i) for i in range(ends)]),
            ],
            axis=dim,
        )
    return cells


def passed_along(block, axis, distance):
    devices = range(lax.axis_size(axis))
    route = [(i - distance, i) for i in devices if i - distance in devices]
    return lax.ppermute(block, axis, route)


def advance(padded, bed_pad, wet_pad):
    depth_now = padded[0]
    flow_u = padded[1]
    flow_v = padded[2]
    depth_safe = jnp.where(wet_pad > 0.5, depth_now, 1.0)
    speed_u = flow_u / depth_safe
    speed_v = flow_v / depth_safe
    celerity = jnp.sqrt(gravity * depth_safe)
    pressure = 0.5 * gravity * depth_safe * depth_safe
    fluxes_x = (flow_u, flow_u * speed_u + pressure, flow_v * speed_u)
    fluxes_y = (flow_v, flow_u * speed_v, flow_v * speed_v + pressure)
    reach_x = jnp.abs(speed_u) + celerity
    reach_y = jnp.abs(speed_v) + celerity
    open_x = wet_pad[1:-1, :-1] * wet_pad[1:-1, 1:]
    open_y = wet_pad[:-1, 1:-1] * wet_pad[1:, 1:-1]
    bound_x = jnp.maximum(reach_x[1:-1, :-1], reach_x[1:-1, 1:])
    bound_y = jnp.maximum(reach_y[:-1, 1:-1], reach_y[1:, 1:-1])
    slope_x = (bed_pad[1:-1, 1:] - bed_pad[1:-1, :-1]) * open_x
    slope_y = (bed_pad[1:, 1:-1] - bed_pad[:-1, 1:-1]) * open_y
    centre = depth_now[1:-1, 1:-1]
    sources = (
        None,
        -0.5 * gravity * centre * (slope_x[:, 1:] + slope_x[:, :-1]),
        -0.5 * gravity * centre * (slope_y[1:] + slope_y[:-1]),
    )
    results = []
    for plane in range(3):
        state = padded[plane]
        flux_col = fluxes_x[plane]
        flux_row = fluxes_y[plane]
        face_x = (
            0.5 * (flux_col[1:-1, :-1] + flux_col[1:-1, 1:])
            - 0.5 * bound_x * (state[1:-1, 1:] - state[1:-1, :-1])
        ) * open_x
        face_y = (
            0.5 * (flux_row[:-1, 1:-1] + flux_row[1:, 1:-1])
            - 0.5 * bound_y * (state[1:, 1:-1] - state[:-1, 1:-1])
        ) * open_y
        value = (
            state[1:-1, 1:-1]
            - courant * (face_x[:, 1:] - face_x[:, :-1])
            - courant * (face_y[1:] - face_y[:-1])
        )
        if plane > 0:
            value = value + courant * sources[plane]
        results.append(value)
    return jnp.stack(results)


def expand(cells):
    return jnp.repeat(jnp.repeat(cells, 3, axis=-2), 3, axis=-1)


def lookup(classes, levels):
    ladder = jnp.arange(levels.shape[0], dtype=jnp.int32)
    matches = classes[None] == ladder[:, None, None]
    return jnp.sum(jnp.where(matches, levels[:, None, None], 0.0), axis=0)


def restrict(updated):
    planes, row_count, col_count = updated.shape
    return updated.reshape(planes, row_count // 3, 3, col_count // 3, 3).sum(axis=(2, 4)) / 9.0


def local_general(strips, anchor, wet_mask, bathy_index, bed_levels, coarse):
    tile_blocks = strips.shape[2]
    band_rows = strips.shape[4]
    full_cols = strips.shape[5]
    columns = lax.axis_size("col")
    tile_cols = full_cols // columns
    layered = (
        strips[0, :, :, 0]
        .reshape(3, tile_blocks, band_rows, columns, tile_cols)
        .transpose(0, 1, 3, 2, 4)
    )
    flattened = layered.reshape(3, tile_blocks * columns, band_rows, tile_cols)
    arrived = lax.all_to_all(flattened, ("row", "col"), split_axis=1, concat_axis=1, tiled=True)
    fields = arrived.reshape(3, tile_blocks * columns * band_rows, tile_cols)
    bed_fine = expand(lookup(bathy_index[0], bed_levels))
    wetness = expand(wet_mask[0].astype(F32))
    stacked = jnp.concatenate([fields, bed_fine[None], wetness[None]], axis=0)
    padded_all = padded_2(stacked, (("row", 1), ("col", 2)), 1)
    updated = advance(padded_all[:3], padded_all[3], padded_all[4])
    restricted = restrict(updated)
    coarse_rows = restricted.shape[1]
    coarse_cols = restricted.shape[2]
    contribution = jnp.concatenate(
        [restricted, jnp.ones((1, coarse_rows, coarse_cols), F32)], axis=0
    )
    nest_index = lax.axis_index("nest")
    corner = lax.dynamic_index_in_dim(anchor, nest_index, 0, keepdims=False)
    canvas = lax.dynamic_update_slice(
        jnp.zeros((4, 2 * coarse_rows, 2 * coarse_cols), F32),
        contribution,
        (jnp.int32(0), corner[0], corner[1]),
    )
    spilled = passed_along(canvas[:, :, coarse_cols:], "col", 1)
    merged = canvas[:, :, :coarse_cols] + spilled
    lowered = passed_along(merged[:, coarse_rows:], ("nest", "row"), 1)
    received_sum = merged[:, :coarse_rows] + lowered
    coarse_next = (coarse + received_sum[:3]) / (1.0 + received_sum[3])
    return (updated[None], coarse_next)


def half_rows(row):
    return pltpu.roll(row, 64, 1), row


def from_half_rows(block, at, lane):
    upper = block[at : at + 1]
    return jnp.where(lane < 64, pltpu.roll(upper, 64, 1), block[at + 1 : at + 2])


def pack_body(dims, ds, after, strips_hbm, wet_hbm, class_hbm, levels_hbm, *rest):
    blocks, band, columns, lane_blocks = dims
    rest = rest[after:]
    outs = rest[: len(ds)]
    strips, wet_ref, class_ref, levels_ref, sems, small = rest[len(ds) :]
    tile_cols = lane_blocks * 128
    me = lax.axis_index(("row", "col")).astype(jnp.int32)
    my_row = me // columns
    my_col = me % columns
    loads = [
        pltpu.make_async_copy(wet_hbm, wet_ref, small.at[0]),
        pltpu.make_async_copy(class_hbm, class_ref, small.at[1]),
        pltpu.make_async_copy(levels_hbm, levels_ref, small.at[2]),
    ]
    for c in loads:
        c.start()
    copies = []
    for r in range(blocks):
        j = my_row ^ (r ^ (ds[0] // columns))
        copies.append(
            pltpu.make_async_copy(strips_hbm.at[0, :, j, 0], strips.at[:, j], sems.at[r])
        )
    for c in copies:
        c.start()
    lane = lax.broadcasted_iota(jnp.int32, (8, 128), 1)
    sub = lax.broadcasted_iota(jnp.int32, (8, 128), 0)
    size = wet_ref.shape[1]
    diag = lax.broadcasted_iota(jnp.int32, (size, 128), 0) == lax.broadcasted_iota(
        jnp.int32, (size, 128), 1
    )
    for c in loads:
        c.wait()
    edges = []
    for ref in (wet_ref, class_ref):
        cells = ref[0].astype(F32)
        north = cells[0:1]
        south = cells[size - 1 : size]
        west = jnp.sum(jnp.where(diag, cells[:, 0:1], 0.0), axis=0, keepdims=True)
        east = jnp.sum(jnp.where(diag, cells[:, 127:128], 0.0), axis=0, keepdims=True)
        four = (north, south, west, east)
        if ref is class_ref:
            four = tuple(level_of(row, levels_ref) for row in four)
        edges.append(four)
    first = me == 0
    for c in copies:
        c.wait()
    for out, d in zip(outs, ds):
        to = me ^ d
        j = to // columns
        c = to % columns
        base = pl.multiple_of(c * tile_cols, 128)
        for k in range(3):
            for q in range(lane_blocks):
                at = (k * lane_blocks + q) * band
                out[at : at + band] = strips[k, j, :, pl.ds(pl.multiple_of(base + q * 128, 128), 128)]
        at = 3 * lane_blocks * band
        west_at = pl.multiple_of(jnp.maximum(base - 128, 0), 128)
        east_at = pl.multiple_of(jnp.where(c == columns - 1, base, base + tile_cols), 128)
        mixed = jnp.zeros((8, 128), F32)
        for g in range(band // 8):
            for k in range(3):
                i = g * 3 + k
                west = strips[k, j, g * 8 : g * 8 + 8, pl.ds(west_at, 128)]
                east = strips[k, j, g * 8 : g * 8 + 8, pl.ds(east_at, 128)]
                both = pltpu.roll(jnp.where(lane == 127, west, east), 2 * i + 1, 1)
                mixed = jnp.where((lane == 2 * i) | (lane == 2 * i + 1), both, mixed)
        jj = jnp.clip(jnp.where(first, j + 1, j - 1), 0, blocks - 1)
        rows = []
        for k in range(3):
            for q in range(lane_blocks):
                spot = pl.ds(pl.multiple_of(base + q * 128, 128), 128)
                head = strips[k, jj, 0:8, spot][0:1]
                tail = strips[k, jj, band - 8 : band, spot][7:8]
                rows.append(jnp.where(first, head, tail))
        halo = jnp.zeros((8, 128), F32)
        for i in range(8):
            halo = jnp.where(sub == i, rows[i], halo)
        out[at : at + 8] = halo
        tucked = [rows[8]]
        for north, south, west, east in edges:
            row = jnp.where(
                c == my_col,
                jnp.where(j > my_row, south, north),
                jnp.where(c > my_col, east, west),
            )
            tucked.append(row)
        for n, row in enumerate(tucked):
            low, high = half_rows(row)
            mixed = jnp.where((sub == 2 * n) & (lane >= 64), low, mixed)
            mixed = jnp.where((sub == 2 * n + 1) & (lane >= 64), high, mixed)
        out[at + 8 : at + 16] = mixed


def spread(rows, cols, width, offset=None):
    i = lax.broadcasted_iota(jnp.int32, (rows, cols), 0)
    m = lax.broadcasted_iota(jnp.int32, (rows, cols), 1)
    if offset is not None:
        m = m - offset
        m = jnp.where(m < 0, m + cols, m)
    low = m * width
    return jnp.where((i >= low) & (i < low + width), 1.0, 0.0)


def spread_t(rows, cols, width, offset=None):
    m = lax.broadcasted_iota(jnp.int32, (rows, cols), 0)
    i = lax.broadcasted_iota(jnp.int32, (rows, cols), 1)
    if offset is not None:
        m = m - offset
        m = jnp.where(m < 0, m + rows, m)
    low = m * width
    return jnp.where((i >= low) & (i < low + width), 1.0, 0.0)


def level_of(classes, levels_ref):
    out = jnp.zeros_like(classes)
    for n in range(levels_ref.shape[0]):
        out = jnp.where(classes == n, levels_ref[n], out)
    return out


def prep_body(columns, levels_ref, anchor_ref, wet_ref, class_ref, wet_out, bed_out, weights):
    lane_blocks, rows, _ = wet_out.shape
    size, width = wet_ref.shape[1], wet_ref.shape[2]
    wet = wet_ref[0].astype(F32)
    bed = level_of(class_ref[0].astype(F32), levels_ref)
    across = spread_t(width, lane_blocks * 128, 3)
    down = spread(rows, size, 3)
    for out, cells, parts in ((wet_out, wet, 1), (bed_out, bed, 3)):
        fine = mul_left(down, mul_right(cells, across, parts), parts)
        for q in range(lane_blocks):
            out[q] = fine[:, q * 128 : q * 128 + 128]
    nest = lax.axis_index("nest").astype(jnp.int32)
    row_at = lax.axis_index("row").astype(jnp.int32)
    col_at = lax.axis_index("col").astype(jnp.int32)
    up_nest = jnp.where(row_at == 0, jnp.maximum(nest - 1, 0), nest)
    i = lax.broadcasted_iota(jnp.int32, weights.shape[1:], 0)
    m = lax.broadcasted_iota(jnp.int32, weights.shape[1:], 1)
    has_left = jnp.where(col_at > 0, 1.0, 0.0)
    has_up = jnp.where((row_at > 0) | (nest > 0), 1.0, 0.0)
    own_rows = jnp.where(i >= anchor_ref[nest, 0], 1.0, 0.0)
    up_rows = jnp.where(i < anchor_ref[up_nest, 0], has_up, 0.0)
    own_cols = m >= anchor_ref[nest, 1]
    up_cols = m >= anchor_ref[up_nest, 1]
    shares = (
        jnp.where(own_cols, own_rows, 0.0),
        jnp.where(own_cols, 0.0, own_rows * has_left),
        jnp.where(up_cols, up_rows, 0.0),
        jnp.where(up_cols, 0.0, up_rows * has_left),
    )
    scale = 1.0 / (1.0 + shares[0] + shares[1] + shares[2] + shares[3])
    weights[0] = scale
    for n, share in enumerate(shares):
        weights[n + 1] = share * scale


def split(x, parts):
    out = []
    for n in range(parts):
        piece = x.astype(jnp.bfloat16)
        out.append(piece)
        if n + 1 < parts:
            x = x - piece.astype(F32)
    return out


def mul_left(matrix, x, parts):
    matrix = matrix.astype(jnp.bfloat16)
    return sum(jnp.dot(matrix, piece, preferred_element_type=F32) for piece in split(x, parts))


def mul_right(x, matrix, parts):
    matrix = matrix.astype(jnp.bfloat16)
    return sum(jnp.dot(piece, matrix, preferred_element_type=F32) for piece in split(x, parts))


def mul_left_t(matrix, x, parts):
    matrix = matrix.astype(jnp.bfloat16)
    return sum(
        lax.dot_general(matrix, piece, (((1,), (1,)), ((), ())), preferred_element_type=F32)
        for piece in split(x, parts)
    )


def unpack(dims, me, first_row, messages, ds, field, extra):
    blocks, band, columns, lane_blocks = dims
    body_rows = 3 * lane_blocks * band
    for message, d in zip(messages, ds):
        p = me ^ d
        top = pl.multiple_of(8 + p * band - first_row, 8)
        mixed = message[body_rows + 8 : body_rows + 16]
        for k in range(3):
            for q in range(lane_blocks):
                n = k * lane_blocks + q
                field[k, q, pl.ds(top, band)] = message[
                    n * band : n * band + band
                ]
            for g in range(band // 8):
                i = g * 3 + k
                at = pl.multiple_of(top + g * 8, 8)
                field[k, lane_blocks, pl.ds(at, 8)] = pltpu.roll(mixed, 127 - 2 * i, 1)
        extra[p] = message[body_rows : body_rows + 16]


def edge_rows(dims, extra, source, inside):
    blocks, band, columns, lane_blocks = dims
    lane = lax.broadcasted_iota(jnp.int32, (1, 128), 1)
    block = extra[jnp.where(inside, source, 0), 8:16]
    wet_row = from_half_rows(block, 2, lane)
    bed_row = from_half_rows(block, 4, lane)
    return jnp.where(inside, wet_row, 0.0), jnp.where(inside, bed_row, 0.0)


def side_cells(dims, me, first_row, extra, wet, bed, rows):
    blocks, band, columns, lane_blocks = dims
    my_col = me % columns
    west = edge_rows(dims, extra, me - 1, my_col > 0)
    east = edge_rows(dims, extra, me + 1, my_col < columns - 1)
    sub = lax.broadcasted_iota(jnp.int32, (128, 128), 0)
    pair = jnp.zeros((128, 128), F32)
    for n, row in ((0, east[0]), (127, west[0]), (64, east[1]), (63, west[1])):
        pair = jnp.where(sub == n, row, pair)
    i = lax.broadcasted_iota(jnp.int32, (rows, 128), 0) + first_row
    low = lax.broadcasted_iota(jnp.int32, (rows, 128), 1) * 3
    sides = mul_left_t(jnp.where((i >= low) & (i < low + 3), 1.0, 0.0), pair, 3)
    wet[lane_blocks, 8 : 8 + rows] = sides
    bed[lane_blocks, 8 : 8 + rows] = pltpu.roll(sides, 64, 1)


def sweep(dims, field, wet, bed, more, made, start, count, unroll):
    lane_blocks = dims[3]
    sides = lane_blocks + 1
    lane = lax.broadcasted_iota(jnp.int32, (8, 128), 1)
    sub = lax.broadcasted_iota(jnp.int32, (8, 128), 0)

    def cells(group, q):
        at = pl.ds(pl.multiple_of(8 + group * 8, 8), 8)
        h, hu, hv = (field[k, q, at] for k in range(3))
        w, z = wet[q, at], bed[q, at]
        hs = jnp.where(w > 0.5, h, 1.0)
        root = lax.rsqrt(hs)
        inv = root * root
        u = hu * inv
        v = hv * inv
        c = (gravity**0.5) * (hs * root)
        p = 0.5 * gravity * hs * hs
        f2 = hu * u + p
        m = hv * u
        a = jnp.abs(u) + c
        if q < lane_blocks:
            more[0, q, at] = m
            more[1, q, at] = hv * v + p
            more[2, q, at] = jnp.abs(v) + c
        return h, hu, hv, w, z, f2, m, a

    def face(near, far):
        half = (0.5 * courant) * (near[3] * far[3])
        bound = half * jnp.maximum(near[8], far[8])
        out = [half * (near[5 + k] + far[5 + k]) - bound * (far[k] - near[k]) for k in range(3)]
        out.append(half * (far[4] - near[4]))
        return out

    def across(t, _):
        group = start + t
        blocks = [cells(group, q) for q in range(sides)]
        faces = []
        for q in range(sides):
            now, nxt = blocks[q], blocks[(q + 1) % sides]
            h, hu, hv, w, z, f2, m, a = now
            h2, hu2, hv2, w2, z2, f22, m2, a2 = (
                pltpu.roll(jnp.where(lane == 0, y, x), 127, 1) for x, y in zip(now, nxt)
            )
            faces.append(
                face((h, hu, hv, w, z, hu, f2, m, a), (h2, hu2, hv2, w2, z2, hu2, f22, m2, a2))
            )
        spot = pl.ds(pl.multiple_of(group * 8, 8), 8)
        for q in range(lane_blocks):
            right = faces[q]
            left = [
                pltpu.roll(jnp.where(lane == 127, y, x), 1, 1) for x, y in zip(right, faces[q - 1])
            ]
            h, hu, hv = blocks[q][:3]
            made[0, q, spot] = h - (right[0] - left[0])
            made[1, q, spot] = hu - (right[1] - left[1]) - gravity * h * (right[3] + left[3])
            made[2, q, spot] = hv - (right[2] - left[2])
        return 0

    def south_face(group, q):
        at = pl.multiple_of(8 + group * 8, 8)
        sides = []
        for step in range(2):
            rows = pl.ds(at + step, 8)
            h, hu, hv = (field[k, q, rows] for k in range(3))
            m, g3, b = (more[k, q, rows] for k in range(3))
            sides.append((h, hu, hv, wet[q, rows], bed[q, rows], hv, m, g3, b))
        return face(*sides)

    def down(t, above):
        group = start + t
        spot = pl.ds(pl.multiple_of(group * 8, 8), 8)
        new = []
        for q in range(lane_blocks):
            below = south_face(group, q)
            up = [
                pltpu.roll(jnp.where(sub == 7, y, x), 1, 0) for x, y in zip(below, above[q])
            ]
            h = field[0, q, pl.ds(pl.multiple_of(8 + group * 8, 8), 8)]
            made[0, q, spot] = made[0, q, spot] - (below[0] - up[0])
            made[1, q, spot] = made[1, q, spot] - (below[1] - up[1])
            made[2, q, spot] = (
                made[2, q, spot] - (below[2] - up[2]) - gravity * h * (below[3] + up[3])
            )
            new.append(below)
        return new

    for q in range(lane_blocks):
        cells(start - 1, q)
        cells(start + count, q)
    if count == 1:
        across(0, 0)
        down(0, [south_face(start - 1, q) for q in range(lane_blocks)])
    else:
        lax.fori_loop(0, count, across, 0, unroll=unroll)
        above = [south_face(start - 1, q) for q in range(lane_blocks)]
        lax.fori_loop(0, count, down, above, unroll=unroll)


def half_body(dims, ds, wet_in, bed_in, *rest):
    blocks, band, columns, lane_blocks = dims
    owners = blocks * columns
    messages = rest[: len(ds)]
    made, field, wet, bed, more, extra = rest[len(ds) :]
    rows = owners * band // 2
    me = lax.axis_index(("row", "col")).astype(jnp.int32)
    first_row = pl.multiple_of((me * 2 // owners) * rows, 8)
    for q in range(lane_blocks):
        wet[q, 8 : 8 + rows] = wet_in[q, pl.ds(first_row, rows)]
        bed[q, 8 : 8 + rows] = bed_in[q, pl.ds(first_row, rows)]
    unpack(dims, me, first_row, messages, ds, field, extra)
    side_cells(dims, me, first_row, extra, wet, bed, rows)
    for k in range(3):
        for q in range(lane_blocks):
            made[k, q, 0:8] = jnp.zeros((8, 128), F32)
            made[k, q, rows - 8 : rows] = jnp.zeros((8, 128), F32)
    sweep(dims, field, wet, bed, more, made, 1, rows // 8 - 2, 2)


def main_body(dims, ds, anchor_hbm, wet_in, bed_in, half_in, *rest):
    blocks, band, columns, lane_blocks = dims
    owners = blocks * columns
    messages = rest[:owners]
    fine_out, rolled_out = rest[owners : owners + 2]
    field, wet, bed, more, extra, made, anchor_ref, sem_in, sem_out = rest[owners + 2 :]
    rows = owners * band
    cols = lane_blocks * 128
    me = lax.axis_index(("row", "col")).astype(jnp.int32)
    nest = lax.axis_index("nest").astype(jnp.int32)
    my_row = me // columns
    done_half = me * 2 // owners
    half_rows_at = pl.multiple_of(done_half * (rows // 2), 8)
    corners = pltpu.make_async_copy(anchor_hbm, anchor_ref, sem_in)
    corners.start()

    def fine_copy(source, count, at, n):
        return pltpu.make_async_copy(
            source, fine_out.at[0, :, pl.ds(at, count), pl.ds((n % lane_blocks) * 128, 128)], sem_out.at[n]
        )

    inner = rows // 2 - 16
    done = [
        fine_copy(half_in.at[:, q, pl.ds(8, inner)], inner, pl.multiple_of(half_rows_at + 8, 8), q)
        for q in range(lane_blocks)
    ]
    for c in done:
        c.start()
    for k in range(3):
        for q in range(lane_blocks):
            made[k, q, pl.ds(half_rows_at, rows // 2)] = half_in[k, q]
    lane1 = lax.broadcasted_iota(jnp.int32, (1, 128), 1)
    for q in range(lane_blocks):
        wet[q, 8 : 8 + rows] = wet_in[q]
        bed[q, 8 : 8 + rows] = bed_in[q]
    unpack(dims, me, 0, messages, ds, field, extra)

    for source, at in ((owners - 1, 0), (0, 8 + rows)):
        last = from_half_rows(extra[source, 8:16], 0, lane1)
        for k in range(3):
            for q in range(lane_blocks):
                n = k * lane_blocks + q
                row = last if n == 8 else extra[source, n : n + 1]
                field[k, q, at : at + 8] = jnp.broadcast_to(row, (8, 128))
    north = edge_rows(dims, extra, me - columns, my_row > 0)
    south = edge_rows(dims, extra, me + columns, my_row < blocks - 1)
    sub8 = lax.broadcasted_iota(jnp.int32, (8, 128), 0)
    stack = jnp.zeros((8, 128), F32)
    for n, row in enumerate((north[0], north[1], south[0], south[1])):
        stack = jnp.where(sub8 == n, row, stack)
    ends = mul_right(stack, spread_t(128, cols, 3), 3)
    for n, (ref, at) in enumerate(((wet, 0), (bed, 0), (wet, 8 + rows), (bed, 8 + rows))):
        for q in range(lane_blocks):
            ref[q, at : at + 8] = jnp.broadcast_to(ends[n : n + 1, q * 128 : q * 128 + 128], (8, 128))
    side_cells(dims, me, 0, extra, wet, bed, rows)

    groups = rows // 8
    one = done_half * (groups - 1)
    sweep(dims, field, wet, bed, more, made, one, 1, 1)
    many = (1 - done_half) * (groups // 2 - 1)
    sweep(dims, field, wet, bed, more, made, many, groups // 2 + 1, 5)
    late = []
    for n, (group, count) in enumerate(((one, 8), (many, rows // 2 + 8)), 1):
        at = pl.multiple_of(group * 8, 8)
        for q in range(lane_blocks):
            late.append(fine_copy(made.at[:, q, pl.ds(at, count)], count, at, n * lane_blocks + q))
    for c in late:
        c.start()
    corners.wait()
    coarse_rows = rows // 3
    coarse_cols = cols // 3
    a0 = anchor_ref[nest, 0]
    a1 = anchor_ref[nest, 1]
    gather_cols = spread(cols, coarse_cols, 3, a1)
    for k in range(3):
        total = jnp.concatenate(
            [
                sum(made[k, q, pl.ds(n, coarse_rows, stride=3), :] for n in range(3))
                for q in range(lane_blocks)
            ],
            axis=1,
        )
        mean = mul_right(total, gather_cols, 2) * (1.0 / 9.0)
        rolled_out[k] = pltpu.roll(mean, a0, 0)
    for c in done + late:
        c.wait()


def finish_body(coarse, weights, up, left, diagonal, own, out):
    for k in range(3):
        out[k] = (
            coarse[k] * weights[0]
            + own[k] * weights[1]
            + left[k] * weights[2]
            + up[k] * weights[3]
            + diagonal[k] * weights[4]
        )


def in_vmem(x):
    return pltpu.with_memory_space_constraint(x, pltpu.VMEM)


def in_hbm(x):
    return pltpu.with_memory_space_constraint(x, pltpu.HBM)


SMEM = pl.BlockSpec(memory_space=pltpu.SMEM)
VMEM = pl.BlockSpec(memory_space=pltpu.VMEM)
HBM = pl.BlockSpec(memory_space=pltpu.HBM)


def half_call(dims, ds, wet_fine, bed_fine, messages):
    blocks, band, columns, lane_blocks = dims
    owners = blocks * columns
    rows = owners * band // 2
    return pl.pallas_call(
        lambda *refs: half_body(dims, ds, *refs),
        in_specs=[VMEM, VMEM] + [VMEM] * len(ds),
        out_specs=VMEM,
        out_shape=pltpu.VMEM((3, lane_blocks, rows, 128), F32),
        scratch_shapes=[
            pltpu.VMEM((3, lane_blocks + 1, rows + 16, 128), F32),
            pltpu.VMEM((lane_blocks + 1, rows + 16, 128), F32),
            pltpu.VMEM((lane_blocks + 1, rows + 16, 128), F32),
            pltpu.VMEM((3, lane_blocks, rows + 16, 128), F32),
            pltpu.VMEM((owners, 16, 128), F32),
        ],
        name="half", compiler_params=pltpu.CompilerParams(vmem_limit_bytes=12 << 20),
    )(wet_fine, bed_fine, *messages)


def main_call(dims, ds, anchor, wet_fine, bed_fine, half, messages):
    blocks, band, columns, lane_blocks = dims
    owners = blocks * columns
    rows = owners * band
    cols = lane_blocks * 128
    return pl.pallas_call(
        lambda *refs: main_body(dims, ds, *refs),
        in_specs=[HBM, VMEM, VMEM, VMEM] + [VMEM] * owners,
        out_specs=[HBM, VMEM],
        out_shape=[
            jax.ShapeDtypeStruct((1, 3, rows, cols), F32),
            pltpu.VMEM((3, rows // 3, cols // 3), F32),
        ],
        scratch_shapes=[
            pltpu.VMEM((3, lane_blocks + 1, rows + 16, 128), F32),
            pltpu.VMEM((lane_blocks + 1, rows + 16, 128), F32),
            pltpu.VMEM((lane_blocks + 1, rows + 16, 128), F32),
            pltpu.VMEM((3, lane_blocks, rows + 16, 128), F32),
            pltpu.VMEM((owners, 16, 128), F32),
            pltpu.VMEM((3, lane_blocks, rows, 128), F32),
            pltpu.SMEM((2, 2), jnp.int32),
            pltpu.SemaphoreType.DMA,
            pltpu.SemaphoreType.DMA((3 * lane_blocks,)),
        ],
        name="main", compiler_params=pltpu.CompilerParams(vmem_limit_bytes=20 << 20),
    )(anchor, wet_fine, bed_fine, half, *messages)


def local_packed(strips, anchor, wet_mask, bathy_index, bed_levels, coarse):
    blocks, band, full_cols = strips.shape[2], strips.shape[4], strips.shape[5]
    columns = lax.axis_size("col")
    owners = blocks * columns
    cols = full_cols // columns
    lane_blocks = cols // 128
    rows = owners * band
    dims = (blocks, band, columns, lane_blocks)
    height = 3 * lane_blocks * band + 16
    half_owners = owners // 2
    messages = []
    for ds in (range(half_owners), range(half_owners, owners)):
        made = pl.pallas_call(
            lambda *refs, ds=ds, after=len(messages[:1]): pack_body(dims, ds, after, *refs),
            in_specs=[HBM] * 4 + [VMEM] * len(messages[:1]),
            out_specs=[VMEM] * half_owners,
            out_shape=[pltpu.VMEM((height, 128), F32)] * half_owners,
            scratch_shapes=[
                pltpu.VMEM((3, blocks, band, full_cols), F32),
                pltpu.VMEM(wet_mask.shape, jnp.int32),
                pltpu.VMEM(bathy_index.shape, jnp.int32),
                pltpu.SMEM(bed_levels.shape, F32),
                pltpu.SemaphoreType.DMA((blocks,)),
                pltpu.SemaphoreType.DMA((3,)),
            ],
            name="pack", compiler_params=pltpu.CompilerParams(vmem_limit_bytes=10 << 20),
        )(
            in_hbm(strips),
            in_hbm(wet_mask),
            in_hbm(bathy_index),
            in_hbm(bed_levels),
            *messages[:1],
        )
        messages += [in_vmem(x) for x in made]

    def rank(d):
        r, c = d // columns, d % columns
        return (d >= half_owners, c * 2 < columns, r, c)

    wanted = sorted(range(1, owners), key=rank)
    arrived = {
        d: lax.ppermute(messages[d], ("row", "col"), [(i, i ^ d) for i in range(owners)])
        for d in wanted
    }
    arrived[0] = messages[0]
    arrived = {d: in_vmem(x) if d else x for d, x in arrived.items()}

    coarse_rows = rows // 3
    coarse_cols = cols // 3
    wet_fine, bed_fine, weights = pl.pallas_call(
        lambda *refs: prep_body(columns, *refs),
        in_specs=[SMEM, SMEM, VMEM, VMEM],
        out_specs=[VMEM] * 3,
        out_shape=[pltpu.VMEM((lane_blocks, rows, 128), F32)] * 2
        + [pltpu.VMEM((5, coarse_rows, coarse_cols), F32)],
        name="prep", compiler_params=pltpu.CompilerParams(vmem_limit_bytes=12 << 20),
    )(bed_levels, anchor, wet_mask, bathy_index)

    early = [0] + wanted[: half_owners - 1]
    order = [0] + wanted
    wet_fine, bed_fine, weights = in_vmem(wet_fine), in_vmem(bed_fine), in_vmem(weights)
    half = half_call(dims, early, wet_fine, bed_fine, [arrived[d] for d in early])
    half = in_vmem(half)
    fine, rolled = main_call(
        dims, order, anchor, wet_fine, bed_fine, half, [arrived[d] for d in order]
    )
    rolled = in_vmem(rolled)

    lines = lax.axis_size("nest") * lax.axis_size("row")
    rights = [(c, c + 1) for c in range(columns - 1)]
    downs = [(l, l + 1) for l in range(lines - 1)]
    both = [(l * columns + c, l2 * columns + c2) for l, l2 in downs for c, c2 in rights]
    diagonal = lax.ppermute(rolled, ("nest", "row", "col"), both)
    from_left = lax.ppermute(rolled, "col", rights)
    from_up = lax.ppermute(rolled, ("nest", "row"), downs)

    coarse_next = pl.pallas_call(
        finish_body,
        in_specs=[VMEM] * 6,
        out_specs=VMEM,
        out_shape=jax.ShapeDtypeStruct(coarse.shape, F32),
        name="finish", compiler_params=pltpu.CompilerParams(vmem_limit_bytes=4 << 20),
    )(
        in_vmem(coarse),
        weights,
        in_vmem(from_up),
        in_vmem(from_left),
        in_vmem(diagonal),
        rolled,
    )
    return (fine, coarse_next)


def local(strips, anchor, wet_mask, bathy_index, bed_levels, coarse):
    columns = lax.axis_size("col")
    owners = strips.shape[2] * columns
    cols = strips.shape[5] // columns
    band = strips.shape[4]
    fits = (
        owners & (owners - 1) == 0
        and 2 <= owners <= 16
        and strips.shape[2] == lax.axis_size("row")
        and band == 24
        and cols == 384
        and owners * band == 384
        and wet_mask.shape[1:] == (128, 128)
    )
    run = local_packed if fits else local_general
    return run(strips, anchor, wet_mask, bathy_index, bed_levels, coarse)


def solution(mesh):
    return jax.shard_map(
        local,
        mesh=mesh,
        in_specs=(
            P("nest", None, None, ("row", "col"), None, None),
            P(),
            P("nest", "row", "col"),
            P("nest", "row", "col"),
            P(),
            P(None, ("nest", "row"), "col"),
        ),
        out_specs=(P("nest", None, "row", "col"), P(None, ("nest", "row"), "col")),
        check_vma=False,
    )
```

```python
import jax
import jax.numpy as jnp
from jax import lax
from jax.experimental import pallas as pl
from jax.experimental.pallas import tpu as pltpu
from jax.sharding import PartitionSpec as P


gravity = 1.0
courant = 0.2
F32 = jnp.float32


def padded_2(cells, sides, width):
    for axis, dim in sides:
        count = lax.axis_size(axis)
        ends = count - 1
        head = lax.slice_in_dim(cells, 0, width, axis=dim)
        tail = lax.slice_in_dim(cells, cells.shape[dim] - width, cells.shape[dim], axis=dim)
        cells = jnp.concatenate(
            [
                lax.ppermute(tail, axis, [(i, (i + 1) % count) for i in range(ends)]),
                cells,
                lax.ppermute(head, axis, [((i + 1) % count, i) for i in range(ends)]),
            ],
            axis=dim,
        )
    return cells


def passed_along(block, axis, distance):
    devices = range(lax.axis_size(axis))
    route = [(i - distance, i) for i in devices if i - distance in devices]
    return lax.ppermute(block, axis, route)


def advance(padded, bed_pad, wet_pad):
    depth_now = padded[0]
    flow_u = padded[1]
    flow_v = padded[2]
    depth_safe = jnp.where(wet_pad > 0.5, depth_now, 1.0)
    speed_u = flow_u / depth_safe
    speed_v = flow_v / depth_safe
    celerity = jnp.sqrt(gravity * depth_safe)
    pressure = 0.5 * gravity * depth_safe * depth_safe
    fluxes_x = (flow_u, flow_u * speed_u + pressure, flow_v * speed_u)
    fluxes_y = (flow_v, flow_u * speed_v, flow_v * speed_v + pressure)
    reach_x = jnp.abs(speed_u) + celerity
    reach_y = jnp.abs(speed_v) + celerity
    open_x = wet_pad[1:-1, :-1] * wet_pad[1:-1, 1:]
    open_y = wet_pad[:-1, 1:-1] * wet_pad[1:, 1:-1]
    bound_x = jnp.maximum(reach_x[1:-1, :-1], reach_x[1:-1, 1:])
    bound_y = jnp.maximum(reach_y[:-1, 1:-1], reach_y[1:, 1:-1])
    slope_x = (bed_pad[1:-1, 1:] - bed_pad[1:-1, :-1]) * open_x
    slope_y = (bed_pad[1:, 1:-1] - bed_pad[:-1, 1:-1]) * open_y
    centre = depth_now[1:-1, 1:-1]
    sources = (
        None,
        -0.5 * gravity * centre * (slope_x[:, 1:] + slope_x[:, :-1]),
        -0.5 * gravity * centre * (slope_y[1:] + slope_y[:-1]),
    )
    results = []
    for plane in range(3):
        state = padded[plane]
        flux_col = fluxes_x[plane]
        flux_row = fluxes_y[plane]
        face_x = (
            0.5 * (flux_col[1:-1, :-1] + flux_col[1:-1, 1:])
            - 0.5 * bound_x * (state[1:-1, 1:] - state[1:-1, :-1])
        ) * open_x
        face_y = (
            0.5 * (flux_row[:-1, 1:-1] + flux_row[1:, 1:-1])
            - 0.5 * bound_y * (state[1:, 1:-1] - state[:-1, 1:-1])
        ) * open_y
        value = (
            state[1:-1, 1:-1]
            - courant * (face_x[:, 1:] - face_x[:, :-1])
            - courant * (face_y[1:] - face_y[:-1])
        )
        if plane > 0:
            value = value + courant * sources[plane]
        results.append(value)
    return jnp.stack(results)


def expand(cells):
    return jnp.repeat(jnp.repeat(cells, 3, axis=-2), 3, axis=-1)


def lookup(classes, levels):
    ladder = jnp.arange(levels.shape[0], dtype=jnp.int32)
    matches = classes[None] == ladder[:, None, None]
    return jnp.sum(jnp.where(matches, levels[:, None, None], 0.0), axis=0)


def restrict(updated):
    planes, row_count, col_count = updated.shape
    return updated.reshape(planes, row_count // 3, 3, col_count // 3, 3).sum(axis=(2, 4)) / 9.0


def local_general(strips, anchor, wet_mask, bathy_index, bed_levels, coarse):
    tile_blocks = strips.shape[2]
    band_rows = strips.shape[4]
    full_cols = strips.shape[5]
    columns = lax.axis_size("col")
    tile_cols = full_cols // columns
    layered = (
        strips[0, :, :, 0]
        .reshape(3, tile_blocks, band_rows, columns, tile_cols)
        .transpose(0, 1, 3, 2, 4)
    )
    flattened = layered.reshape(3, tile_blocks * columns, band_rows, tile_cols)
    arrived = lax.all_to_all(flattened, ("row", "col"), split_axis=1, concat_axis=1, tiled=True)
    fields = arrived.reshape(3, tile_blocks * columns * band_rows, tile_cols)
    bed_fine = expand(lookup(bathy_index[0], bed_levels))
    wetness = expand(wet_mask[0].astype(F32))
    stacked = jnp.concatenate([fields, bed_fine[None], wetness[None]], axis=0)
    padded_all = padded_2(stacked, (("row", 1), ("col", 2)), 1)
    updated = advance(padded_all[:3], padded_all[3], padded_all[4])
    restricted = restrict(updated)
    coarse_rows = restricted.shape[1]
    coarse_cols = restricted.shape[2]
    contribution = jnp.concatenate(
        [restricted, jnp.ones((1, coarse_rows, coarse_cols), F32)], axis=0
    )
    nest_index = lax.axis_index("nest")
    corner = lax.dynamic_index_in_dim(anchor, nest_index, 0, keepdims=False)
    canvas = lax.dynamic_update_slice(
        jnp.zeros((4, 2 * coarse_rows, 2 * coarse_cols), F32),
        contribution,
        (jnp.int32(0), corner[0], corner[1]),
    )
    spilled = passed_along(canvas[:, :, coarse_cols:], "col", 1)
    merged = canvas[:, :, :coarse_cols] + spilled
    lowered = passed_along(merged[:, coarse_rows:], ("nest", "row"), 1)
    received_sum = merged[:, :coarse_rows] + lowered
    coarse_next = (coarse + received_sum[:3]) / (1.0 + received_sum[3])
    return (updated[None], coarse_next)


def half_rows(row):
    return pltpu.roll(row, 64, 1), row


def from_half_rows(block, at, lane):
    upper = block[at : at + 1]
    return jnp.where(lane < 64, pltpu.roll(upper, 64, 1), block[at + 1 : at + 2])


def pack_body(dims, ds, after, strips_hbm, wet_hbm, class_hbm, levels_hbm, *rest):
    blocks, band, columns, lane_blocks = dims
    rest = rest[after:]
    outs = rest[: len(ds)]
    strips, wet_ref, class_ref, levels_ref, sems, small = rest[len(ds) :]
    tile_cols = lane_blocks * 128
    me = lax.axis_index(("row", "col")).astype(jnp.int32)
    my_row = me // columns
    my_col = me % columns
    loads = [
        pltpu.make_async_copy(wet_hbm, wet_ref, small.at[0]),
        pltpu.make_async_copy(class_hbm, class_ref, small.at[1]),
        pltpu.make_async_copy(levels_hbm, levels_ref, small.at[2]),
    ]
    for c in loads:
        c.start()
    copies = []
    for r in range(blocks):
        j = my_row ^ (r ^ (ds[0] // columns))
        copies.append(
            pltpu.make_async_copy(strips_hbm.at[0, :, j, 0], strips.at[:, j], sems.at[r])
        )
    for c in copies:
        c.start()
    lane = lax.broadcasted_iota(jnp.int32, (8, 128), 1)
    sub = lax.broadcasted_iota(jnp.int32, (8, 128), 0)
    size = wet_ref.shape[1]
    diag = lax.broadcasted_iota(jnp.int32, (size, 128), 0) == lax.broadcasted_iota(
        jnp.int32, (size, 128), 1
    )
    for c in loads:
        c.wait()
    edges = []
    for ref in (wet_ref, class_ref):
        cells = ref[0].astype(F32)
        north = cells[0:1]
        south = cells[size - 1 : size]
        west = jnp.sum(jnp.where(diag, cells[:, 0:1], 0.0), axis=0, keepdims=True)
        east = jnp.sum(jnp.where(diag, cells[:, 127:128], 0.0), axis=0, keepdims=True)
        four = (north, south, west, east)
        if ref is class_ref:
            four = tuple(level_of(row, levels_ref) for row in four)
        edges.append(four)
    first = me == 0
    for c in copies:
        c.wait()
    for out, d in zip(outs, ds):
        to = me ^ d
        j = to // columns
        c = to % columns
        base = pl.multiple_of(c * tile_cols, 128)
        for k in range(3):
            for q in range(lane_blocks):
                at = (k * lane_blocks + q) * band
                out[at : at + band] = strips[k, j, :, pl.ds(pl.multiple_of(base + q * 128, 128), 128)]
        at = 3 * lane_blocks * band
        west_at = pl.multiple_of(jnp.maximum(base - 128, 0), 128)
        east_at = pl.multiple_of(jnp.where(c == columns - 1, base, base + tile_cols), 128)
        mixed = jnp.zeros((8, 128), F32)
        for g in range(band // 8):
            for k in range(3):
                i = g * 3 + k
                west = strips[k, j, g * 8 : g * 8 + 8, pl.ds(west_at, 128)]
                east = strips[k, j, g * 8 : g * 8 + 8, pl.ds(east_at, 128)]
                both = pltpu.roll(jnp.where(lane == 127, west, east), 2 * i + 1, 1)
                mixed = jnp.where((lane == 2 * i) | (lane == 2 * i + 1), both, mixed)
        jj = jnp.clip(jnp.where(first, j + 1, j - 1), 0, blocks - 1)
        rows = []
        for k in range(3):
            for q in range(lane_blocks):
                spot = pl.ds(pl.multiple_of(base + q * 128, 128), 128)
                head = strips[k, jj, 0:8, spot][0:1]
                tail = strips[k, jj, band - 8 : band, spot][7:8]
                rows.append(jnp.where(first, head, tail))
        halo = jnp.zeros((8, 128), F32)
        for i in range(8):
            halo = jnp.where(sub == i, rows[i], halo)
        out[at : at + 8] = halo
        tucked = [rows[8]]
        for north, south, west, east in edges:
            row = jnp.where(
                c == my_col,
                jnp.where(j > my_row, south, north),
                jnp.where(c > my_col, east, west),
            )
            tucked.append(row)
        for n, row in enumerate(tucked):
            low, high = half_rows(row)
            mixed = jnp.where((sub == 2 * n) & (lane >= 64), low, mixed)
            mixed = jnp.where((sub == 2 * n + 1) & (lane >= 64), high, mixed)
        out[at + 8 : at + 16] = mixed


def spread(rows, cols, width, offset=None):
    i = lax.broadcasted_iota(jnp.int32, (rows, cols), 0)
    m = lax.broadcasted_iota(jnp.int32, (rows, cols), 1)
    if offset is not None:
        m = m - offset
        m = jnp.where(m < 0, m + cols, m)
    low = m * width
    return jnp.where((i >= low) & (i < low + width), 1.0, 0.0)


def spread_t(rows, cols, width, offset=None):
    m = lax.broadcasted_iota(jnp.int32, (rows, cols), 0)
    i = lax.broadcasted_iota(jnp.int32, (rows, cols), 1)
    if offset is not None:
        m = m - offset
        m = jnp.where(m < 0, m + rows, m)
    low = m * width
    return jnp.where((i >= low) & (i < low + width), 1.0, 0.0)


def level_of(classes, levels_ref):
    out = jnp.zeros_like(classes)
    for n in range(levels_ref.shape[0]):
        out = jnp.where(classes == n, levels_ref[n], out)
    return out


def prep_body(columns, levels_ref, anchor_ref, wet_ref, class_ref, wet_out, bed_out, weights):
    lane_blocks, rows, _ = wet_out.shape
    size, width = wet_ref.shape[1], wet_ref.shape[2]
    wet = wet_ref[0].astype(F32)
    bed = level_of(class_ref[0].astype(F32), levels_ref)
    across = spread_t(width, lane_blocks * 128, 3)
    down = spread(rows, size, 3)
    for out, cells, parts in ((wet_out, wet, 1), (bed_out, bed, 3)):
        fine = mul_left(down, mul_right(cells, across, parts), parts)
        for q in range(lane_blocks):
            out[q] = fine[:, q * 128 : q * 128 + 128]
    nest = lax.axis_index("nest").astype(jnp.int32)
    row_at = lax.axis_index("row").astype(jnp.int32)
    col_at = lax.axis_index("col").astype(jnp.int32)
    up_nest = jnp.where(row_at == 0, jnp.maximum(nest - 1, 0), nest)
    i = lax.broadcasted_iota(jnp.int32, weights.shape[1:], 0)
    m = lax.broadcasted_iota(jnp.int32, weights.shape[1:], 1)
    has_left = jnp.where(col_at > 0, 1.0, 0.0)
    has_up = jnp.where((row_at > 0) | (nest > 0), 1.0, 0.0)
    own_rows = jnp.where(i >= anchor_ref[nest, 0], 1.0, 0.0)
    up_rows = jnp.where(i < anchor_ref[up_nest, 0], has_up, 0.0)
    own_cols = m >= anchor_ref[nest, 1]
    up_cols = m >= anchor_ref[up_nest, 1]
    shares = (
        jnp.where(own_cols, own_rows, 0.0),
        jnp.where(own_cols, 0.0, own_rows * has_left),
        jnp.where(up_cols, up_rows, 0.0),
        jnp.where(up_cols, 0.0, up_rows * has_left),
    )
    scale = 1.0 / (1.0 + shares[0] + shares[1] + shares[2] + shares[3])
    weights[0] = scale
    for n, share in enumerate(shares):
        weights[n + 1] = share * scale


def split(x, parts):
    out = []
    for n in range(parts):
        piece = x.astype(jnp.bfloat16)
        out.append(piece)
        if n + 1 < parts:
            x = x - piece.astype(F32)
    return out


def mul_left(matrix, x, parts):
    matrix = matrix.astype(jnp.bfloat16)
    return sum(jnp.dot(matrix, piece, preferred_element_type=F32) for piece in split(x, parts))


def mul_right(x, matrix, parts):
    matrix = matrix.astype(jnp.bfloat16)
    return sum(jnp.dot(piece, matrix, preferred_element_type=F32) for piece in split(x, parts))


def mul_left_t(matrix, x, parts):
    matrix = matrix.astype(jnp.bfloat16)
    return sum(
        lax.dot_general(matrix, piece, (((1,), (1,)), ((), ())), preferred_element_type=F32)
        for piece in split(x, parts)
    )


def unpack(dims, me, first_row, messages, ds, field, extra):
    blocks, band, columns, lane_blocks = dims
    body_rows = 3 * lane_blocks * band
    for message, d in zip(messages, ds):
        p = me ^ d
        top = pl.multiple_of(8 + p * band - first_row, 8)
        mixed = message[body_rows + 8 : body_rows + 16]
        for k in range(3):
            for q in range(lane_blocks):
                n = k * lane_blocks + q
                field[k, q, pl.ds(top, band)] = message[
                    n * band : n * band + band
                ]
            for g in range(band // 8):
                i = g * 3 + k
                at = pl.multiple_of(top + g * 8, 8)
                field[k, lane_blocks, pl.ds(at, 8)] = pltpu.roll(mixed, 127 - 2 * i, 1)
        extra[p] = message[body_rows : body_rows + 16]


def edge_rows(dims, extra, source, inside):
    blocks, band, columns, lane_blocks = dims
    lane = lax.broadcasted_iota(jnp.int32, (1, 128), 1)
    block = extra[jnp.where(inside, source, 0), 8:16]
    wet_row = from_half_rows(block, 2, lane)
    bed_row = from_half_rows(block, 4, lane)
    return jnp.where(inside, wet_row, 0.0), jnp.where(inside, bed_row, 0.0)


def side_cells(dims, me, extra, wet_side, bed_side):
    columns = dims[2]
    my_col = me % columns
    west = edge_rows(dims, extra, me - 1, my_col > 0)
    east = edge_rows(dims, extra, me + 1, my_col < columns - 1)
    sub = lax.broadcasted_iota(jnp.int32, (128, 128), 0)
    pair = jnp.zeros((128, 128), F32)
    for n, row in ((0, east[0]), (127, west[0]), (64, east[1]), (63, west[1])):
        pair = jnp.where(sub == n, row, pair)
    sides = mul_left_t(spread(wet_side.shape[0], 128, 3), pair, 3)
    wet_side[...] = sides
    bed_side[...] = pltpu.roll(sides, 64, 1)


def slopes(lane_blocks, wet, bed, wet_side, bed_side, open_x, slope_x, rows):
    lane = lax.broadcasted_iota(jnp.int32, (8, 128), 1)
    sides = lane_blocks + 1

    def step(t, _):
        at = pl.ds(pl.multiple_of(t * 8, 8), 8)
        w = [wet[q, at] for q in range(lane_blocks)] + [wet_side[at]]
        z = [bed[q, at] for q in range(lane_blocks)] + [bed_side[at]]
        steps = []
        for q in range(sides):
            w2, z2 = (
                pltpu.roll(jnp.where(lane == 0, x[(q + 1) % sides], x[q]), 127, 1) for x in (w, z)
            )
            half = (0.5 * courant) * (w[q] * w2)
            open_x[q, at] = half
            steps.append(half * (z2 - z[q]))
        for q in range(lane_blocks):
            left = pltpu.roll(jnp.where(lane == 127, steps[q - 1], steps[q]), 1, 1)
            slope_x[q, at] = gravity * (steps[q] + left)
        return 0

    lax.fori_loop(0, rows // 8, step, 0, unroll=2)


def sweep(dims, field, wet, bed, wet_at, open_x, slope_x, open_at, more, made, start, count, unroll):
    lane_blocks = dims[3]
    sides = lane_blocks + 1
    lane = lax.broadcasted_iota(jnp.int32, (8, 128), 1)
    sub = lax.broadcasted_iota(jnp.int32, (8, 128), 0)

    def rates(h, hu, hv):
        root = lax.rsqrt(h)
        inv = root * root
        u = hu * inv
        c = (gravity**0.5) * (h * root)
        p = (0.5 * gravity) * (h * h)
        return hu * u + p, hv * u, jnp.abs(u) + c, inv, c, p

    def cells(group, q):
        at = pl.ds(pl.multiple_of(8 + group * 8, 8), 8)
        h, hu, hv = (field[k, q, at] for k in range(3))
        f2, m, a, inv, c, p = rates(h, hu, hv)
        if q < lane_blocks:
            v = hv * inv
            more[0, q, at] = m
            more[1, q, at] = hv * v + p
            more[2, q, at] = jnp.abs(v) + c
        return h, hu, hv, f2, m, a

    def face(half, near, far):
        bound = half * jnp.maximum(near[6], far[6])
        return [half * (near[3 + k] + far[3 + k]) - bound * (far[k] - near[k]) for k in range(3)]

    def across(t, _):
        group = start + t
        spot = pl.ds(pl.multiple_of(group * 8, 8), 8)
        opened = pl.ds(pl.multiple_of(open_at + group * 8, 8), 8)
        blocks = [cells(group, q) for q in range(sides)]
        faces = []
        for q in range(sides):
            now, nxt = blocks[q], blocks[(q + 1) % sides]
            h, hu, hv, f2, m, a = now
            h2, hu2, hv2 = (
                pltpu.roll(jnp.where(lane == 0, y, x), 127, 1) for x, y in zip(now[:3], nxt[:3])
            )
            f22, m2, a2 = rates(h2, hu2, hv2)[:3]
            faces.append(
                face(open_x[q, opened], (h, hu, hv, hu, f2, m, a), (h2, hu2, hv2, hu2, f22, m2, a2))
            )
        for q in range(lane_blocks):
            right = faces[q]
            left = [
                pltpu.roll(jnp.where(lane == 127, y, x), 1, 1) for x, y in zip(right, faces[q - 1])
            ]
            h, hu, hv = blocks[q][:3]
            made[0, q, spot] = h - (right[0] - left[0])
            made[1, q, spot] = hu - (right[1] - left[1]) - h * slope_x[q, opened]
            made[2, q, spot] = hv - (right[2] - left[2])
        return 0

    def south_face(group, q):
        at = pl.multiple_of(8 + group * 8, 8)
        w_at = pl.multiple_of(wet_at + group * 8, 8)
        sides = []
        for step in range(2):
            rows = pl.ds(at + step, 8)
            h, hu, hv = (field[k, q, rows] for k in range(3))
            m, g3, b = (more[k, q, rows] for k in range(3))
            sides.append((h, hu, hv, hv, m, g3, b))
        half = (0.5 * courant) * (wet[q, pl.ds(w_at, 8)] * wet[q, pl.ds(w_at + 1, 8)])
        slope = half * (bed[q, pl.ds(w_at + 1, 8)] - bed[q, pl.ds(w_at, 8)])
        return face(half, *sides) + [slope]

    def down(t, above):
        group = start + t
        spot = pl.ds(pl.multiple_of(group * 8, 8), 8)
        new = []
        for q in range(lane_blocks):
            below = south_face(group, q)
            up = [
                pltpu.roll(jnp.where(sub == 7, y, x), 1, 0) for x, y in zip(below, above[q])
            ]
            h = field[0, q, pl.ds(pl.multiple_of(8 + group * 8, 8), 8)]
            made[0, q, spot] = made[0, q, spot] - (below[0] - up[0])
            made[1, q, spot] = made[1, q, spot] - (below[1] - up[1])
            made[2, q, spot] = (
                made[2, q, spot] - (below[2] - up[2]) - gravity * h * (below[3] + up[3])
            )
            new.append(below)
        return new

    for q in range(lane_blocks):
        cells(start - 1, q)
        cells(start + count, q)
    if count == 1:
        across(0, 0)
        down(0, [south_face(start - 1, q) for q in range(lane_blocks)])
    else:
        lax.fori_loop(0, count, across, 0, unroll=unroll)
        above = [south_face(start - 1, q) for q in range(lane_blocks)]
        lax.fori_loop(0, count, down, above, unroll=unroll)


def half_body(dims, ds, wet_in, bed_in, *rest):
    blocks, band, columns, lane_blocks = dims
    owners = blocks * columns
    messages = rest[: len(ds)]
    made, open_x, slope_x, field, wet_side, bed_side, more, extra = rest[len(ds) :]
    rows = owners * band // 2
    me = lax.axis_index(("row", "col")).astype(jnp.int32)
    first_row = pl.multiple_of((me * 2 // owners) * rows, 8)
    unpack(dims, me, first_row, messages, ds, field, extra)
    side_cells(dims, me, extra, wet_side, bed_side)
    slopes(lane_blocks, wet_in, bed_in, wet_side, bed_side, open_x, slope_x, 2 * rows)
    for k in range(3):
        for q in range(lane_blocks):
            made[k, q, 0:8] = jnp.zeros((8, 128), F32)
            made[k, q, rows - 8 : rows] = jnp.zeros((8, 128), F32)
    sweep(
        dims, field, wet_in, bed_in, first_row, open_x, slope_x, first_row, more, made, 1, rows // 8 - 2, 2
    )


def main_body(dims, ds, anchor_hbm, wet_in, bed_in, half_in, open_x, slope_x, *rest):
    blocks, band, columns, lane_blocks = dims
    owners = blocks * columns
    messages = rest[:owners]
    fine_out, rolled_out = rest[owners : owners + 2]
    field, wet, bed, more, extra, made, anchor_ref, sem_in, sem_out = rest[owners + 2 :]
    rows = owners * band
    cols = lane_blocks * 128
    me = lax.axis_index(("row", "col")).astype(jnp.int32)
    nest = lax.axis_index("nest").astype(jnp.int32)
    my_row = me // columns
    done_half = me * 2 // owners
    half_rows_at = pl.multiple_of(done_half * (rows // 2), 8)
    corners = pltpu.make_async_copy(anchor_hbm, anchor_ref, sem_in)
    corners.start()

    def fine_copy(source, count, at, n):
        return pltpu.make_async_copy(
            source, fine_out.at[0, :, pl.ds(at, count), pl.ds((n % lane_blocks) * 128, 128)], sem_out.at[n]
        )

    inner = rows // 2 - 16
    done = [
        fine_copy(half_in.at[:, q, pl.ds(8, inner)], inner, pl.multiple_of(half_rows_at + 8, 8), q)
        for q in range(lane_blocks)
    ]
    for c in done:
        c.start()
    for k in range(3):
        for q in range(lane_blocks):
            made[k, q, pl.ds(half_rows_at, rows // 2)] = half_in[k, q]
    lane1 = lax.broadcasted_iota(jnp.int32, (1, 128), 1)
    for q in range(lane_blocks):
        wet[q, 8 : 8 + rows] = wet_in[q]
        bed[q, 8 : 8 + rows] = bed_in[q]
    unpack(dims, me, 0, messages, ds, field, extra)

    for source, at in ((owners - 1, 0), (0, 8 + rows)):
        last = from_half_rows(extra[source, 8:16], 0, lane1)
        for k in range(3):
            for q in range(lane_blocks):
                n = k * lane_blocks + q
                row = last if n == 8 else extra[source, n : n + 1]
                field[k, q, at : at + 8] = jnp.broadcast_to(row, (8, 128))
    north = edge_rows(dims, extra, me - columns, my_row > 0)
    south = edge_rows(dims, extra, me + columns, my_row < blocks - 1)
    sub8 = lax.broadcasted_iota(jnp.int32, (8, 128), 0)
    stack = jnp.zeros((8, 128), F32)
    for n, row in enumerate((north[0], north[1], south[0], south[1])):
        stack = jnp.where(sub8 == n, row, stack)
    ends = mul_right(stack, spread_t(128, cols, 3), 3)
    for n, (ref, at) in enumerate(((wet, 0), (bed, 0), (wet, 8 + rows), (bed, 8 + rows))):
        for q in range(lane_blocks):
            ref[q, at : at + 8] = jnp.broadcast_to(ends[n : n + 1, q * 128 : q * 128 + 128], (8, 128))

    groups = rows // 8
    one = done_half * (groups - 1)
    along = (dims, field, wet, bed, 8, open_x, slope_x, 0, more, made)
    sweep(*along, one, 1, 1)
    many = (1 - done_half) * (groups // 2 - 1)
    sweep(*along, many, groups // 2 + 1, 5)
    late = []
    for n, (group, count) in enumerate(((one, 8), (many, rows // 2 + 8)), 1):
        at = pl.multiple_of(group * 8, 8)
        for q in range(lane_blocks):
            late.append(fine_copy(made.at[:, q, pl.ds(at, count)], count, at, n * lane_blocks + q))
    for c in late:
        c.start()
    corners.wait()
    coarse_rows = rows // 3
    coarse_cols = cols // 3
    a0 = anchor_ref[nest, 0]
    a1 = anchor_ref[nest, 1]
    gather_cols = spread(cols, coarse_cols, 3, a1)
    for k in range(3):
        total = jnp.concatenate(
            [
                sum(made[k, q, pl.ds(n, coarse_rows, stride=3), :] for n in range(3))
                for q in range(lane_blocks)
            ],
            axis=1,
        )
        mean = mul_right(total, gather_cols, 2) * (1.0 / 9.0)
        rolled_out[k] = pltpu.roll(mean, a0, 0)
    for c in done + late:
        c.wait()


def finish_body(coarse, weights, up, left, diagonal, own, out):
    for k in range(3):
        out[k] = (
            coarse[k] * weights[0]
            + own[k] * weights[1]
            + left[k] * weights[2]
            + up[k] * weights[3]
            + diagonal[k] * weights[4]
        )


def in_vmem(x):
    return pltpu.with_memory_space_constraint(x, pltpu.VMEM)


def in_hbm(x):
    return pltpu.with_memory_space_constraint(x, pltpu.HBM)


SMEM = pl.BlockSpec(memory_space=pltpu.SMEM)
VMEM = pl.BlockSpec(memory_space=pltpu.VMEM)
HBM = pl.BlockSpec(memory_space=pltpu.HBM)


def half_call(dims, ds, wet_fine, bed_fine, messages):
    blocks, band, columns, lane_blocks = dims
    owners = blocks * columns
    rows = owners * band // 2
    return pl.pallas_call(
        lambda *refs: half_body(dims, ds, *refs),
        in_specs=[VMEM, VMEM] + [VMEM] * len(ds),
        out_specs=[VMEM] * 3,
        out_shape=[
            pltpu.VMEM((3, lane_blocks, rows, 128), F32),
            pltpu.VMEM((lane_blocks + 1, 2 * rows, 128), F32),
            pltpu.VMEM((lane_blocks, 2 * rows, 128), F32),
        ],
        scratch_shapes=[
            pltpu.VMEM((3, lane_blocks + 1, rows + 16, 128), F32),
            pltpu.VMEM((2 * rows, 128), F32),
            pltpu.VMEM((2 * rows, 128), F32),
            pltpu.VMEM((3, lane_blocks, rows + 16, 128), F32),
            pltpu.VMEM((owners, 16, 128), F32),
        ],
        name="half", compiler_params=pltpu.CompilerParams(vmem_limit_bytes=12 << 20),
    )(wet_fine, bed_fine, *messages)


def main_call(dims, ds, anchor, wet_fine, bed_fine, half, open_x, slope_x, messages):
    blocks, band, columns, lane_blocks = dims
    owners = blocks * columns
    rows = owners * band
    cols = lane_blocks * 128
    return pl.pallas_call(
        lambda *refs: main_body(dims, ds, *refs),
        in_specs=[HBM] + [VMEM] * (5 + owners),
        out_specs=[HBM, VMEM],
        out_shape=[
            jax.ShapeDtypeStruct((1, 3, rows, cols), F32),
            pltpu.VMEM((3, rows // 3, cols // 3), F32),
        ],
        scratch_shapes=[
            pltpu.VMEM((3, lane_blocks + 1, rows + 16, 128), F32),
            pltpu.VMEM((lane_blocks, rows + 16, 128), F32),
            pltpu.VMEM((lane_blocks, rows + 16, 128), F32),
            pltpu.VMEM((3, lane_blocks, rows + 16, 128), F32),
            pltpu.VMEM((owners, 16, 128), F32),
            pltpu.VMEM((3, lane_blocks, rows, 128), F32),
            pltpu.SMEM((2, 2), jnp.int32),
            pltpu.SemaphoreType.DMA,
            pltpu.SemaphoreType.DMA((3 * lane_blocks,)),
        ],
        name="main", compiler_params=pltpu.CompilerParams(vmem_limit_bytes=20 << 20),
    )(anchor, wet_fine, bed_fine, half, open_x, slope_x, *messages)


def local_packed(strips, anchor, wet_mask, bathy_index, bed_levels, coarse):
    blocks, band, full_cols = strips.shape[2], strips.shape[4], strips.shape[5]
    columns = lax.axis_size("col")
    owners = blocks * columns
    cols = full_cols // columns
    lane_blocks = cols // 128
    rows = owners * band
    dims = (blocks, band, columns, lane_blocks)
    height = 3 * lane_blocks * band + 16
    half_owners = owners // 2
    messages = []
    for ds in (range(half_owners), range(half_owners, owners)):
        made = pl.pallas_call(
            lambda *refs, ds=ds, after=len(messages[:1]): pack_body(dims, ds, after, *refs),
            in_specs=[HBM] * 4 + [VMEM] * len(messages[:1]),
            out_specs=[VMEM] * half_owners,
            out_shape=[pltpu.VMEM((height, 128), F32)] * half_owners,
            scratch_shapes=[
                pltpu.VMEM((3, blocks, band, full_cols), F32),
                pltpu.VMEM(wet_mask.shape, jnp.int32),
                pltpu.VMEM(bathy_index.shape, jnp.int32),
                pltpu.SMEM(bed_levels.shape, F32),
                pltpu.SemaphoreType.DMA((blocks,)),
                pltpu.SemaphoreType.DMA((3,)),
            ],
            name="pack", compiler_params=pltpu.CompilerParams(vmem_limit_bytes=10 << 20),
        )(
            in_hbm(strips),
            in_hbm(wet_mask),
            in_hbm(bathy_index),
            in_hbm(bed_levels),
            *messages[:1],
        )
        messages += [in_vmem(x) for x in made]

    def rank(d):
        r, c = d // columns, d % columns
        return (d >= half_owners, c * 2 < columns, r, c)

    wanted = sorted(range(1, owners), key=rank)
    arrived = {
        d: lax.ppermute(messages[d], ("row", "col"), [(i, i ^ d) for i in range(owners)])
        for d in wanted
    }
    arrived[0] = messages[0]
    arrived = {d: in_vmem(x) if d else x for d, x in arrived.items()}

    coarse_rows = rows // 3
    coarse_cols = cols // 3
    wet_fine, bed_fine, weights = pl.pallas_call(
        lambda *refs: prep_body(columns, *refs),
        in_specs=[SMEM, SMEM, VMEM, VMEM],
        out_specs=[VMEM] * 3,
        out_shape=[pltpu.VMEM((lane_blocks, rows, 128), F32)] * 2
        + [pltpu.VMEM((5, coarse_rows, coarse_cols), F32)],
        name="prep", compiler_params=pltpu.CompilerParams(vmem_limit_bytes=12 << 20),
    )(bed_levels, anchor, wet_mask, bathy_index)

    early = [0] + wanted[: half_owners - 1]
    order = [0] + wanted
    wet_fine, bed_fine, weights = in_vmem(wet_fine), in_vmem(bed_fine), in_vmem(weights)
    half, open_x, slope_x = half_call(dims, early, wet_fine, bed_fine, [arrived[d] for d in early])
    half, open_x, slope_x = in_vmem(half), in_vmem(open_x), in_vmem(slope_x)
    fine, rolled = main_call(
        dims,
        order,
        in_hbm(anchor),
        wet_fine,
        bed_fine,
        half,
        open_x,
        slope_x,
        [arrived[d] for d in order],
    )
    rolled = in_vmem(rolled)

    lines = lax.axis_size("nest") * lax.axis_size("row")
    rights = [(c, c + 1) for c in range(columns - 1)]
    downs = [(l, l + 1) for l in range(lines - 1)]
    both = [(l * columns + c, l2 * columns + c2) for l, l2 in downs for c, c2 in rights]
    diagonal = lax.ppermute(rolled, ("nest", "row", "col"), both)
    from_left = lax.ppermute(rolled, "col", rights)
    from_up = lax.ppermute(rolled, ("nest", "row"), downs)

    coarse_next = pl.pallas_call(
        finish_body,
        in_specs=[VMEM] * 6,
        out_specs=VMEM,
        out_shape=jax.ShapeDtypeStruct(coarse.shape, F32),
        name="finish", compiler_params=pltpu.CompilerParams(vmem_limit_bytes=4 << 20),
    )(
        in_vmem(coarse),
        weights,
        in_vmem(from_up),
        in_vmem(from_left),
        in_vmem(diagonal),
        rolled,
    )
    return (fine, coarse_next)


def local(strips, anchor, wet_mask, bathy_index, bed_levels, coarse):
    columns = lax.axis_size("col")
    owners = strips.shape[2] * columns
    cols = strips.shape[5] // columns
    band = strips.shape[4]
    fits = (
        owners & (owners - 1) == 0
        and 2 <= owners <= 16
        and strips.shape[2] == lax.axis_size("row")
        and band == 24
        and cols == 384
        and owners * band == 384
        and wet_mask.shape[1:] == (128, 128)
    )
    run = local_packed if fits else local_general
    return run(strips, anchor, wet_mask, bathy_index, bed_levels, coarse)


def solution(mesh):
    return jax.shard_map(
        local,
        mesh=mesh,
        in_specs=(
            P("nest", None, None, ("row", "col"), None, None),
            P(),
            P("nest", "row", "col"),
            P("nest", "row", "col"),
            P(),
            P(None, ("nest", "row"), "col"),
        ),
        out_specs=(P("nest", None, "row", "col"), P(None, ("nest", "row"), "col")),
        check_vma=False,
    )
```

```python
import jax
import jax.numpy as jnp
from jax import lax
from jax.experimental import pallas as pl
from jax.experimental.pallas import tpu as pltpu
from jax.sharding import PartitionSpec as P


gravity = 1.0
courant = 0.2
F32 = jnp.float32


def padded_2(cells, sides, width):
    for axis, dim in sides:
        count = lax.axis_size(axis)
        ends = count - 1
        head = lax.slice_in_dim(cells, 0, width, axis=dim)
        tail = lax.slice_in_dim(cells, cells.shape[dim] - width, cells.shape[dim], axis=dim)
        cells = jnp.concatenate(
            [
                lax.ppermute(tail, axis, [(i, (i + 1) % count) for i in range(ends)]),
                cells,
                lax.ppermute(head, axis, [((i + 1) % count, i) for i in range(ends)]),
            ],
            axis=dim,
        )
    return cells


def passed_along(block, axis, distance):
    devices = range(lax.axis_size(axis))
    route = [(i - distance, i) for i in devices if i - distance in devices]
    return lax.ppermute(block, axis, route)


def advance(padded, bed_pad, wet_pad):
    depth_now = padded[0]
    flow_u = padded[1]
    flow_v = padded[2]
    depth_safe = jnp.where(wet_pad > 0.5, depth_now, 1.0)
    speed_u = flow_u / depth_safe
    speed_v = flow_v / depth_safe
    celerity = jnp.sqrt(gravity * depth_safe)
    pressure = 0.5 * gravity * depth_safe * depth_safe
    fluxes_x = (flow_u, flow_u * speed_u + pressure, flow_v * speed_u)
    fluxes_y = (flow_v, flow_u * speed_v, flow_v * speed_v + pressure)
    reach_x = jnp.abs(speed_u) + celerity
    reach_y = jnp.abs(speed_v) + celerity
    open_x = wet_pad[1:-1, :-1] * wet_pad[1:-1, 1:]
    open_y = wet_pad[:-1, 1:-1] * wet_pad[1:, 1:-1]
    bound_x = jnp.maximum(reach_x[1:-1, :-1], reach_x[1:-1, 1:])
    bound_y = jnp.maximum(reach_y[:-1, 1:-1], reach_y[1:, 1:-1])
    slope_x = (bed_pad[1:-1, 1:] - bed_pad[1:-1, :-1]) * open_x
    slope_y = (bed_pad[1:, 1:-1] - bed_pad[:-1, 1:-1]) * open_y
    centre = depth_now[1:-1, 1:-1]
    sources = (
        None,
        -0.5 * gravity * centre * (slope_x[:, 1:] + slope_x[:, :-1]),
        -0.5 * gravity * centre * (slope_y[1:] + slope_y[:-1]),
    )
    results = []
    for plane in range(3):
        state = padded[plane]
        flux_col = fluxes_x[plane]
        flux_row = fluxes_y[plane]
        face_x = (
            0.5 * (flux_col[1:-1, :-1] + flux_col[1:-1, 1:])
            - 0.5 * bound_x * (state[1:-1, 1:] - state[1:-1, :-1])
        ) * open_x
        face_y = (
            0.5 * (flux_row[:-1, 1:-1] + flux_row[1:, 1:-1])
            - 0.5 * bound_y * (state[1:, 1:-1] - state[:-1, 1:-1])
        ) * open_y
        value = (
            state[1:-1, 1:-1]
            - courant * (face_x[:, 1:] - face_x[:, :-1])
            - courant * (face_y[1:] - face_y[:-1])
        )
        if plane > 0:
            value = value + courant * sources[plane]
        results.append(value)
    return jnp.stack(results)


def expand(cells):
    return jnp.repeat(jnp.repeat(cells, 3, axis=-2), 3, axis=-1)


def lookup(classes, levels):
    ladder = jnp.arange(levels.shape[0], dtype=jnp.int32)
    matches = classes[None] == ladder[:, None, None]
    return jnp.sum(jnp.where(matches, levels[:, None, None], 0.0), axis=0)


def restrict(updated):
    planes, row_count, col_count = updated.shape
    return updated.reshape(planes, row_count // 3, 3, col_count // 3, 3).sum(axis=(2, 4)) / 9.0


def local_general(strips, anchor, wet_mask, bathy_index, bed_levels, coarse):
    tile_blocks = strips.shape[2]
    band_rows = strips.shape[4]
    full_cols = strips.shape[5]
    columns = lax.axis_size("col")
    tile_cols = full_cols // columns
    layered = (
        strips[0, :, :, 0]
        .reshape(3, tile_blocks, band_rows, columns, tile_cols)
        .transpose(0, 1, 3, 2, 4)
    )
    flattened = layered.reshape(3, tile_blocks * columns, band_rows, tile_cols)
    arrived = lax.all_to_all(flattened, ("row", "col"), split_axis=1, concat_axis=1, tiled=True)
    fields = arrived.reshape(3, tile_blocks * columns * band_rows, tile_cols)
    bed_fine = expand(lookup(bathy_index[0], bed_levels))
    wetness = expand(wet_mask[0].astype(F32))
    stacked = jnp.concatenate([fields, bed_fine[None], wetness[None]], axis=0)
    padded_all = padded_2(stacked, (("row", 1), ("col", 2)), 1)
    updated = advance(padded_all[:3], padded_all[3], padded_all[4])
    restricted = restrict(updated)
    coarse_rows = restricted.shape[1]
    coarse_cols = restricted.shape[2]
    contribution = jnp.concatenate(
        [restricted, jnp.ones((1, coarse_rows, coarse_cols), F32)], axis=0
    )
    nest_index = lax.axis_index("nest")
    corner = lax.dynamic_index_in_dim(anchor, nest_index, 0, keepdims=False)
    canvas = lax.dynamic_update_slice(
        jnp.zeros((4, 2 * coarse_rows, 2 * coarse_cols), F32),
        contribution,
        (jnp.int32(0), corner[0], corner[1]),
    )
    spilled = passed_along(canvas[:, :, coarse_cols:], "col", 1)
    merged = canvas[:, :, :coarse_cols] + spilled
    lowered = passed_along(merged[:, coarse_rows:], ("nest", "row"), 1)
    received_sum = merged[:, :coarse_rows] + lowered
    coarse_next = (coarse + received_sum[:3]) / (1.0 + received_sum[3])
    return (updated[None], coarse_next)


def halo_rows(dims, d):
    return d // dims[2] != dims[0] - 1


def message_rows(dims, d):
    blocks, band, columns, lane_blocks = dims
    return 3 * lane_blocks * band + (16 if halo_rows(dims, d) else 8)


def half_rows(row):
    return pltpu.roll(row, 64, 1), row


def from_half_rows(block, at, lane):
    upper = block[at : at + 1]
    return jnp.where(lane < 64, pltpu.roll(upper, 64, 1), block[at + 1 : at + 2])


def pack_body(dims, ds, after, strips_hbm, wet_hbm, class_hbm, levels_hbm, *rest):
    blocks, band, columns, lane_blocks = dims
    rest = rest[after:]
    outs = rest[: len(ds)]
    strips, wet_ref, class_ref, levels_ref, sems, small = rest[len(ds) :]
    tile_cols = lane_blocks * 128
    me = lax.axis_index(("row", "col")).astype(jnp.int32)
    my_row = me // columns
    my_col = me % columns
    loads = [
        pltpu.make_async_copy(wet_hbm, wet_ref, small.at[0]),
        pltpu.make_async_copy(class_hbm, class_ref, small.at[1]),
        pltpu.make_async_copy(levels_hbm, levels_ref, small.at[2]),
    ]
    for c in loads:
        c.start()
    copies = []
    for r in range(blocks):
        j = my_row ^ (r ^ (ds[0] // columns))
        copies.append(
            pltpu.make_async_copy(strips_hbm.at[0, :, j, 0], strips.at[:, j], sems.at[r])
        )
    for c in copies:
        c.start()
    lane = lax.broadcasted_iota(jnp.int32, (8, 128), 1)
    sub = lax.broadcasted_iota(jnp.int32, (8, 128), 0)
    size = wet_ref.shape[1]
    diag = lax.broadcasted_iota(jnp.int32, (size, 128), 0) == lax.broadcasted_iota(
        jnp.int32, (size, 128), 1
    )
    for c in loads:
        c.wait()
    edges = []
    for ref in (wet_ref, class_ref):
        cells = ref[0].astype(F32)
        north = cells[0:1]
        south = cells[size - 1 : size]
        west = jnp.sum(jnp.where(diag, cells[:, 0:1], 0.0), axis=0, keepdims=True)
        east = jnp.sum(jnp.where(diag, cells[:, 127:128], 0.0), axis=0, keepdims=True)
        four = (north, south, west, east)
        if ref is class_ref:
            four = tuple(level_of(row, levels_ref) for row in four)
        edges.append(four)
    first = me == 0
    body_rows = 3 * lane_blocks * band
    waiting = list(copies)
    mixes = []
    for out, d in zip(outs, ds):
        while len(copies) - len(waiting) <= d // columns - ds[0] // columns:
            waiting.pop(0).wait()
        to = me ^ d
        j = to // columns
        c = to % columns
        base = pl.multiple_of(c * tile_cols, 128)
        for k in range(3):
            for q in range(lane_blocks):
                at = (k * lane_blocks + q) * band
                out[at : at + band] = strips[k, j, :, pl.ds(pl.multiple_of(base + q * 128, 128), 128)]
        west_at = pl.multiple_of(jnp.maximum(base - 128, 0), 128)
        east_at = pl.multiple_of(jnp.where(c == columns - 1, base, base + tile_cols), 128)
        mixed = jnp.zeros((8, 128), F32)
        for g in range(band // 8):
            for k in range(3):
                i = g * 3 + k
                west = strips[k, j, g * 8 : g * 8 + 8, pl.ds(west_at, 128)]
                east = strips[k, j, g * 8 : g * 8 + 8, pl.ds(east_at, 128)]
                both = pltpu.roll(jnp.where(lane == 127, west, east), 2 * i + 1, 1)
                mixed = jnp.where((lane == 2 * i) | (lane == 2 * i + 1), both, mixed)
        mixes.append(mixed)
    for c in waiting:
        c.wait()
    for out, d, mixed in zip(outs, ds, mixes):
        to = me ^ d
        j = to // columns
        c = to % columns
        base = pl.multiple_of(c * tile_cols, 128)
        tucked = [jnp.zeros((1, 128), F32)]
        if halo_rows(dims, d):
            jj = jnp.clip(jnp.where(first, j + 1, j - 1), 0, blocks - 1)
            rows = []
            for k in range(3):
                for q in range(lane_blocks):
                    spot = pl.ds(pl.multiple_of(base + q * 128, 128), 128)
                    head = strips[k, jj, 0:8, spot][0:1]
                    tail = strips[k, jj, band - 8 : band, spot][7:8]
                    rows.append(jnp.where(first, head, tail))
            halo = jnp.zeros((8, 128), F32)
            for i in range(8):
                halo = jnp.where(sub == i, rows[i], halo)
            out[body_rows + 8 : body_rows + 16] = halo
            tucked = [rows[8]]
        for north, south, west, east in edges:
            row = jnp.where(
                c == my_col,
                jnp.where(j > my_row, south, north),
                jnp.where(c > my_col, east, west),
            )
            tucked.append(row)
        for n, row in enumerate(tucked):
            low, high = half_rows(row)
            mixed = jnp.where((sub == 2 * n) & (lane >= 64), low, mixed)
            mixed = jnp.where((sub == 2 * n + 1) & (lane >= 64), high, mixed)
        out[body_rows : body_rows + 8] = mixed


def spread(rows, cols, width, offset=None):
    i = lax.broadcasted_iota(jnp.int32, (rows, cols), 0)
    m = lax.broadcasted_iota(jnp.int32, (rows, cols), 1)
    if offset is not None:
        m = m - offset
        m = jnp.where(m < 0, m + cols, m)
    low = m * width
    return jnp.where((i >= low) & (i < low + width), 1.0, 0.0)


def spread_t(rows, cols, width, offset=None):
    m = lax.broadcasted_iota(jnp.int32, (rows, cols), 0)
    i = lax.broadcasted_iota(jnp.int32, (rows, cols), 1)
    if offset is not None:
        m = m - offset
        m = jnp.where(m < 0, m + rows, m)
    low = m * width
    return jnp.where((i >= low) & (i < low + width), 1.0, 0.0)


def level_of(classes, levels_ref):
    out = jnp.zeros_like(classes)
    for n in range(levels_ref.shape[0]):
        out = jnp.where(classes == n, levels_ref[n], out)
    return out


def prep_body(columns, levels_ref, anchor_ref, wet_ref, class_ref, wet_out, bed_out, weights):
    lane_blocks, rows, _ = wet_out.shape
    size, width = wet_ref.shape[1], wet_ref.shape[2]
    wet = wet_ref[0].astype(F32)
    bed = level_of(class_ref[0].astype(F32), levels_ref)
    across = spread_t(width, lane_blocks * 128, 3)
    down = spread(rows, size, 3)
    for out, cells, parts in ((wet_out, wet, 1), (bed_out, bed, 3)):
        fine = mul_left(down, mul_right(cells, across, parts), parts)
        for q in range(lane_blocks):
            out[q] = fine[:, q * 128 : q * 128 + 128]
    nest = lax.axis_index("nest").astype(jnp.int32)
    row_at = lax.axis_index("row").astype(jnp.int32)
    col_at = lax.axis_index("col").astype(jnp.int32)
    up_nest = jnp.where(row_at == 0, jnp.maximum(nest - 1, 0), nest)
    i = lax.broadcasted_iota(jnp.int32, weights.shape[1:], 0)
    m = lax.broadcasted_iota(jnp.int32, weights.shape[1:], 1)
    has_left = jnp.where(col_at > 0, 1.0, 0.0)
    has_up = jnp.where((row_at > 0) | (nest > 0), 1.0, 0.0)
    own_rows = jnp.where(i >= anchor_ref[nest, 0], 1.0, 0.0)
    up_rows = jnp.where(i < anchor_ref[up_nest, 0], has_up, 0.0)
    own_cols = m >= anchor_ref[nest, 1]
    up_cols = m >= anchor_ref[up_nest, 1]
    shares = (
        jnp.where(own_cols, own_rows, 0.0),
        jnp.where(own_cols, 0.0, own_rows * has_left),
        jnp.where(up_cols, up_rows, 0.0),
        jnp.where(up_cols, 0.0, up_rows * has_left),
    )
    scale = 1.0 / (1.0 + shares[0] + shares[1] + shares[2] + shares[3])
    weights[0] = scale
    for n, share in enumerate(shares):
        weights[n + 1] = share * scale


def split(x, parts):
    out = []
    for n in range(parts):
        piece = x.astype(jnp.bfloat16)
        out.append(piece)
        if n + 1 < parts:
            x = x - piece.astype(F32)
    return out


def mul_left(matrix, x, parts):
    matrix = matrix.astype(jnp.bfloat16)
    return sum(jnp.dot(matrix, piece, preferred_element_type=F32) for piece in split(x, parts))


def mul_right(x, matrix, parts):
    matrix = matrix.astype(jnp.bfloat16)
    return sum(jnp.dot(piece, matrix, preferred_element_type=F32) for piece in split(x, parts))


def mul_left_t(matrix, x, parts):
    matrix = matrix.astype(jnp.bfloat16)
    return sum(
        lax.dot_general(matrix, piece, (((1,), (1,)), ((), ())), preferred_element_type=F32)
        for piece in split(x, parts)
    )


def unpack(dims, me, first_row, messages, ds, field, extra):
    blocks, band, columns, lane_blocks = dims
    body_rows = 3 * lane_blocks * band
    for message, d in zip(messages, ds):
        p = me ^ d
        top = pl.multiple_of(8 + p * band - first_row, 8)
        mixed = message[body_rows : body_rows + 8]
        for k in range(3):
            for q in range(lane_blocks):
                n = k * lane_blocks + q
                field[k, q, pl.ds(top, band)] = message[
                    n * band : n * band + band
                ]
            for g in range(band // 8):
                i = g * 3 + k
                at = pl.multiple_of(top + g * 8, 8)
                field[k, lane_blocks, pl.ds(at, 8)] = pltpu.roll(mixed, 127 - 2 * i, 1)
        extra[p, 0:8] = mixed
        if halo_rows(dims, d):
            extra[p, 8:16] = message[body_rows + 8 : body_rows + 16]


def edge_rows(dims, extra, source, inside):
    blocks, band, columns, lane_blocks = dims
    lane = lax.broadcasted_iota(jnp.int32, (1, 128), 1)
    block = extra[jnp.where(inside, source, 0), 0:8]
    wet_row = from_half_rows(block, 2, lane)
    bed_row = from_half_rows(block, 4, lane)
    return jnp.where(inside, wet_row, 0.0), jnp.where(inside, bed_row, 0.0)


def side_cells(dims, me, extra, wet_side, bed_side):
    columns = dims[2]
    my_col = me % columns
    west = edge_rows(dims, extra, me - 1, my_col > 0)
    east = edge_rows(dims, extra, me + 1, my_col < columns - 1)
    sub = lax.broadcasted_iota(jnp.int32, (128, 128), 0)
    pair = jnp.zeros((128, 128), F32)
    for n, row in ((0, east[0]), (127, west[0]), (64, east[1]), (63, west[1])):
        pair = jnp.where(sub == n, row, pair)
    sides = mul_left_t(spread(wet_side.shape[0], 128, 3), pair, 3)
    wet_side[...] = sides
    bed_side[...] = pltpu.roll(sides, 64, 1)


def slopes(lane_blocks, wet, bed, wet_side, bed_side, open_x, slope_x, rows):
    lane = lax.broadcasted_iota(jnp.int32, (8, 128), 1)
    sides = lane_blocks + 1

    def step(t, _):
        at = pl.ds(pl.multiple_of(t * 8, 8), 8)
        w = [wet[q, at] for q in range(lane_blocks)] + [wet_side[at]]
        z = [bed[q, at] for q in range(lane_blocks)] + [bed_side[at]]
        steps = []
        for q in range(sides):
            w2, z2 = (
                pltpu.roll(jnp.where(lane == 0, x[(q + 1) % sides], x[q]), 127, 1) for x in (w, z)
            )
            half = (0.5 * courant) * (w[q] * w2)
            open_x[q, at] = half
            steps.append(half * (z2 - z[q]))
        for q in range(lane_blocks):
            left = pltpu.roll(jnp.where(lane == 127, steps[q - 1], steps[q]), 1, 1)
            slope_x[q, at] = gravity * (steps[q] + left)
        return 0

    lax.fori_loop(0, rows // 8, step, 0, unroll=2)


def sweep(dims, field, wet, bed, wet_at, open_x, slope_x, open_at, more, made, fine, start, count, unroll):
    lane_blocks = dims[3]
    sides = lane_blocks + 1
    lane = lax.broadcasted_iota(jnp.int32, (8, 128), 1)
    sub = lax.broadcasted_iota(jnp.int32, (8, 128), 0)

    def rates(h, hu, hv):
        root = lax.rsqrt(h)
        inv = root * root
        u = hu * inv
        c = (gravity**0.5) * (h * root)
        p = (0.5 * gravity) * (h * h)
        return hu * u + p, hv * u, jnp.abs(u) + c, inv, c, p

    def cells(group, q):
        at = pl.ds(pl.multiple_of(8 + group * 8, 8), 8)
        h, hu, hv = (field[k, q, at] for k in range(3))
        f2, m, a, inv, c, p = rates(h, hu, hv)
        if q < lane_blocks:
            v = hv * inv
            more[0, q, at] = m
            more[1, q, at] = hv * v + p
            more[2, q, at] = jnp.abs(v) + c
        return h, hu, hv, f2, m, a

    def face(half, near, far):
        bound = half * jnp.maximum(near[6], far[6])
        return [half * (near[3 + k] + far[3 + k]) - bound * (far[k] - near[k]) for k in range(3)]

    def across(t, _):
        group = start + t
        spot = pl.ds(pl.multiple_of(group * 8, 8), 8)
        opened = pl.ds(pl.multiple_of(open_at + group * 8, 8), 8)
        blocks = [cells(group, q) for q in range(sides)]
        faces = []
        for q in range(sides):
            now, nxt = blocks[q], blocks[(q + 1) % sides]
            h, hu, hv, f2, m, a = now
            h2, hu2, hv2 = (
                pltpu.roll(jnp.where(lane == 0, y, x), 127, 1) for x, y in zip(now[:3], nxt[:3])
            )
            f22, m2, a2 = rates(h2, hu2, hv2)[:3]
            faces.append(
                face(open_x[q, opened], (h, hu, hv, hu, f2, m, a), (h2, hu2, hv2, hu2, f22, m2, a2))
            )
        for q in range(lane_blocks):
            right = faces[q]
            left = [
                pltpu.roll(jnp.where(lane == 127, y, x), 1, 1) for x, y in zip(right, faces[q - 1])
            ]
            h, hu, hv = blocks[q][:3]
            made[0, q, spot] = h - (right[0] - left[0])
            made[1, q, spot] = hu - (right[1] - left[1]) - h * slope_x[q, opened]
            made[2, q, spot] = hv - (right[2] - left[2])
        return 0

    def south_face(group, q):
        at = pl.multiple_of(8 + group * 8, 8)
        w_at = pl.multiple_of(wet_at + group * 8, 8)
        sides = []
        for step in range(2):
            rows = pl.ds(at + step, 8)
            h, hu, hv = (field[k, q, rows] for k in range(3))
            m, g3, b = (more[k, q, rows] for k in range(3))
            sides.append((h, hu, hv, hv, m, g3, b))
        half = (0.5 * courant) * (wet[q, pl.ds(w_at, 8)] * wet[q, pl.ds(w_at + 1, 8)])
        slope = half * (bed[q, pl.ds(w_at + 1, 8)] - bed[q, pl.ds(w_at, 8)])
        return face(half, *sides) + [slope]

    def down(t, above):
        group = start + t
        spot = pl.ds(pl.multiple_of(group * 8, 8), 8)
        new = []
        for q in range(lane_blocks):
            below = south_face(group, q)
            up = [
                pltpu.roll(jnp.where(sub == 7, y, x), 1, 0) for x, y in zip(below, above[q])
            ]
            h = field[0, q, pl.ds(pl.multiple_of(8 + group * 8, 8), 8)]
            done = [made[k, q, spot] - (below[k] - up[k]) for k in range(3)]
            done[2] = done[2] - gravity * h * (below[3] + up[3])
            for k in range(3):
                made[k, q, spot] = done[k]
                if fine is not None:
                    fine[0, k, spot, q * 128 : q * 128 + 128] = done[k]
            new.append(below)
        return new

    for q in range(lane_blocks):
        cells(start - 1, q)
        cells(start + count, q)
    if count == 1:
        across(0, 0)
        down(0, [south_face(start - 1, q) for q in range(lane_blocks)])
    else:
        lax.fori_loop(0, count, across, 0, unroll=unroll)
        above = [south_face(start - 1, q) for q in range(lane_blocks)]
        lax.fori_loop(0, count, down, above, unroll=unroll)


def half_body(dims, ds, wet_in, bed_in, *rest):
    blocks, band, columns, lane_blocks = dims
    owners = blocks * columns
    messages = rest[: len(ds)]
    made, open_x, slope_x, field, wet_side, bed_side, more, extra = rest[len(ds) :]
    rows = owners * band // 2
    me = lax.axis_index(("row", "col")).astype(jnp.int32)
    first_row = pl.multiple_of((me * 2 // owners) * rows, 8)
    unpack(dims, me, first_row, messages, ds, field, extra)
    side_cells(dims, me, extra, wet_side, bed_side)
    slopes(lane_blocks, wet_in, bed_in, wet_side, bed_side, open_x, slope_x, 2 * rows)
    for k in range(3):
        for q in range(lane_blocks):
            made[k, q, 0:8] = jnp.zeros((8, 128), F32)
            made[k, q, rows - 8 : rows] = jnp.zeros((8, 128), F32)
    sweep(
        dims, field, wet_in, bed_in, first_row, open_x, slope_x, first_row, more, made, None, 1, rows // 8 - 2, 2
    )


def main_body(dims, ds, anchor_hbm, wet_in, bed_in, half_in, open_x, slope_x, *rest):
    blocks, band, columns, lane_blocks = dims
    owners = blocks * columns
    messages = rest[:owners]
    fine_out, rolled_out = rest[owners : owners + 2]
    field, wet, bed, more, extra, made, anchor_ref, sem_in = rest[owners + 2 :]
    rows = owners * band
    cols = lane_blocks * 128
    me = lax.axis_index(("row", "col")).astype(jnp.int32)
    nest = lax.axis_index("nest").astype(jnp.int32)
    my_row = me // columns
    done_half = me * 2 // owners
    half_rows_at = pl.multiple_of(done_half * (rows // 2), 8)
    corners = pltpu.make_async_copy(anchor_hbm, anchor_ref, sem_in)
    corners.start()

    for k in range(3):
        for q in range(lane_blocks):
            made[k, q, pl.ds(half_rows_at, rows // 2)] = half_in[k, q]
            fine_out[0, k, pl.ds(half_rows_at, rows // 2), q * 128 : q * 128 + 128] = half_in[k, q]
    lane1 = lax.broadcasted_iota(jnp.int32, (1, 128), 1)
    for q in range(lane_blocks):
        wet[q, 8 : 8 + rows] = wet_in[q]
        bed[q, 8 : 8 + rows] = bed_in[q]
    unpack(dims, me, 0, messages, ds, field, extra)

    for source, at, inside, near in (
        (owners - 1, 0, my_row > 0, 8),
        (0, 8 + rows, my_row < blocks - 1, rows),
    ):
        last = from_half_rows(extra[source, 0:8], 0, lane1)
        for k in range(3):
            for q in range(lane_blocks):
                n = k * lane_blocks + q
                row = last if n == 8 else extra[source, 8 + n : 9 + n]
                row = jnp.broadcast_to(row, (8, 128))
                field[k, q, at : at + 8] = jnp.where(inside, row, field[k, q, near : near + 8])
    north = edge_rows(dims, extra, me - columns, my_row > 0)
    south = edge_rows(dims, extra, me + columns, my_row < blocks - 1)
    sub8 = lax.broadcasted_iota(jnp.int32, (8, 128), 0)
    stack = jnp.zeros((8, 128), F32)
    for n, row in enumerate((north[0], north[1], south[0], south[1])):
        stack = jnp.where(sub8 == n, row, stack)
    ends = mul_right(stack, spread_t(128, cols, 3), 3)
    for n, (ref, at) in enumerate(((wet, 0), (bed, 0), (wet, 8 + rows), (bed, 8 + rows))):
        for q in range(lane_blocks):
            ref[q, at : at + 8] = jnp.broadcast_to(ends[n : n + 1, q * 128 : q * 128 + 128], (8, 128))

    groups = rows // 8
    one = done_half * (groups - 1)
    along = (dims, field, wet, bed, 8, open_x, slope_x, 0, more, made, fine_out)
    sweep(*along, one, 1, 1)
    many = (1 - done_half) * (groups // 2 - 1)
    sweep(*along, many, groups // 2 + 1, 5)
    corners.wait()
    coarse_rows = rows // 3
    coarse_cols = cols // 3
    a0 = anchor_ref[nest, 0]
    a1 = anchor_ref[nest, 1]
    gather_cols = spread(cols, coarse_cols, 3, a1)
    for k in range(3):
        total = jnp.concatenate(
            [
                sum(made[k, q, pl.ds(n, coarse_rows, stride=3), :] for n in range(3))
                for q in range(lane_blocks)
            ],
            axis=1,
        )
        mean = mul_right(total, gather_cols, 2) * (1.0 / 9.0)
        rolled_out[k] = pltpu.roll(mean, a0, 0)


def finish_body(coarse, weights, up, left, diagonal, own, out):
    for k in range(3):
        out[k] = (
            coarse[k] * weights[0]
            + own[k] * weights[1]
            + left[k] * weights[2]
            + up[k] * weights[3]
            + diagonal[k] * weights[4]
        )


def in_vmem(x):
    return pltpu.with_memory_space_constraint(x, pltpu.VMEM)


def in_hbm(x):
    return pltpu.with_memory_space_constraint(x, pltpu.HBM)


SMEM = pl.BlockSpec(memory_space=pltpu.SMEM)
VMEM = pl.BlockSpec(memory_space=pltpu.VMEM)
HBM = pl.BlockSpec(memory_space=pltpu.HBM)


def half_call(dims, ds, wet_fine, bed_fine, messages):
    blocks, band, columns, lane_blocks = dims
    owners = blocks * columns
    rows = owners * band // 2
    return pl.pallas_call(
        lambda *refs: half_body(dims, ds, *refs),
        in_specs=[VMEM, VMEM] + [VMEM] * len(ds),
        out_specs=[VMEM] * 3,
        out_shape=[
            pltpu.VMEM((3, lane_blocks, rows, 128), F32),
            pltpu.VMEM((lane_blocks + 1, 2 * rows, 128), F32),
            pltpu.VMEM((lane_blocks, 2 * rows, 128), F32),
        ],
        scratch_shapes=[
            pltpu.VMEM((3, lane_blocks + 1, rows + 16, 128), F32),
            pltpu.VMEM((2 * rows, 128), F32),
            pltpu.VMEM((2 * rows, 128), F32),
            pltpu.VMEM((3, lane_blocks, rows + 16, 128), F32),
            pltpu.VMEM((owners, 16, 128), F32),
        ],
        name="half", compiler_params=pltpu.CompilerParams(vmem_limit_bytes=12 << 20),
    )(wet_fine, bed_fine, *messages)


def main_call(dims, ds, anchor, wet_fine, bed_fine, half, open_x, slope_x, messages):
    blocks, band, columns, lane_blocks = dims
    owners = blocks * columns
    rows = owners * band
    cols = lane_blocks * 128
    return pl.pallas_call(
        lambda *refs: main_body(dims, ds, *refs),
        in_specs=[HBM] + [VMEM] * (5 + owners),
        out_specs=[VMEM, VMEM],
        out_shape=[
            pltpu.VMEM((1, 3, rows, cols), F32),
            pltpu.VMEM((3, rows // 3, cols // 3), F32),
        ],
        scratch_shapes=[
            pltpu.VMEM((3, lane_blocks + 1, rows + 16, 128), F32),
            pltpu.VMEM((lane_blocks, rows + 16, 128), F32),
            pltpu.VMEM((lane_blocks, rows + 16, 128), F32),
            pltpu.VMEM((3, lane_blocks, rows + 16, 128), F32),
            pltpu.VMEM((owners, 16, 128), F32),
            pltpu.VMEM((3, lane_blocks, rows, 128), F32),
            pltpu.SMEM((2, 2), jnp.int32),
            pltpu.SemaphoreType.DMA,
        ],
        name="main", compiler_params=pltpu.CompilerParams(vmem_limit_bytes=20 << 20),
    )(anchor, wet_fine, bed_fine, half, open_x, slope_x, *messages)


def local_packed(strips, anchor, wet_mask, bathy_index, bed_levels, coarse):
    blocks, band, full_cols = strips.shape[2], strips.shape[4], strips.shape[5]
    columns = lax.axis_size("col")
    owners = blocks * columns
    cols = full_cols // columns
    lane_blocks = cols // 128
    rows = owners * band
    dims = (blocks, band, columns, lane_blocks)
    half_owners = owners // 2
    messages = []
    for ds in (range(half_owners), range(half_owners, owners)):
        made = pl.pallas_call(
            lambda *refs, ds=ds, after=len(messages[:1]): pack_body(dims, ds, after, *refs),
            in_specs=[HBM] * 4 + [VMEM] * len(messages[:1]),
            out_specs=[VMEM] * half_owners,
            out_shape=[pltpu.VMEM((message_rows(dims, d), 128), F32) for d in ds],
            scratch_shapes=[
                pltpu.VMEM((3, blocks, band, full_cols), F32),
                pltpu.VMEM(wet_mask.shape, jnp.int32),
                pltpu.VMEM(bathy_index.shape, jnp.int32),
                pltpu.SMEM(bed_levels.shape, F32),
                pltpu.SemaphoreType.DMA((blocks,)),
                pltpu.SemaphoreType.DMA((3,)),
            ],
            name="pack", compiler_params=pltpu.CompilerParams(vmem_limit_bytes=10 << 20),
        )(
            in_hbm(strips),
            in_hbm(wet_mask),
            in_hbm(bathy_index),
            in_hbm(bed_levels),
            *messages[:1],
        )
        messages += [in_vmem(x) for x in made]

    def rank(d):
        r, c = d // columns, d % columns
        return (d >= half_owners, c * 2 < columns, r, c)

    wanted = sorted(range(1, owners), key=rank)
    arrived = {
        d: lax.ppermute(messages[d], ("row", "col"), [(i, i ^ d) for i in range(owners)])
        for d in wanted
    }
    arrived[0] = messages[0]
    arrived = {d: in_vmem(x) if d else x for d, x in arrived.items()}

    coarse_rows = rows // 3
    coarse_cols = cols // 3
    wet_fine, bed_fine, weights = pl.pallas_call(
        lambda *refs: prep_body(columns, *refs),
        in_specs=[SMEM, SMEM, VMEM, VMEM],
        out_specs=[VMEM] * 3,
        out_shape=[pltpu.VMEM((lane_blocks, rows, 128), F32)] * 2
        + [pltpu.VMEM((5, coarse_rows, coarse_cols), F32)],
        name="prep", compiler_params=pltpu.CompilerParams(vmem_limit_bytes=12 << 20),
    )(bed_levels, anchor, wet_mask, bathy_index)

    early = [0] + wanted[: half_owners - 1]
    order = [0] + wanted
    wet_fine, bed_fine, weights = in_vmem(wet_fine), in_vmem(bed_fine), in_vmem(weights)
    half, open_x, slope_x = half_call(dims, early, wet_fine, bed_fine, [arrived[d] for d in early])
    half, open_x, slope_x = in_vmem(half), in_vmem(open_x), in_vmem(slope_x)
    fine, rolled = main_call(
        dims,
        order,
        in_hbm(anchor),
        wet_fine,
        bed_fine,
        half,
        open_x,
        slope_x,
        [arrived[d] for d in order],
    )
    rolled = in_vmem(rolled)

    lines = lax.axis_size("nest") * lax.axis_size("row")
    rights = [(c, c + 1) for c in range(columns - 1)]
    downs = [(l, l + 1) for l in range(lines - 1)]
    both = [(l * columns + c, l2 * columns + c2) for l, l2 in downs for c, c2 in rights]
    diagonal = lax.ppermute(rolled, ("nest", "row", "col"), both)
    from_left = lax.ppermute(rolled, "col", rights)
    from_up = lax.ppermute(rolled, ("nest", "row"), downs)

    coarse_next = pl.pallas_call(
        finish_body,
        in_specs=[VMEM] * 6,
        out_specs=VMEM,
        out_shape=jax.ShapeDtypeStruct(coarse.shape, F32),
        name="finish", compiler_params=pltpu.CompilerParams(vmem_limit_bytes=4 << 20),
    )(
        in_vmem(coarse),
        weights,
        in_vmem(from_up),
        in_vmem(from_left),
        in_vmem(diagonal),
        rolled,
    )
    return (fine, coarse_next)


def local(strips, anchor, wet_mask, bathy_index, bed_levels, coarse):
    columns = lax.axis_size("col")
    owners = strips.shape[2] * columns
    cols = strips.shape[5] // columns
    band = strips.shape[4]
    fits = (
        owners & (owners - 1) == 0
        and 2 <= owners <= 16
        and strips.shape[2] == lax.axis_size("row")
        and band == 24
        and cols == 384
        and owners * band == 384
        and wet_mask.shape[1:] == (128, 128)
    )
    run = local_packed if fits else local_general
    return run(strips, anchor, wet_mask, bathy_index, bed_levels, coarse)


def solution(mesh):
    return jax.shard_map(
        local,
        mesh=mesh,
        in_specs=(
            P("nest", None, None, ("row", "col"), None, None),
            P(),
            P("nest", "row", "col"),
            P("nest", "row", "col"),
            P(),
            P(None, ("nest", "row"), "col"),
        ),
        out_specs=(P("nest", None, "row", "col"), P(None, ("nest", "row"), "col")),
        check_vma=False,
    )
```

```python
import jax
import jax.numpy as jnp
from jax import lax
from jax.experimental import pallas as pl
from jax.experimental.pallas import tpu as pltpu
from jax.sharding import PartitionSpec as P


gravity = 1.0
courant = 0.2
F32 = jnp.float32


def padded_2(cells, sides, width):
    for axis, dim in sides:
        count = lax.axis_size(axis)
        ends = count - 1
        head = lax.slice_in_dim(cells, 0, width, axis=dim)
        tail = lax.slice_in_dim(cells, cells.shape[dim] - width, cells.shape[dim], axis=dim)
        cells = jnp.concatenate(
            [
                lax.ppermute(tail, axis, [(i, (i + 1) % count) for i in range(ends)]),
                cells,
                lax.ppermute(head, axis, [((i + 1) % count, i) for i in range(ends)]),
            ],
            axis=dim,
        )
    return cells


def passed_along(block, axis, distance):
    devices = range(lax.axis_size(axis))
    route = [(i - distance, i) for i in devices if i - distance in devices]
    return lax.ppermute(block, axis, route)


def advance(padded, bed_pad, wet_pad):
    depth_now = padded[0]
    flow_u = padded[1]
    flow_v = padded[2]
    depth_safe = jnp.where(wet_pad > 0.5, depth_now, 1.0)
    speed_u = flow_u / depth_safe
    speed_v = flow_v / depth_safe
    celerity = jnp.sqrt(gravity * depth_safe)
    pressure = 0.5 * gravity * depth_safe * depth_safe
    fluxes_x = (flow_u, flow_u * speed_u + pressure, flow_v * speed_u)
    fluxes_y = (flow_v, flow_u * speed_v, flow_v * speed_v + pressure)
    reach_x = jnp.abs(speed_u) + celerity
    reach_y = jnp.abs(speed_v) + celerity
    open_x = wet_pad[1:-1, :-1] * wet_pad[1:-1, 1:]
    open_y = wet_pad[:-1, 1:-1] * wet_pad[1:, 1:-1]
    bound_x = jnp.maximum(reach_x[1:-1, :-1], reach_x[1:-1, 1:])
    bound_y = jnp.maximum(reach_y[:-1, 1:-1], reach_y[1:, 1:-1])
    slope_x = (bed_pad[1:-1, 1:] - bed_pad[1:-1, :-1]) * open_x
    slope_y = (bed_pad[1:, 1:-1] - bed_pad[:-1, 1:-1]) * open_y
    centre = depth_now[1:-1, 1:-1]
    sources = (
        None,
        -0.5 * gravity * centre * (slope_x[:, 1:] + slope_x[:, :-1]),
        -0.5 * gravity * centre * (slope_y[1:] + slope_y[:-1]),
    )
    results = []
    for plane in range(3):
        state = padded[plane]
        flux_col = fluxes_x[plane]
        flux_row = fluxes_y[plane]
        face_x = (
            0.5 * (flux_col[1:-1, :-1] + flux_col[1:-1, 1:])
            - 0.5 * bound_x * (state[1:-1, 1:] - state[1:-1, :-1])
        ) * open_x
        face_y = (
            0.5 * (flux_row[:-1, 1:-1] + flux_row[1:, 1:-1])
            - 0.5 * bound_y * (state[1:, 1:-1] - state[:-1, 1:-1])
        ) * open_y
        value = (
            state[1:-1, 1:-1]
            - courant * (face_x[:, 1:] - face_x[:, :-1])
            - courant * (face_y[1:] - face_y[:-1])
        )
        if plane > 0:
            value = value + courant * sources[plane]
        results.append(value)
    return jnp.stack(results)


def expand(cells):
    return jnp.repeat(jnp.repeat(cells, 3, axis=-2), 3, axis=-1)


def lookup(classes, levels):
    ladder = jnp.arange(levels.shape[0], dtype=jnp.int32)
    matches = classes[None] == ladder[:, None, None]
    return jnp.sum(jnp.where(matches, levels[:, None, None], 0.0), axis=0)


def restrict(updated):
    planes, row_count, col_count = updated.shape
    return updated.reshape(planes, row_count // 3, 3, col_count // 3, 3).sum(axis=(2, 4)) / 9.0


def local_general(strips, anchor, wet_mask, bathy_index, bed_levels, coarse):
    tile_blocks = strips.shape[2]
    band_rows = strips.shape[4]
    full_cols = strips.shape[5]
    columns = lax.axis_size("col")
    tile_cols = full_cols // columns
    layered = (
        strips[0, :, :, 0]
        .reshape(3, tile_blocks, band_rows, columns, tile_cols)
        .transpose(0, 1, 3, 2, 4)
    )
    flattened = layered.reshape(3, tile_blocks * columns, band_rows, tile_cols)
    arrived = lax.all_to_all(flattened, ("row", "col"), split_axis=1, concat_axis=1, tiled=True)
    fields = arrived.reshape(3, tile_blocks * columns * band_rows, tile_cols)
    bed_fine = expand(lookup(bathy_index[0], bed_levels))
    wetness = expand(wet_mask[0].astype(F32))
    stacked = jnp.concatenate([fields, bed_fine[None], wetness[None]], axis=0)
    padded_all = padded_2(stacked, (("row", 1), ("col", 2)), 1)
    updated = advance(padded_all[:3], padded_all[3], padded_all[4])
    restricted = restrict(updated)
    coarse_rows = restricted.shape[1]
    coarse_cols = restricted.shape[2]
    contribution = jnp.concatenate(
        [restricted, jnp.ones((1, coarse_rows, coarse_cols), F32)], axis=0
    )
    nest_index = lax.axis_index("nest")
    corner = lax.dynamic_index_in_dim(anchor, nest_index, 0, keepdims=False)
    canvas = lax.dynamic_update_slice(
        jnp.zeros((4, 2 * coarse_rows, 2 * coarse_cols), F32),
        contribution,
        (jnp.int32(0), corner[0], corner[1]),
    )
    spilled = passed_along(canvas[:, :, coarse_cols:], "col", 1)
    merged = canvas[:, :, :coarse_cols] + spilled
    lowered = passed_along(merged[:, coarse_rows:], ("nest", "row"), 1)
    received_sum = merged[:, :coarse_rows] + lowered
    coarse_next = (coarse + received_sum[:3]) / (1.0 + received_sum[3])
    return (updated[None], coarse_next)


def halo_rows(dims, d):
    return d // dims[2] != dims[0] - 1


def message_rows(dims, d):
    blocks, band, columns, lane_blocks = dims
    return 3 * lane_blocks * band + (16 if halo_rows(dims, d) else 8)


def half_rows(row):
    return pltpu.roll(row, 64, 1), row


def from_half_rows(block, at, lane):
    upper = block[at : at + 1]
    return jnp.where(lane < 64, pltpu.roll(upper, 64, 1), block[at + 1 : at + 2])


def pack_body(dims, ds, after, strips_hbm, wet_hbm, class_hbm, levels_hbm, *rest):
    blocks, band, columns, lane_blocks = dims
    rest = rest[after:]
    outs = rest[: len(ds)]
    strips, tiles, wet_ref, class_ref, levels_ref, sems, small = rest[len(ds) :]
    tile_cols = lane_blocks * 128
    me = lax.axis_index(("row", "col")).astype(jnp.int32)
    my_row = me // columns
    my_col = me % columns
    loads = [
        pltpu.make_async_copy(wet_hbm, wet_ref, small.at[0]),
        pltpu.make_async_copy(class_hbm, class_ref, small.at[1]),
        pltpu.make_async_copy(levels_hbm, levels_ref, small.at[2]),
    ]
    for c in loads:
        c.start()
    first = me == 0
    groups = sorted({d // columns for d in ds})
    copies = []
    for n, r in enumerate(groups):
        j = my_row ^ r
        jj = jnp.clip(jnp.where(first, j + 1, j - 1), 0, blocks - 1)
        edge = pl.ds(pl.multiple_of(jnp.where(first, 0, band - 8), 8), 8)
        copies.append(
            (
                pltpu.make_async_copy(strips_hbm.at[0, :, j, 0], strips.at[n], sems.at[0, n]),
                pltpu.make_async_copy(strips_hbm.at[0, :, jj, 0, edge], tiles.at[n], sems.at[1, n]),
            )
        )
    for pair in copies:
        for c in pair:
            c.start()
    lane = lax.broadcasted_iota(jnp.int32, (8, 128), 1)
    sub = lax.broadcasted_iota(jnp.int32, (8, 128), 0)
    size = wet_ref.shape[1]
    diag = lax.broadcasted_iota(jnp.int32, (size, 128), 0) == lax.broadcasted_iota(
        jnp.int32, (size, 128), 1
    )
    for c in loads:
        c.wait()
    edges = []
    for ref in (wet_ref, class_ref):
        cells = ref[0].astype(F32)
        north = cells[0:1]
        south = cells[size - 1 : size]
        west = jnp.sum(jnp.where(diag, cells[:, 0:1], 0.0), axis=0, keepdims=True)
        east = jnp.sum(jnp.where(diag, cells[:, 127:128], 0.0), axis=0, keepdims=True)
        four = (north, south, west, east)
        if ref is class_ref:
            four = tuple(level_of(row, levels_ref) for row in four)
        edges.append(four)
    body_rows = 3 * lane_blocks * band
    waiting = list(groups)
    mixes = []
    for out, d in zip(outs, ds):
        n = groups.index(d // columns)
        if groups[n] in waiting:
            copies[n][0].wait()
            waiting.remove(groups[n])
        to = me ^ d
        j = to // columns
        c = to % columns
        base = pl.multiple_of(c * tile_cols, 128)
        for k in range(3):
            for q in range(lane_blocks):
                at = (k * lane_blocks + q) * band
                out[at : at + band] = strips[n, k, :, pl.ds(pl.multiple_of(base + q * 128, 128), 128)]
        west_at = pl.multiple_of(jnp.maximum(base - 128, 0), 128)
        east_at = pl.multiple_of(jnp.where(c == columns - 1, base, base + tile_cols), 128)
        mixed = jnp.zeros((8, 128), F32)
        for g in range(band // 8):
            for k in range(3):
                i = g * 3 + k
                west = strips[n, k, g * 8 : g * 8 + 8, pl.ds(west_at, 128)]
                east = strips[n, k, g * 8 : g * 8 + 8, pl.ds(east_at, 128)]
                both = pltpu.roll(jnp.where(lane == 127, west, east), 2 * i + 1, 1)
                mixed = jnp.where((lane == 2 * i) | (lane == 2 * i + 1), both, mixed)
        mixes.append(mixed)
    for pair in copies:
        pair[1].wait()
    for out, d, mixed in zip(outs, ds, mixes):
        n = groups.index(d // columns)
        to = me ^ d
        j = to // columns
        c = to % columns
        base = pl.multiple_of(c * tile_cols, 128)
        tucked = [jnp.zeros((1, 128), F32)]
        if halo_rows(dims, d):
            rows = []
            for k in range(3):
                for q in range(lane_blocks):
                    spot = pl.ds(pl.multiple_of(base + q * 128, 128), 128)
                    tile = tiles[n, k, :, spot]
                    rows.append(jnp.where(first, tile[0:1], tile[7:8]))
            halo = jnp.zeros((8, 128), F32)
            for i in range(8):
                halo = jnp.where(sub == i, rows[i], halo)
            out[body_rows + 8 : body_rows + 16] = halo
            tucked = [rows[8]]
        for north, south, west, east in edges:
            row = jnp.where(
                c == my_col,
                jnp.where(j > my_row, south, north),
                jnp.where(c > my_col, east, west),
            )
            tucked.append(row)
        for t, row in enumerate(tucked):
            low, high = half_rows(row)
            mixed = jnp.where((sub == 2 * t) & (lane >= 64), low, mixed)
            mixed = jnp.where((sub == 2 * t + 1) & (lane >= 64), high, mixed)
        out[body_rows : body_rows + 8] = mixed


def spread(rows, cols, width, offset=None):
    i = lax.broadcasted_iota(jnp.int32, (rows, cols), 0)
    m = lax.broadcasted_iota(jnp.int32, (rows, cols), 1)
    if offset is not None:
        m = m - offset
        m = jnp.where(m < 0, m + cols, m)
    low = m * width
    return jnp.where((i >= low) & (i < low + width), 1.0, 0.0)


def spread_t(rows, cols, width, offset=None):
    m = lax.broadcasted_iota(jnp.int32, (rows, cols), 0)
    i = lax.broadcasted_iota(jnp.int32, (rows, cols), 1)
    if offset is not None:
        m = m - offset
        m = jnp.where(m < 0, m + rows, m)
    low = m * width
    return jnp.where((i >= low) & (i < low + width), 1.0, 0.0)


def level_of(classes, levels_ref):
    out = jnp.zeros_like(classes)
    for n in range(levels_ref.shape[0]):
        out = jnp.where(classes == n, levels_ref[n], out)
    return out


def prep_body(columns, levels_ref, anchor_ref, wet_ref, class_ref, wet_out, bed_out, weights):
    lane_blocks, rows, _ = wet_out.shape
    size, width = wet_ref.shape[1], wet_ref.shape[2]
    wet = wet_ref[0].astype(F32)
    bed = level_of(class_ref[0].astype(F32), levels_ref)
    across = spread_t(width, lane_blocks * 128, 3)
    down = spread(rows, size, 3)
    for out, cells, parts in ((wet_out, wet, 1), (bed_out, bed, 3)):
        fine = mul_left(down, mul_right(cells, across, parts), parts)
        for q in range(lane_blocks):
            out[q] = fine[:, q * 128 : q * 128 + 128]
    nest = lax.axis_index("nest").astype(jnp.int32)
    row_at = lax.axis_index("row").astype(jnp.int32)
    col_at = lax.axis_index("col").astype(jnp.int32)
    up_nest = jnp.where(row_at == 0, jnp.maximum(nest - 1, 0), nest)
    i = lax.broadcasted_iota(jnp.int32, weights.shape[1:], 0)
    m = lax.broadcasted_iota(jnp.int32, weights.shape[1:], 1)
    has_left = jnp.where(col_at > 0, 1.0, 0.0)
    has_up = jnp.where((row_at > 0) | (nest > 0), 1.0, 0.0)
    own_rows = jnp.where(i >= anchor_ref[nest, 0], 1.0, 0.0)
    up_rows = jnp.where(i < anchor_ref[up_nest, 0], has_up, 0.0)
    own_cols = m >= anchor_ref[nest, 1]
    up_cols = m >= anchor_ref[up_nest, 1]
    shares = (
        jnp.where(own_cols, own_rows, 0.0),
        jnp.where(own_cols, 0.0, own_rows * has_left),
        jnp.where(up_cols, up_rows, 0.0),
        jnp.where(up_cols, 0.0, up_rows * has_left),
    )
    scale = 1.0 / (1.0 + shares[0] + shares[1] + shares[2] + shares[3])
    weights[0] = scale
    for n, share in enumerate(shares):
        weights[n + 1] = share * scale


def split(x, parts):
    out = []
    for n in range(parts):
        piece = x.astype(jnp.bfloat16)
        out.append(piece)
        if n + 1 < parts:
            x = x - piece.astype(F32)
    return out


def mul_left(matrix, x, parts):
    matrix = matrix.astype(jnp.bfloat16)
    return sum(jnp.dot(matrix, piece, preferred_element_type=F32) for piece in split(x, parts))


def mul_right(x, matrix, parts):
    matrix = matrix.astype(jnp.bfloat16)
    return sum(jnp.dot(piece, matrix, preferred_element_type=F32) for piece in split(x, parts))


def mul_left_t(matrix, x, parts):
    matrix = matrix.astype(jnp.bfloat16)
    return sum(
        lax.dot_general(matrix, piece, (((1,), (1,)), ((), ())), preferred_element_type=F32)
        for piece in split(x, parts)
    )


def unpack(dims, me, first_row, messages, ds, field, extra):
    blocks, band, columns, lane_blocks = dims
    body_rows = 3 * lane_blocks * band
    for message, d in zip(messages, ds):
        p = me ^ d
        top = pl.multiple_of(8 + p * band - first_row, 8)
        mixed = message[body_rows : body_rows + 8]
        for k in range(3):
            for q in range(lane_blocks):
                n = k * lane_blocks + q
                field[k, q, pl.ds(top, band)] = message[
                    n * band : n * band + band
                ]
            for g in range(band // 8):
                i = g * 3 + k
                at = pl.multiple_of(top + g * 8, 8)
                field[k, lane_blocks, pl.ds(at, 8)] = pltpu.roll(mixed, 127 - 2 * i, 1)
        extra[p, 0:8] = mixed
        if halo_rows(dims, d):
            extra[p, 8:16] = message[body_rows + 8 : body_rows + 16]


def edge_rows(dims, extra, source, inside):
    blocks, band, columns, lane_blocks = dims
    lane = lax.broadcasted_iota(jnp.int32, (1, 128), 1)
    block = extra[jnp.where(inside, source, 0), 0:8]
    wet_row = from_half_rows(block, 2, lane)
    bed_row = from_half_rows(block, 4, lane)
    return jnp.where(inside, wet_row, 0.0), jnp.where(inside, bed_row, 0.0)


def side_cells(dims, me, extra, wet_side, bed_side):
    columns = dims[2]
    my_col = me % columns
    west = edge_rows(dims, extra, me - 1, my_col > 0)
    east = edge_rows(dims, extra, me + 1, my_col < columns - 1)
    sub = lax.broadcasted_iota(jnp.int32, (128, 128), 0)
    pair = jnp.zeros((128, 128), F32)
    for n, row in ((0, east[0]), (127, west[0]), (64, east[1]), (63, west[1])):
        pair = jnp.where(sub == n, row, pair)
    sides = mul_left_t(spread(wet_side.shape[0], 128, 3), pair, 3)
    wet_side[...] = sides
    bed_side[...] = pltpu.roll(sides, 64, 1)


def slopes(lane_blocks, wet, bed, wet_side, bed_side, open_x, slope_x, rows):
    lane = lax.broadcasted_iota(jnp.int32, (8, 128), 1)
    sides = lane_blocks + 1

    def step(t, _):
        at = pl.ds(pl.multiple_of(t * 8, 8), 8)
        w = [wet[q, at] for q in range(lane_blocks)] + [wet_side[at]]
        z = [bed[q, at] for q in range(lane_blocks)] + [bed_side[at]]
        steps = []
        for q in range(sides):
            w2, z2 = (
                pltpu.roll(jnp.where(lane == 0, x[(q + 1) % sides], x[q]), 127, 1) for x in (w, z)
            )
            half = (0.5 * courant) * (w[q] * w2)
            open_x[q, at] = half
            steps.append(half * (z2 - z[q]))
        for q in range(lane_blocks):
            left = pltpu.roll(jnp.where(lane == 127, steps[q - 1], steps[q]), 1, 1)
            slope_x[q, at] = gravity * (steps[q] + left)
        return 0

    lax.fori_loop(0, rows // 8, step, 0, unroll=2)


def sweep(dims, field, wet, bed, wet_at, open_x, slope_x, open_at, more, made, fine, start, count, unroll):
    lane_blocks = dims[3]
    sides = lane_blocks + 1
    lane = lax.broadcasted_iota(jnp.int32, (8, 128), 1)
    sub = lax.broadcasted_iota(jnp.int32, (8, 128), 0)

    def rates(h, hu, hv):
        root = lax.rsqrt(h)
        inv = root * root
        u = hu * inv
        c = (gravity**0.5) * (h * root)
        p = (0.5 * gravity) * (h * h)
        return hu * u + p, hv * u, jnp.abs(u) + c, inv, c, p

    def cells(group, q):
        at = pl.ds(pl.multiple_of(8 + group * 8, 8), 8)
        h, hu, hv = (field[k, q, at] for k in range(3))
        f2, m, a, inv, c, p = rates(h, hu, hv)
        if q < lane_blocks:
            v = hv * inv
            more[0, q, at] = m
            more[1, q, at] = hv * v + p
            more[2, q, at] = jnp.abs(v) + c
        return h, hu, hv, f2, m, a

    def face(half, near, far):
        bound = half * jnp.maximum(near[6], far[6])
        return [half * (near[3 + k] + far[3 + k]) - bound * (far[k] - near[k]) for k in range(3)]

    def across(t, _):
        group = start + t
        spot = pl.ds(pl.multiple_of(group * 8, 8), 8)
        opened = pl.ds(pl.multiple_of(open_at + group * 8, 8), 8)
        blocks = [cells(group, q) for q in range(sides)]
        faces = []
        for q in range(sides):
            now, nxt = blocks[q], blocks[(q + 1) % sides]
            h, hu, hv, f2, m, a = now
            h2, hu2, hv2 = (
                pltpu.roll(jnp.where(lane == 0, y, x), 127, 1) for x, y in zip(now[:3], nxt[:3])
            )
            f22, m2, a2 = rates(h2, hu2, hv2)[:3]
            faces.append(
                face(open_x[q, opened], (h, hu, hv, hu, f2, m, a), (h2, hu2, hv2, hu2, f22, m2, a2))
            )
        for q in range(lane_blocks):
            right = faces[q]
            left = [
                pltpu.roll(jnp.where(lane == 127, y, x), 1, 1) for x, y in zip(right, faces[q - 1])
            ]
            h, hu, hv = blocks[q][:3]
            made[0, q, spot] = h - (right[0] - left[0])
            made[1, q, spot] = hu - (right[1] - left[1]) - h * slope_x[q, opened]
            made[2, q, spot] = hv - (right[2] - left[2])
        return 0

    def south_face(group, q):
        at = pl.multiple_of(8 + group * 8, 8)
        w_at = pl.multiple_of(wet_at + group * 8, 8)
        sides = []
        for step in range(2):
            rows = pl.ds(at + step, 8)
            h, hu, hv = (field[k, q, rows] for k in range(3))
            m, g3, b = (more[k, q, rows] for k in range(3))
            sides.append((h, hu, hv, hv, m, g3, b))
        half = (0.5 * courant) * (wet[q, pl.ds(w_at, 8)] * wet[q, pl.ds(w_at + 1, 8)])
        slope = half * (bed[q, pl.ds(w_at + 1, 8)] - bed[q, pl.ds(w_at, 8)])
        return face(half, *sides) + [slope]

    def down(t, above):
        group = start + t
        spot = pl.ds(pl.multiple_of(group * 8, 8), 8)
        new = []
        for q in range(lane_blocks):
            below = south_face(group, q)
            up = [
                pltpu.roll(jnp.where(sub == 7, y, x), 1, 0) for x, y in zip(below, above[q])
            ]
            h = field[0, q, pl.ds(pl.multiple_of(8 + group * 8, 8), 8)]
            done = [made[k, q, spot] - (below[k] - up[k]) for k in range(3)]
            done[2] = done[2] - gravity * h * (below[3] + up[3])
            for k in range(3):
                made[k, q, spot] = done[k]
                if fine is not None:
                    fine[0, k, spot, q * 128 : q * 128 + 128] = done[k]
            new.append(below)
        return new

    for q in range(lane_blocks):
        cells(start - 1, q)
        cells(start + count, q)
    if count == 1:
        across(0, 0)
        down(0, [south_face(start - 1, q) for q in range(lane_blocks)])
    else:
        lax.fori_loop(0, count, across, 0, unroll=unroll)
        above = [south_face(start - 1, q) for q in range(lane_blocks)]
        lax.fori_loop(0, count, down, above, unroll=unroll)


def half_body(dims, ds, wet_in, bed_in, *rest):
    blocks, band, columns, lane_blocks = dims
    owners = blocks * columns
    messages = rest[: len(ds)]
    made, open_x, slope_x, field, wet_side, bed_side, more, extra = rest[len(ds) :]
    rows = owners * band // 2
    me = lax.axis_index(("row", "col")).astype(jnp.int32)
    first_row = pl.multiple_of((me * 2 // owners) * rows, 8)
    unpack(dims, me, first_row, messages, ds, field, extra)
    side_cells(dims, me, extra, wet_side, bed_side)
    slopes(lane_blocks, wet_in, bed_in, wet_side, bed_side, open_x, slope_x, 2 * rows)
    for k in range(3):
        for q in range(lane_blocks):
            made[k, q, 0:8] = jnp.zeros((8, 128), F32)
            made[k, q, rows - 8 : rows] = jnp.zeros((8, 128), F32)
    sweep(
        dims, field, wet_in, bed_in, first_row, open_x, slope_x, first_row, more, made, None, 1, rows // 8 - 2, 2
    )


def main_body(dims, ds, anchor_hbm, wet_in, bed_in, half_in, open_x, slope_x, *rest):
    blocks, band, columns, lane_blocks = dims
    owners = blocks * columns
    messages = rest[:owners]
    fine_out, rolled_out = rest[owners : owners + 2]
    field, wet, bed, more, extra, made, anchor_ref, sem_in = rest[owners + 2 :]
    rows = owners * band
    cols = lane_blocks * 128
    me = lax.axis_index(("row", "col")).astype(jnp.int32)
    nest = lax.axis_index("nest").astype(jnp.int32)
    my_row = me // columns
    done_half = me * 2 // owners
    half_rows_at = pl.multiple_of(done_half * (rows // 2), 8)
    corners = pltpu.make_async_copy(anchor_hbm, anchor_ref, sem_in)
    corners.start()

    for k in range(3):
        for q in range(lane_blocks):
            made[k, q, pl.ds(half_rows_at, rows // 2)] = half_in[k, q]
            fine_out[0, k, pl.ds(half_rows_at, rows // 2), q * 128 : q * 128 + 128] = half_in[k, q]
    lane1 = lax.broadcasted_iota(jnp.int32, (1, 128), 1)
    for q in range(lane_blocks):
        wet[q, 8 : 8 + rows] = wet_in[q]
        bed[q, 8 : 8 + rows] = bed_in[q]
    unpack(dims, me, 0, messages, ds, field, extra)

    for source, at, inside, near in (
        (owners - 1, 0, my_row > 0, 8),
        (0, 8 + rows, my_row < blocks - 1, rows),
    ):
        last = from_half_rows(extra[source, 0:8], 0, lane1)
        for k in range(3):
            for q in range(lane_blocks):
                n = k * lane_blocks + q
                row = last if n == 8 else extra[source, 8 + n : 9 + n]
                row = jnp.broadcast_to(row, (8, 128))
                field[k, q, at : at + 8] = jnp.where(inside, row, field[k, q, near : near + 8])
    north = edge_rows(dims, extra, me - columns, my_row > 0)
    south = edge_rows(dims, extra, me + columns, my_row < blocks - 1)
    sub8 = lax.broadcasted_iota(jnp.int32, (8, 128), 0)
    stack = jnp.zeros((8, 128), F32)
    for n, row in enumerate((north[0], north[1], south[0], south[1])):
        stack = jnp.where(sub8 == n, row, stack)
    ends = mul_right(stack, spread_t(128, cols, 3), 3)
    for n, (ref, at) in enumerate(((wet, 0), (bed, 0), (wet, 8 + rows), (bed, 8 + rows))):
        for q in range(lane_blocks):
            ref[q, at : at + 8] = jnp.broadcast_to(ends[n : n + 1, q * 128 : q * 128 + 128], (8, 128))

    groups = rows // 8
    one = done_half * (groups - 1)
    along = (dims, field, wet, bed, 8, open_x, slope_x, 0, more, made, fine_out)
    sweep(*along, one, 1, 1)
    many = (1 - done_half) * (groups // 2 - 1)
    sweep(*along, many, groups // 2 + 1, 5)
    corners.wait()
    coarse_rows = rows // 3
    coarse_cols = cols // 3
    a0 = anchor_ref[nest, 0]
    a1 = anchor_ref[nest, 1]
    gather_cols = spread(cols, coarse_cols, 3, a1)
    for k in range(3):
        total = jnp.concatenate(
            [
                sum(made[k, q, pl.ds(n, coarse_rows, stride=3), :] for n in range(3))
                for q in range(lane_blocks)
            ],
            axis=1,
        )
        mean = mul_right(total, gather_cols, 2) * (1.0 / 9.0)
        rolled_out[k] = pltpu.roll(mean, a0, 0)


def finish_body(coarse, weights, left, up, diagonal, own, out):
    for k in range(3):
        out[k] = (
            coarse[k] * weights[0]
            + own[k] * weights[1]
            + left[k] * weights[2]
            + up[k] * weights[3]
            + diagonal[k] * weights[4]
        )


def in_vmem(x):
    return pltpu.with_memory_space_constraint(x, pltpu.VMEM)


def in_hbm(x):
    return pltpu.with_memory_space_constraint(x, pltpu.HBM)


SMEM = pl.BlockSpec(memory_space=pltpu.SMEM)
VMEM = pl.BlockSpec(memory_space=pltpu.VMEM)
HBM = pl.BlockSpec(memory_space=pltpu.HBM)


def half_call(dims, ds, wet_fine, bed_fine, messages):
    blocks, band, columns, lane_blocks = dims
    owners = blocks * columns
    rows = owners * band // 2
    return pl.pallas_call(
        lambda *refs: half_body(dims, ds, *refs),
        in_specs=[VMEM, VMEM] + [VMEM] * len(ds),
        out_specs=[VMEM] * 3,
        out_shape=[
            pltpu.VMEM((3, lane_blocks, rows, 128), F32),
            pltpu.VMEM((lane_blocks + 1, 2 * rows, 128), F32),
            pltpu.VMEM((lane_blocks, 2 * rows, 128), F32),
        ],
        scratch_shapes=[
            pltpu.VMEM((3, lane_blocks + 1, rows + 16, 128), F32),
            pltpu.VMEM((2 * rows, 128), F32),
            pltpu.VMEM((2 * rows, 128), F32),
            pltpu.VMEM((3, lane_blocks, rows + 16, 128), F32),
            pltpu.VMEM((owners, 16, 128), F32),
        ],
        name="half", compiler_params=pltpu.CompilerParams(vmem_limit_bytes=12 << 20),
    )(wet_fine, bed_fine, *messages)


def main_call(dims, ds, anchor, wet_fine, bed_fine, half, open_x, slope_x, messages):
    blocks, band, columns, lane_blocks = dims
    owners = blocks * columns
    rows = owners * band
    cols = lane_blocks * 128
    return pl.pallas_call(
        lambda *refs: main_body(dims, ds, *refs),
        in_specs=[HBM] + [VMEM] * (5 + owners),
        out_specs=[VMEM, VMEM],
        out_shape=[
            pltpu.VMEM((1, 3, rows, cols), F32),
            pltpu.VMEM((3, rows // 3, cols // 3), F32),
        ],
        scratch_shapes=[
            pltpu.VMEM((3, lane_blocks + 1, rows + 16, 128), F32),
            pltpu.VMEM((lane_blocks, rows + 16, 128), F32),
            pltpu.VMEM((lane_blocks, rows + 16, 128), F32),
            pltpu.VMEM((3, lane_blocks, rows + 16, 128), F32),
            pltpu.VMEM((owners, 16, 128), F32),
            pltpu.VMEM((3, lane_blocks, rows, 128), F32),
            pltpu.SMEM((2, 2), jnp.int32),
            pltpu.SemaphoreType.DMA,
        ],
        name="main", compiler_params=pltpu.CompilerParams(vmem_limit_bytes=20 << 20),
    )(anchor, wet_fine, bed_fine, half, open_x, slope_x, *messages)


def local_packed(strips, anchor, wet_mask, bathy_index, bed_levels, coarse):
    blocks, band, full_cols = strips.shape[2], strips.shape[4], strips.shape[5]
    columns = lax.axis_size("col")
    owners = blocks * columns
    cols = full_cols // columns
    lane_blocks = cols // 128
    rows = owners * band
    dims = (blocks, band, columns, lane_blocks)
    half_owners = owners // 2

    def rank(d):
        r, c = d // columns, d % columns
        return (d >= half_owners, c * 2 < columns, r, c)

    wanted = sorted(range(1, owners), key=rank)
    opening = [d for d in wanted if d < columns and d * 2 >= columns]
    rest = [d for d in range(half_owners) if d not in opening]
    messages = {}
    after = []
    for ds in (opening, rest, list(range(half_owners, owners))):
        count = len({d // columns for d in ds})
        made = pl.pallas_call(
            lambda *refs, ds=ds, after=len(after): pack_body(dims, ds, after, *refs),
            in_specs=[HBM] * 4 + [VMEM] * len(after),
            out_specs=[VMEM] * len(ds),
            out_shape=[pltpu.VMEM((message_rows(dims, d), 128), F32) for d in ds],
            scratch_shapes=[
                pltpu.VMEM((count, 3, band, full_cols), F32),
                pltpu.VMEM((count, 3, 8, full_cols), F32),
                pltpu.VMEM(wet_mask.shape, jnp.int32),
                pltpu.VMEM(bathy_index.shape, jnp.int32),
                pltpu.SMEM(bed_levels.shape, F32),
                pltpu.SemaphoreType.DMA((2, count)),
                pltpu.SemaphoreType.DMA((3,)),
            ],
            name="pack",
            compiler_params=pltpu.CompilerParams(vmem_limit_bytes=10 << 20),
        )(
            in_hbm(strips),
            in_hbm(wet_mask),
            in_hbm(bathy_index),
            in_hbm(bed_levels),
            *after,
        )
        messages.update(zip(ds, (in_vmem(x) for x in made)))
        after = [messages[ds[0]]]

    arrived = {
        d: lax.ppermute(messages[d], ("row", "col"), [(i, i ^ d) for i in range(owners)])
        for d in wanted
    }
    arrived[0] = messages[0]
    arrived = {d: in_vmem(x) if d else x for d, x in arrived.items()}

    coarse_rows = rows // 3
    coarse_cols = cols // 3
    wet_fine, bed_fine, weights = pl.pallas_call(
        lambda *refs: prep_body(columns, *refs),
        in_specs=[SMEM, SMEM, VMEM, VMEM],
        out_specs=[VMEM] * 3,
        out_shape=[pltpu.VMEM((lane_blocks, rows, 128), F32)] * 2
        + [pltpu.VMEM((5, coarse_rows, coarse_cols), F32)],
        name="prep", compiler_params=pltpu.CompilerParams(vmem_limit_bytes=12 << 20),
    )(bed_levels, anchor, wet_mask, bathy_index)

    early = [0] + wanted[: half_owners - 1]
    order = [0] + wanted
    wet_fine, bed_fine, weights = in_vmem(wet_fine), in_vmem(bed_fine), in_vmem(weights)
    half, open_x, slope_x = half_call(dims, early, wet_fine, bed_fine, [arrived[d] for d in early])
    half, open_x, slope_x = in_vmem(half), in_vmem(open_x), in_vmem(slope_x)
    fine, rolled = main_call(
        dims,
        order,
        in_hbm(anchor),
        wet_fine,
        bed_fine,
        half,
        open_x,
        slope_x,
        [arrived[d] for d in order],
    )
    rolled = in_vmem(rolled)

    lines = lax.axis_size("nest") * lax.axis_size("row")
    rights = [(c, c + 1) for c in range(columns - 1)]
    downs = [(l, l + 1) for l in range(lines - 1)]
    both = [(l * columns + c, l2 * columns + c2) for l, l2 in downs for c, c2 in rights]
    diagonal = lax.ppermute(rolled, ("nest", "row", "col"), both)
    from_left = lax.ppermute(rolled, "col", rights)
    from_up = lax.ppermute(rolled, ("nest", "row"), downs)

    coarse_next = pl.pallas_call(
        finish_body,
        in_specs=[VMEM] * 6,
        out_specs=VMEM,
        out_shape=jax.ShapeDtypeStruct(coarse.shape, F32),
        name="finish", compiler_params=pltpu.CompilerParams(vmem_limit_bytes=4 << 20),
    )(
        in_vmem(coarse),
        weights,
        in_vmem(from_left),
        in_vmem(from_up),
        in_vmem(diagonal),
        rolled,
    )
    return (fine, coarse_next)


def local(strips, anchor, wet_mask, bathy_index, bed_levels, coarse):
    columns = lax.axis_size("col")
    owners = strips.shape[2] * columns
    cols = strips.shape[5] // columns
    band = strips.shape[4]
    fits = (
        owners & (owners - 1) == 0
        and 2 <= owners <= 16
        and strips.shape[2] == lax.axis_size("row")
        and band == 24
        and cols == 384
        and owners * band == 384
        and wet_mask.shape[1:] == (128, 128)
    )
    run = local_packed if fits else local_general
    return run(strips, anchor, wet_mask, bathy_index, bed_levels, coarse)


def solution(mesh):
    return jax.shard_map(
        local,
        mesh=mesh,
        in_specs=(
            P("nest", None, None, ("row", "col"), None, None),
            P(),
            P("nest", "row", "col"),
            P("nest", "row", "col"),
            P(),
            P(None, ("nest", "row"), "col"),
        ),
        out_specs=(P("nest", None, "row", "col"), P(None, ("nest", "row"), "col")),
        check_vma=False,
    )
```

```python
import jax
import jax.numpy as jnp
from jax import lax
from jax.experimental import pallas as pl
from jax.experimental.pallas import tpu as pltpu
from jax.sharding import PartitionSpec as P


gravity = 1.0
courant = 0.2
F32 = jnp.float32


def padded_2(cells, sides, width):
    for axis, dim in sides:
        count = lax.axis_size(axis)
        ends = count - 1
        head = lax.slice_in_dim(cells, 0, width, axis=dim)
        tail = lax.slice_in_dim(cells, cells.shape[dim] - width, cells.shape[dim], axis=dim)
        cells = jnp.concatenate(
            [
                lax.ppermute(tail, axis, [(i, (i + 1) % count) for i in range(ends)]),
                cells,
                lax.ppermute(head, axis, [((i + 1) % count, i) for i in range(ends)]),
            ],
            axis=dim,
        )
    return cells


def passed_along(block, axis, distance):
    devices = range(lax.axis_size(axis))
    route = [(i - distance, i) for i in devices if i - distance in devices]
    return lax.ppermute(block, axis, route)


def advance(padded, bed_pad, wet_pad):
    depth_now = padded[0]
    flow_u = padded[1]
    flow_v = padded[2]
    depth_safe = jnp.where(wet_pad > 0.5, depth_now, 1.0)
    speed_u = flow_u / depth_safe
    speed_v = flow_v / depth_safe
    celerity = jnp.sqrt(gravity * depth_safe)
    pressure = 0.5 * gravity * depth_safe * depth_safe
    fluxes_x = (flow_u, flow_u * speed_u + pressure, flow_v * speed_u)
    fluxes_y = (flow_v, flow_u * speed_v, flow_v * speed_v + pressure)
    reach_x = jnp.abs(speed_u) + celerity
    reach_y = jnp.abs(speed_v) + celerity
    open_x = wet_pad[1:-1, :-1] * wet_pad[1:-1, 1:]
    open_y = wet_pad[:-1, 1:-1] * wet_pad[1:, 1:-1]
    bound_x = jnp.maximum(reach_x[1:-1, :-1], reach_x[1:-1, 1:])
    bound_y = jnp.maximum(reach_y[:-1, 1:-1], reach_y[1:, 1:-1])
    slope_x = (bed_pad[1:-1, 1:] - bed_pad[1:-1, :-1]) * open_x
    slope_y = (bed_pad[1:, 1:-1] - bed_pad[:-1, 1:-1]) * open_y
    centre = depth_now[1:-1, 1:-1]
    sources = (
        None,
        -0.5 * gravity * centre * (slope_x[:, 1:] + slope_x[:, :-1]),
        -0.5 * gravity * centre * (slope_y[1:] + slope_y[:-1]),
    )
    results = []
    for plane in range(3):
        state = padded[plane]
        flux_col = fluxes_x[plane]
        flux_row = fluxes_y[plane]
        face_x = (
            0.5 * (flux_col[1:-1, :-1] + flux_col[1:-1, 1:])
            - 0.5 * bound_x * (state[1:-1, 1:] - state[1:-1, :-1])
        ) * open_x
        face_y = (
            0.5 * (flux_row[:-1, 1:-1] + flux_row[1:, 1:-1])
            - 0.5 * bound_y * (state[1:, 1:-1] - state[:-1, 1:-1])
        ) * open_y
        value = (
            state[1:-1, 1:-1]
            - courant * (face_x[:, 1:] - face_x[:, :-1])
            - courant * (face_y[1:] - face_y[:-1])
        )
        if plane > 0:
            value = value + courant * sources[plane]
        results.append(value)
    return jnp.stack(results)


def expand(cells):
    return jnp.repeat(jnp.repeat(cells, 3, axis=-2), 3, axis=-1)


def lookup(classes, levels):
    ladder = jnp.arange(levels.shape[0], dtype=jnp.int32)
    matches = classes[None] == ladder[:, None, None]
    return jnp.sum(jnp.where(matches, levels[:, None, None], 0.0), axis=0)


def restrict(updated):
    planes, row_count, col_count = updated.shape
    return updated.reshape(planes, row_count // 3, 3, col_count // 3, 3).sum(axis=(2, 4)) / 9.0


def local_general(strips, anchor, wet_mask, bathy_index, bed_levels, coarse):
    tile_blocks = strips.shape[2]
    band_rows = strips.shape[4]
    full_cols = strips.shape[5]
    columns = lax.axis_size("col")
    tile_cols = full_cols // columns
    layered = (
        strips[0, :, :, 0]
        .reshape(3, tile_blocks, band_rows, columns, tile_cols)
        .transpose(0, 1, 3, 2, 4)
    )
    flattened = layered.reshape(3, tile_blocks * columns, band_rows, tile_cols)
    arrived = lax.all_to_all(flattened, ("row", "col"), split_axis=1, concat_axis=1, tiled=True)
    fields = arrived.reshape(3, tile_blocks * columns * band_rows, tile_cols)
    bed_fine = expand(lookup(bathy_index[0], bed_levels))
    wetness = expand(wet_mask[0].astype(F32))
    stacked = jnp.concatenate([fields, bed_fine[None], wetness[None]], axis=0)
    padded_all = padded_2(stacked, (("row", 1), ("col", 2)), 1)
    updated = advance(padded_all[:3], padded_all[3], padded_all[4])
    restricted = restrict(updated)
    coarse_rows = restricted.shape[1]
    coarse_cols = restricted.shape[2]
    contribution = jnp.concatenate(
        [restricted, jnp.ones((1, coarse_rows, coarse_cols), F32)], axis=0
    )
    nest_index = lax.axis_index("nest")
    corner = lax.dynamic_index_in_dim(anchor, nest_index, 0, keepdims=False)
    canvas = lax.dynamic_update_slice(
        jnp.zeros((4, 2 * coarse_rows, 2 * coarse_cols), F32),
        contribution,
        (jnp.int32(0), corner[0], corner[1]),
    )
    spilled = passed_along(canvas[:, :, coarse_cols:], "col", 1)
    merged = canvas[:, :, :coarse_cols] + spilled
    lowered = passed_along(merged[:, coarse_rows:], ("nest", "row"), 1)
    received_sum = merged[:, :coarse_rows] + lowered
    coarse_next = (coarse + received_sum[:3]) / (1.0 + received_sum[3])
    return (updated[None], coarse_next)


def halo_rows(dims, d):
    return d // dims[2] != dims[0] - 1


def message_rows(dims, d):
    blocks, band, columns, lane_blocks = dims
    return 3 * lane_blocks * band + (16 if halo_rows(dims, d) else 8)


def half_rows(row):
    return pltpu.roll(row, 64, 1), row


def from_half_rows(block, at, lane):
    upper = block[at : at + 1]
    return jnp.where(lane < 64, pltpu.roll(upper, 64, 1), block[at + 1 : at + 2])


def pack_body(dims, ds, after, strips_hbm, wet_hbm, class_hbm, levels_hbm, *rest):
    blocks, band, columns, lane_blocks = dims
    rest = rest[after:]
    outs = rest[: len(ds)]
    strips, tiles, wet_ref, class_ref, levels_ref, sems, small = rest[len(ds) :]
    tile_cols = lane_blocks * 128
    me = lax.axis_index(("row", "col")).astype(jnp.int32)
    my_row = me // columns
    my_col = me % columns
    loads = [
        pltpu.make_async_copy(wet_hbm, wet_ref, small.at[0]),
        pltpu.make_async_copy(class_hbm, class_ref, small.at[1]),
        pltpu.make_async_copy(levels_hbm, levels_ref, small.at[2]),
    ]
    for c in loads:
        c.start()
    first = me == 0
    groups = sorted({d // columns for d in ds})
    copies = []
    for n, r in enumerate(groups):
        j = my_row ^ r
        jj = jnp.clip(jnp.where(first, j + 1, j - 1), 0, blocks - 1)
        edge = pl.ds(pl.multiple_of(jnp.where(first, 0, band - 8), 8), 8)
        copies.append(
            (
                pltpu.make_async_copy(strips_hbm.at[0, :, j, 0], strips.at[n], sems.at[0, n]),
                pltpu.make_async_copy(strips_hbm.at[0, :, jj, 0, edge], tiles.at[n], sems.at[1, n]),
            )
        )
    for pair in copies:
        for c in pair:
            c.start()
    lane = lax.broadcasted_iota(jnp.int32, (8, 128), 1)
    sub = lax.broadcasted_iota(jnp.int32, (8, 128), 0)
    size = wet_ref.shape[1]
    diag = lax.broadcasted_iota(jnp.int32, (size, 128), 0) == lax.broadcasted_iota(
        jnp.int32, (size, 128), 1
    )
    for c in loads:
        c.wait()
    edges = []
    for ref in (wet_ref, class_ref):
        cells = ref[0].astype(F32)
        north = cells[0:1]
        south = cells[size - 1 : size]
        west = jnp.sum(jnp.where(diag, cells[:, 0:1], 0.0), axis=0, keepdims=True)
        east = jnp.sum(jnp.where(diag, cells[:, 127:128], 0.0), axis=0, keepdims=True)
        four = (north, south, west, east)
        if ref is class_ref:
            four = tuple(level_of(row, levels_ref) for row in four)
        edges.append(four)
    body_rows = 3 * lane_blocks * band
    waiting = list(groups)
    mixes = []
    for out, d in zip(outs, ds):
        n = groups.index(d // columns)
        if groups[n] in waiting:
            copies[n][0].wait()
            waiting.remove(groups[n])
        to = me ^ d
        j = to // columns
        c = to % columns
        base = pl.multiple_of(c * tile_cols, 128)
        for k in range(3):
            for q in range(lane_blocks):
                at = (k * lane_blocks + q) * band
                out[at : at + band] = strips[n, k, :, pl.ds(pl.multiple_of(base + q * 128, 128), 128)]
        west_at = pl.multiple_of(jnp.maximum(base - 128, 0), 128)
        east_at = pl.multiple_of(jnp.where(c == columns - 1, base, base + tile_cols), 128)
        mixed = jnp.zeros((8, 128), F32)
        for g in range(band // 8):
            for k in range(3):
                i = g * 3 + k
                west = strips[n, k, g * 8 : g * 8 + 8, pl.ds(west_at, 128)]
                east = strips[n, k, g * 8 : g * 8 + 8, pl.ds(east_at, 128)]
                both = pltpu.roll(jnp.where(lane == 127, west, east), 2 * i + 1, 1)
                mixed = jnp.where((lane == 2 * i) | (lane == 2 * i + 1), both, mixed)
        mixes.append(mixed)
    for pair in copies:
        pair[1].wait()
    for out, d, mixed in zip(outs, ds, mixes):
        n = groups.index(d // columns)
        to = me ^ d
        j = to // columns
        c = to % columns
        base = pl.multiple_of(c * tile_cols, 128)
        tucked = [jnp.zeros((1, 128), F32)]
        if halo_rows(dims, d):
            rows = []
            for k in range(3):
                for q in range(lane_blocks):
                    spot = pl.ds(pl.multiple_of(base + q * 128, 128), 128)
                    tile = tiles[n, k, :, spot]
                    rows.append(jnp.where(first, tile[0:1], tile[7:8]))
            halo = jnp.zeros((8, 128), F32)
            for i in range(8):
                halo = jnp.where(sub == i, rows[i], halo)
            out[body_rows + 8 : body_rows + 16] = halo
            tucked = [rows[8]]
        for north, south, west, east in edges:
            row = jnp.where(
                c == my_col,
                jnp.where(j > my_row, south, north),
                jnp.where(c > my_col, east, west),
            )
            tucked.append(row)
        for t, row in enumerate(tucked):
            low, high = half_rows(row)
            mixed = jnp.where((sub == 2 * t) & (lane >= 64), low, mixed)
            mixed = jnp.where((sub == 2 * t + 1) & (lane >= 64), high, mixed)
        out[body_rows : body_rows + 8] = mixed


def spread(rows, cols, width, offset=None):
    i = lax.broadcasted_iota(jnp.int32, (rows, cols), 0)
    m = lax.broadcasted_iota(jnp.int32, (rows, cols), 1)
    if offset is not None:
        m = m - offset
        m = jnp.where(m < 0, m + cols, m)
    low = m * width
    return jnp.where((i >= low) & (i < low + width), 1.0, 0.0)


def spread_t(rows, cols, width, offset=None):
    m = lax.broadcasted_iota(jnp.int32, (rows, cols), 0)
    i = lax.broadcasted_iota(jnp.int32, (rows, cols), 1)
    if offset is not None:
        m = m - offset
        m = jnp.where(m < 0, m + rows, m)
    low = m * width
    return jnp.where((i >= low) & (i < low + width), 1.0, 0.0)


def level_of(classes, levels_ref):
    out = jnp.zeros_like(classes)
    for n in range(levels_ref.shape[0]):
        out = jnp.where(classes == n, levels_ref[n], out)
    return out


def prep_body(columns, levels_ref, anchor_ref, wet_ref, class_ref, wet_out, bed_out, weights):
    lane_blocks, rows, _ = wet_out.shape
    size, width = wet_ref.shape[1], wet_ref.shape[2]
    wet = wet_ref[0].astype(F32)
    bed = level_of(class_ref[0].astype(F32), levels_ref)
    across = spread_t(width, lane_blocks * 128, 3)
    down = spread(rows, size, 3)
    for out, cells, parts in ((wet_out, wet, 1), (bed_out, bed, 3)):
        fine = mul_left(down, mul_right(cells, across, parts), parts)
        for q in range(lane_blocks):
            out[q] = fine[:, q * 128 : q * 128 + 128]
    nest = lax.axis_index("nest").astype(jnp.int32)
    row_at = lax.axis_index("row").astype(jnp.int32)
    col_at = lax.axis_index("col").astype(jnp.int32)
    up_nest = jnp.where(row_at == 0, jnp.maximum(nest - 1, 0), nest)
    i = lax.broadcasted_iota(jnp.int32, weights.shape[1:], 0)
    m = lax.broadcasted_iota(jnp.int32, weights.shape[1:], 1)
    has_left = jnp.where(col_at > 0, 1.0, 0.0)
    has_up = jnp.where((row_at > 0) | (nest > 0), 1.0, 0.0)
    own_rows = jnp.where(i >= anchor_ref[nest, 0], 1.0, 0.0)
    up_rows = jnp.where(i < anchor_ref[up_nest, 0], has_up, 0.0)
    own_cols = m >= anchor_ref[nest, 1]
    up_cols = m >= anchor_ref[up_nest, 1]
    shares = (
        jnp.where(own_cols, own_rows, 0.0),
        jnp.where(own_cols, 0.0, own_rows * has_left),
        jnp.where(up_cols, up_rows, 0.0),
        jnp.where(up_cols, 0.0, up_rows * has_left),
    )
    scale = 1.0 / (1.0 + shares[0] + shares[1] + shares[2] + shares[3])
    weights[0] = scale
    for n, share in enumerate(shares):
        weights[n + 1] = share * scale


def split(x, parts):
    out = []
    for n in range(parts):
        piece = x.astype(jnp.bfloat16)
        out.append(piece)
        if n + 1 < parts:
            x = x - piece.astype(F32)
    return out


def mul_left(matrix, x, parts):
    matrix = matrix.astype(jnp.bfloat16)
    return sum(jnp.dot(matrix, piece, preferred_element_type=F32) for piece in split(x, parts))


def mul_right(x, matrix, parts):
    matrix = matrix.astype(jnp.bfloat16)
    return sum(jnp.dot(piece, matrix, preferred_element_type=F32) for piece in split(x, parts))


def mul_left_t(matrix, x, parts):
    matrix = matrix.astype(jnp.bfloat16)
    return sum(
        lax.dot_general(matrix, piece, (((1,), (1,)), ((), ())), preferred_element_type=F32)
        for piece in split(x, parts)
    )


def unpack(dims, me, first_row, messages, ds, field, extra):
    blocks, band, columns, lane_blocks = dims
    body_rows = 3 * lane_blocks * band
    for message, d in zip(messages, ds):
        p = me ^ d
        top = pl.multiple_of(8 + p * band - first_row, 8)
        mixed = message[body_rows : body_rows + 8]
        for k in range(3):
            for q in range(lane_blocks):
                n = k * lane_blocks + q
                field[k, q, pl.ds(top, band)] = message[
                    n * band : n * band + band
                ]
            for g in range(band // 8):
                i = g * 3 + k
                at = pl.multiple_of(top + g * 8, 8)
                field[k, lane_blocks, pl.ds(at, 8)] = pltpu.roll(mixed, 127 - 2 * i, 1)
        extra[p, 0:8] = mixed
        if halo_rows(dims, d):
            extra[p, 8:16] = message[body_rows + 8 : body_rows + 16]


def edge_rows(dims, extra, source, inside):
    blocks, band, columns, lane_blocks = dims
    lane = lax.broadcasted_iota(jnp.int32, (1, 128), 1)
    block = extra[jnp.where(inside, source, 0), 0:8]
    wet_row = from_half_rows(block, 2, lane)
    bed_row = from_half_rows(block, 4, lane)
    return jnp.where(inside, wet_row, 0.0), jnp.where(inside, bed_row, 0.0)


def side_cells(dims, me, extra, wet_side, bed_side):
    columns = dims[2]
    my_col = me % columns
    west = edge_rows(dims, extra, me - 1, my_col > 0)
    east = edge_rows(dims, extra, me + 1, my_col < columns - 1)
    sub = lax.broadcasted_iota(jnp.int32, (128, 128), 0)
    pair = jnp.zeros((128, 128), F32)
    for n, row in ((0, east[0]), (127, west[0]), (64, east[1]), (63, west[1])):
        pair = jnp.where(sub == n, row, pair)
    sides = mul_left_t(spread(wet_side.shape[0], 128, 3), pair, 3)
    wet_side[...] = sides
    bed_side[...] = pltpu.roll(sides, 64, 1)


def slopes(lane_blocks, wet, bed, wet_side, bed_side, open_x, slope_x, rows):
    lane = lax.broadcasted_iota(jnp.int32, (8, 128), 1)
    sides = lane_blocks + 1

    def step(t, _):
        at = pl.ds(pl.multiple_of(t * 8, 8), 8)
        w = [wet[q, at] for q in range(lane_blocks)] + [wet_side[at]]
        z = [bed[q, at] for q in range(lane_blocks)] + [bed_side[at]]
        steps = []
        for q in range(sides):
            w2, z2 = (
                pltpu.roll(jnp.where(lane == 0, x[(q + 1) % sides], x[q]), 127, 1) for x in (w, z)
            )
            half = (0.5 * courant) * (w[q] * w2)
            open_x[q, at] = half
            steps.append(half * (z2 - z[q]))
        for q in range(lane_blocks):
            left = pltpu.roll(jnp.where(lane == 127, steps[q - 1], steps[q]), 1, 1)
            slope_x[q, at] = gravity * (steps[q] + left)
        return 0

    lax.fori_loop(0, rows // 8, step, 0, unroll=2)


def sweep(dims, field, wet, bed, wet_at, open_x, slope_x, open_at, more, made, fine, start, count, unroll):
    lane_blocks = dims[3]
    sides = lane_blocks + 1
    lane = lax.broadcasted_iota(jnp.int32, (8, 128), 1)
    sub = lax.broadcasted_iota(jnp.int32, (8, 128), 0)

    def rates(h, hu, hv):
        root = lax.rsqrt(h)
        inv = root * root
        u = hu * inv
        c = (gravity**0.5) * (h * root)
        p = (0.5 * gravity) * (h * h)
        return hu * u + p, hv * u, jnp.abs(u) + c, inv, c, p

    def cells(group, q):
        at = pl.ds(pl.multiple_of(8 + group * 8, 8), 8)
        h, hu, hv = (field[k, q, at] for k in range(3))
        f2, m, a, inv, c, p = rates(h, hu, hv)
        if q < lane_blocks:
            v = hv * inv
            more[0, q, at] = m
            more[1, q, at] = hv * v + p
            more[2, q, at] = jnp.abs(v) + c
        return h, hu, hv, f2, m, a

    def face(half, near, far):
        bound = half * jnp.maximum(near[6], far[6])
        return [half * (near[3 + k] + far[3 + k]) - bound * (far[k] - near[k]) for k in range(3)]

    def across(t, _):
        group = start + t
        spot = pl.ds(pl.multiple_of(group * 8, 8), 8)
        opened = pl.ds(pl.multiple_of(open_at + group * 8, 8), 8)
        blocks = [cells(group, q) for q in range(sides)]
        faces = []
        for q in range(sides):
            now, nxt = blocks[q], blocks[(q + 1) % sides]
            h, hu, hv, f2, m, a = now
            h2, hu2, hv2 = (
                pltpu.roll(jnp.where(lane == 0, y, x), 127, 1) for x, y in zip(now[:3], nxt[:3])
            )
            f22, m2, a2 = rates(h2, hu2, hv2)[:3]
            faces.append(
                face(open_x[q, opened], (h, hu, hv, hu, f2, m, a), (h2, hu2, hv2, hu2, f22, m2, a2))
            )
        for q in range(lane_blocks):
            right = faces[q]
            left = [
                pltpu.roll(jnp.where(lane == 127, y, x), 1, 1) for x, y in zip(right, faces[q - 1])
            ]
            h, hu, hv = blocks[q][:3]
            made[0, q, spot] = h - (right[0] - left[0])
            made[1, q, spot] = hu - (right[1] - left[1]) - h * slope_x[q, opened]
            made[2, q, spot] = hv - (right[2] - left[2])
        return 0

    def south_face(group, q):
        at = pl.multiple_of(8 + group * 8, 8)
        w_at = pl.multiple_of(wet_at + group * 8, 8)
        sides = []
        for step in range(2):
            rows = pl.ds(at + step, 8)
            h, hu, hv = (field[k, q, rows] for k in range(3))
            m, g3, b = (more[k, q, rows] for k in range(3))
            sides.append((h, hu, hv, hv, m, g3, b))
        half = (0.5 * courant) * (wet[q, pl.ds(w_at, 8)] * wet[q, pl.ds(w_at + 1, 8)])
        slope = half * (bed[q, pl.ds(w_at + 1, 8)] - bed[q, pl.ds(w_at, 8)])
        return face(half, *sides) + [slope]

    def down(t, above):
        group = start + t
        spot = pl.ds(pl.multiple_of(group * 8, 8), 8)
        new = []
        for q in range(lane_blocks):
            below = south_face(group, q)
            up = [
                pltpu.roll(jnp.where(sub == 7, y, x), 1, 0) for x, y in zip(below, above[q])
            ]
            h = field[0, q, pl.ds(pl.multiple_of(8 + group * 8, 8), 8)]
            done = [made[k, q, spot] - (below[k] - up[k]) for k in range(3)]
            done[2] = done[2] - gravity * h * (below[3] + up[3])
            for k in range(3):
                made[k, q, spot] = done[k]
                if fine is not None:
                    fine[0, k, spot, q * 128 : q * 128 + 128] = done[k]
            new.append(below)
        return new

    for q in range(lane_blocks):
        cells(start - 1, q)
        cells(start + count, q)
    if count == 1:
        across(0, 0)
        down(0, [south_face(start - 1, q) for q in range(lane_blocks)])
    else:
        lax.fori_loop(0, count, across, 0, unroll=unroll)
        above = [south_face(start - 1, q) for q in range(lane_blocks)]
        lax.fori_loop(0, count, down, above, unroll=unroll)


def half_body(dims, ds, wet_in, bed_in, *rest):
    blocks, band, columns, lane_blocks = dims
    owners = blocks * columns
    messages = rest[: len(ds)]
    made, open_x, slope_x, field, wet_side, bed_side, more, extra = rest[len(ds) :]
    rows = owners * band // 2
    me = lax.axis_index(("row", "col")).astype(jnp.int32)
    first_row = pl.multiple_of((me * 2 // owners) * rows, 8)
    unpack(dims, me, first_row, messages, ds, field, extra)
    side_cells(dims, me, extra, wet_side, bed_side)
    slopes(lane_blocks, wet_in, bed_in, wet_side, bed_side, open_x, slope_x, 2 * rows)
    for k in range(3):
        for q in range(lane_blocks):
            made[k, q, 0:8] = jnp.zeros((8, 128), F32)
            made[k, q, rows - 8 : rows] = jnp.zeros((8, 128), F32)
    sweep(
        dims, field, wet_in, bed_in, first_row, open_x, slope_x, first_row, more, made, None, 1, rows // 8 - 2, 2
    )


def main_body(dims, ds, anchor_hbm, wet_in, bed_in, half_in, open_x, slope_x, *rest):
    blocks, band, columns, lane_blocks = dims
    owners = blocks * columns
    messages = rest[:owners]
    fine_out, rolled_out = rest[owners : owners + 2]
    field, wet, bed, more, extra, made, anchor_ref, sem_in = rest[owners + 2 :]
    rows = owners * band
    cols = lane_blocks * 128
    me = lax.axis_index(("row", "col")).astype(jnp.int32)
    nest = lax.axis_index("nest").astype(jnp.int32)
    my_row = me // columns
    done_half = me * 2 // owners
    half_rows_at = pl.multiple_of(done_half * (rows // 2), 8)
    corners = pltpu.make_async_copy(anchor_hbm, anchor_ref, sem_in)
    corners.start()

    for k in range(3):
        for q in range(lane_blocks):
            made[k, q, pl.ds(half_rows_at, rows // 2)] = half_in[k, q]
            fine_out[0, k, pl.ds(half_rows_at, rows // 2), q * 128 : q * 128 + 128] = half_in[k, q]
    lane1 = lax.broadcasted_iota(jnp.int32, (1, 128), 1)
    for q in range(lane_blocks):
        wet[q, 8 : 8 + rows] = wet_in[q]
        bed[q, 8 : 8 + rows] = bed_in[q]
    unpack(dims, me, 0, messages, ds, field, extra)

    for source, at, inside, near in (
        (owners - 1, 0, my_row > 0, 8),
        (0, 8 + rows, my_row < blocks - 1, rows),
    ):
        last = from_half_rows(extra[source, 0:8], 0, lane1)
        for k in range(3):
            for q in range(lane_blocks):
                n = k * lane_blocks + q
                row = last if n == 8 else extra[source, 8 + n : 9 + n]
                row = jnp.broadcast_to(row, (8, 128))
                field[k, q, at : at + 8] = jnp.where(inside, row, field[k, q, near : near + 8])
    north = edge_rows(dims, extra, me - columns, my_row > 0)
    south = edge_rows(dims, extra, me + columns, my_row < blocks - 1)
    sub8 = lax.broadcasted_iota(jnp.int32, (8, 128), 0)
    stack = jnp.zeros((8, 128), F32)
    for n, row in enumerate((north[0], north[1], south[0], south[1])):
        stack = jnp.where(sub8 == n, row, stack)
    ends = mul_right(stack, spread_t(128, cols, 3), 3)
    for n, (ref, at) in enumerate(((wet, 0), (bed, 0), (wet, 8 + rows), (bed, 8 + rows))):
        for q in range(lane_blocks):
            ref[q, at : at + 8] = jnp.broadcast_to(ends[n : n + 1, q * 128 : q * 128 + 128], (8, 128))

    groups = rows // 8
    one = done_half * (groups - 1)
    along = (dims, field, wet, bed, 8, open_x, slope_x, 0, more, made, fine_out)
    sweep(*along, one, 1, 1)
    many = (1 - done_half) * (groups // 2 - 1)
    sweep(*along, many, groups // 2 + 1, 5)
    corners.wait()
    coarse_rows = rows // 3
    coarse_cols = cols // 3
    a0 = anchor_ref[nest, 0]
    a1 = anchor_ref[nest, 1]
    gather_cols = spread(cols, coarse_cols, 3, a1)
    for k in range(3):
        total = jnp.concatenate(
            [
                sum(made[k, q, pl.ds(n, coarse_rows, stride=3), :] for n in range(3))
                for q in range(lane_blocks)
            ],
            axis=1,
        )
        mean = mul_right(total, gather_cols, 2) * (1.0 / 9.0)
        rolled_out[k] = pltpu.roll(mean, a0, 0)


def finish_body(coarse, weights, left, up, diagonal, own, out):
    for k in range(3):
        out[k] = (
            coarse[k] * weights[0]
            + own[k] * weights[1]
            + left[k] * weights[2]
            + up[k] * weights[3]
            + diagonal[k] * weights[4]
        )


def in_vmem(x):
    return pltpu.with_memory_space_constraint(x, pltpu.VMEM)


def in_hbm(x):
    return pltpu.with_memory_space_constraint(x, pltpu.HBM)


SMEM = pl.BlockSpec(memory_space=pltpu.SMEM)
VMEM = pl.BlockSpec(memory_space=pltpu.VMEM)
HBM = pl.BlockSpec(memory_space=pltpu.HBM)


def half_call(dims, ds, wet_fine, bed_fine, messages):
    blocks, band, columns, lane_blocks = dims
    owners = blocks * columns
    rows = owners * band // 2
    return pl.pallas_call(
        lambda *refs: half_body(dims, ds, *refs),
        in_specs=[VMEM, VMEM] + [VMEM] * len(ds),
        out_specs=[VMEM] * 3,
        out_shape=[
            pltpu.VMEM((3, lane_blocks, rows, 128), F32),
            pltpu.VMEM((lane_blocks + 1, 2 * rows, 128), F32),
            pltpu.VMEM((lane_blocks, 2 * rows, 128), F32),
        ],
        scratch_shapes=[
            pltpu.VMEM((3, lane_blocks + 1, rows + 16, 128), F32),
            pltpu.VMEM((2 * rows, 128), F32),
            pltpu.VMEM((2 * rows, 128), F32),
            pltpu.VMEM((3, lane_blocks, rows + 16, 128), F32),
            pltpu.VMEM((owners, 16, 128), F32),
        ],
        name="half", compiler_params=pltpu.CompilerParams(vmem_limit_bytes=12 << 20),
    )(wet_fine, bed_fine, *messages)


def main_call(dims, ds, anchor, wet_fine, bed_fine, half, open_x, slope_x, messages):
    blocks, band, columns, lane_blocks = dims
    owners = blocks * columns
    rows = owners * band
    cols = lane_blocks * 128
    return pl.pallas_call(
        lambda *refs: main_body(dims, ds, *refs),
        in_specs=[HBM] + [VMEM] * (5 + owners),
        out_specs=[VMEM, VMEM],
        out_shape=[
            pltpu.VMEM((1, 3, rows, cols), F32),
            pltpu.VMEM((3, rows // 3, cols // 3), F32),
        ],
        scratch_shapes=[
            pltpu.VMEM((3, lane_blocks + 1, rows + 16, 128), F32),
            pltpu.VMEM((lane_blocks, rows + 16, 128), F32),
            pltpu.VMEM((lane_blocks, rows + 16, 128), F32),
            pltpu.VMEM((3, lane_blocks, rows + 16, 128), F32),
            pltpu.VMEM((owners, 16, 128), F32),
            pltpu.VMEM((3, lane_blocks, rows, 128), F32),
            pltpu.SMEM((2, 2), jnp.int32),
            pltpu.SemaphoreType.DMA,
        ],
        name="main", compiler_params=pltpu.CompilerParams(vmem_limit_bytes=20 << 20),
    )(anchor, wet_fine, bed_fine, half, open_x, slope_x, *messages)


def local_packed(strips, anchor, wet_mask, bathy_index, bed_levels, coarse):
    blocks, band, full_cols = strips.shape[2], strips.shape[4], strips.shape[5]
    columns = lax.axis_size("col")
    owners = blocks * columns
    cols = full_cols // columns
    lane_blocks = cols // 128
    rows = owners * band
    dims = (blocks, band, columns, lane_blocks)
    half_owners = owners // 2

    def rank(d):
        r, c = d // columns, d % columns
        turn = 1 if c * 2 < columns else 2 if r == blocks - 1 else 0
        return (d >= half_owners, turn, r, c)

    wanted = sorted(range(1, owners), key=rank)
    opening = [d for d in wanted if d < columns and d * 2 >= columns]
    rest = [d for d in range(half_owners) if d not in opening]
    messages = {}
    after = []
    for ds in (opening, rest, list(range(half_owners, owners))):
        count = len({d // columns for d in ds})
        made = pl.pallas_call(
            lambda *refs, ds=ds, after=len(after): pack_body(dims, ds, after, *refs),
            in_specs=[HBM] * 4 + [VMEM] * len(after),
            out_specs=[VMEM] * len(ds),
            out_shape=[pltpu.VMEM((message_rows(dims, d), 128), F32) for d in ds],
            scratch_shapes=[
                pltpu.VMEM((count, 3, band, full_cols), F32),
                pltpu.VMEM((count, 3, 8, full_cols), F32),
                pltpu.VMEM(wet_mask.shape, jnp.int32),
                pltpu.VMEM(bathy_index.shape, jnp.int32),
                pltpu.SMEM(bed_levels.shape, F32),
                pltpu.SemaphoreType.DMA((2, count)),
                pltpu.SemaphoreType.DMA((3,)),
            ],
            name="pack",
            compiler_params=pltpu.CompilerParams(vmem_limit_bytes=10 << 20),
        )(
            in_hbm(strips),
            in_hbm(wet_mask),
            in_hbm(bathy_index),
            in_hbm(bed_levels),
            *after,
        )
        messages.update(zip(ds, (in_vmem(x) for x in made)))
        after = [messages[ds[0]]]

    arrived = {
        d: lax.ppermute(messages[d], ("row", "col"), [(i, i ^ d) for i in range(owners)])
        for d in wanted
    }
    arrived[0] = messages[0]
    arrived = {d: in_vmem(x) if d else x for d, x in arrived.items()}

    coarse_rows = rows // 3
    coarse_cols = cols // 3
    wet_fine, bed_fine, weights = pl.pallas_call(
        lambda *refs: prep_body(columns, *refs),
        in_specs=[SMEM, SMEM, VMEM, VMEM],
        out_specs=[VMEM] * 3,
        out_shape=[pltpu.VMEM((lane_blocks, rows, 128), F32)] * 2
        + [pltpu.VMEM((5, coarse_rows, coarse_cols), F32)],
        name="prep", compiler_params=pltpu.CompilerParams(vmem_limit_bytes=12 << 20),
    )(bed_levels, anchor, wet_mask, bathy_index)

    early = [0] + wanted[: half_owners - 1]
    order = [0] + wanted
    wet_fine, bed_fine, weights = in_vmem(wet_fine), in_vmem(bed_fine), in_vmem(weights)
    half, open_x, slope_x = half_call(dims, early, wet_fine, bed_fine, [arrived[d] for d in early])
    half, open_x, slope_x = in_vmem(half), in_vmem(open_x), in_vmem(slope_x)
    fine, rolled = main_call(
        dims,
        order,
        in_hbm(anchor),
        wet_fine,
        bed_fine,
        half,
        open_x,
        slope_x,
        [arrived[d] for d in order],
    )
    rolled = in_vmem(rolled)

    lines = lax.axis_size("nest") * lax.axis_size("row")
    rights = [(c, c + 1) for c in range(columns - 1)]
    downs = [(l, l + 1) for l in range(lines - 1)]
    both = [(l * columns + c, l2 * columns + c2) for l, l2 in downs for c, c2 in rights]
    diagonal = lax.ppermute(rolled, ("nest", "row", "col"), both)
    from_left = lax.ppermute(rolled, "col", rights)
    from_up = lax.ppermute(rolled, ("nest", "row"), downs)

    coarse_next = pl.pallas_call(
        finish_body,
        in_specs=[VMEM] * 6,
        out_specs=VMEM,
        out_shape=jax.ShapeDtypeStruct(coarse.shape, F32),
        name="finish", compiler_params=pltpu.CompilerParams(vmem_limit_bytes=4 << 20),
    )(
        in_vmem(coarse),
        weights,
        in_vmem(from_left),
        in_vmem(from_up),
        in_vmem(diagonal),
        rolled,
    )
    return (fine, coarse_next)


def local(strips, anchor, wet_mask, bathy_index, bed_levels, coarse):
    columns = lax.axis_size("col")
    owners = strips.shape[2] * columns
    cols = strips.shape[5] // columns
    band = strips.shape[4]
    fits = (
        owners & (owners - 1) == 0
        and 2 <= owners <= 16
        and strips.shape[2] == lax.axis_size("row")
        and band == 24
        and cols == 384
        and owners * band == 384
        and wet_mask.shape[1:] == (128, 128)
    )
    run = local_packed if fits else local_general
    return run(strips, anchor, wet_mask, bathy_index, bed_levels, coarse)


def solution(mesh):
    return jax.shard_map(
        local,
        mesh=mesh,
        in_specs=(
            P("nest", None, None, ("row", "col"), None, None),
            P(),
            P("nest", "row", "col"),
            P("nest", "row", "col"),
            P(),
            P(None, ("nest", "row"), "col"),
        ),
        out_specs=(P("nest", None, "row", "col"), P(None, ("nest", "row"), "col")),
        check_vma=False,
    )
```

```python
import jax
import jax.numpy as jnp
from jax import lax
from jax.experimental import pallas as pl
from jax.experimental.pallas import tpu as pltpu
from jax.sharding import PartitionSpec as P


gravity = 1.0
courant = 0.2
F32 = jnp.float32


def padded_2(cells, sides, width):
    for axis, dim in sides:
        count = lax.axis_size(axis)
        ends = count - 1
        head = lax.slice_in_dim(cells, 0, width, axis=dim)
        tail = lax.slice_in_dim(cells, cells.shape[dim] - width, cells.shape[dim], axis=dim)
        cells = jnp.concatenate(
            [
                lax.ppermute(tail, axis, [(i, (i + 1) % count) for i in range(ends)]),
                cells,
                lax.ppermute(head, axis, [((i + 1) % count, i) for i in range(ends)]),
            ],
            axis=dim,
        )
    return cells


def passed_along(block, axis, distance):
    devices = range(lax.axis_size(axis))
    route = [(i - distance, i) for i in devices if i - distance in devices]
    return lax.ppermute(block, axis, route)


def advance(padded, bed_pad, wet_pad):
    depth_now = padded[0]
    flow_u = padded[1]
    flow_v = padded[2]
    depth_safe = jnp.where(wet_pad > 0.5, depth_now, 1.0)
    speed_u = flow_u / depth_safe
    speed_v = flow_v / depth_safe
    celerity = jnp.sqrt(gravity * depth_safe)
    pressure = 0.5 * gravity * depth_safe * depth_safe
    fluxes_x = (flow_u, flow_u * speed_u + pressure, flow_v * speed_u)
    fluxes_y = (flow_v, flow_u * speed_v, flow_v * speed_v + pressure)
    reach_x = jnp.abs(speed_u) + celerity
    reach_y = jnp.abs(speed_v) + celerity
    open_x = wet_pad[1:-1, :-1] * wet_pad[1:-1, 1:]
    open_y = wet_pad[:-1, 1:-1] * wet_pad[1:, 1:-1]
    bound_x = jnp.maximum(reach_x[1:-1, :-1], reach_x[1:-1, 1:])
    bound_y = jnp.maximum(reach_y[:-1, 1:-1], reach_y[1:, 1:-1])
    slope_x = (bed_pad[1:-1, 1:] - bed_pad[1:-1, :-1]) * open_x
    slope_y = (bed_pad[1:, 1:-1] - bed_pad[:-1, 1:-1]) * open_y
    centre = depth_now[1:-1, 1:-1]
    sources = (
        None,
        -0.5 * gravity * centre * (slope_x[:, 1:] + slope_x[:, :-1]),
        -0.5 * gravity * centre * (slope_y[1:] + slope_y[:-1]),
    )
    results = []
    for plane in range(3):
        state = padded[plane]
        flux_col = fluxes_x[plane]
        flux_row = fluxes_y[plane]
        face_x = (
            0.5 * (flux_col[1:-1, :-1] + flux_col[1:-1, 1:])
            - 0.5 * bound_x * (state[1:-1, 1:] - state[1:-1, :-1])
        ) * open_x
        face_y = (
            0.5 * (flux_row[:-1, 1:-1] + flux_row[1:, 1:-1])
            - 0.5 * bound_y * (state[1:, 1:-1] - state[:-1, 1:-1])
        ) * open_y
        value = (
            state[1:-1, 1:-1]
            - courant * (face_x[:, 1:] - face_x[:, :-1])
            - courant * (face_y[1:] - face_y[:-1])
        )
        if plane > 0:
            value = value + courant * sources[plane]
        results.append(value)
    return jnp.stack(results)


def expand(cells):
    return jnp.repeat(jnp.repeat(cells, 3, axis=-2), 3, axis=-1)


def lookup(classes, levels):
    ladder = jnp.arange(levels.shape[0], dtype=jnp.int32)
    matches = classes[None] == ladder[:, None, None]
    return jnp.sum(jnp.where(matches, levels[:, None, None], 0.0), axis=0)


def restrict(updated):
    planes, row_count, col_count = updated.shape
    return updated.reshape(planes, row_count // 3, 3, col_count // 3, 3).sum(axis=(2, 4)) / 9.0


def local_general(strips, anchor, wet_mask, bathy_index, bed_levels, coarse):
    tile_blocks = strips.shape[2]
    band_rows = strips.shape[4]
    full_cols = strips.shape[5]
    columns = lax.axis_size("col")
    tile_cols = full_cols // columns
    layered = (
        strips[0, :, :, 0]
        .reshape(3, tile_blocks, band_rows, columns, tile_cols)
        .transpose(0, 1, 3, 2, 4)
    )
    flattened = layered.reshape(3, tile_blocks * columns, band_rows, tile_cols)
    arrived = lax.all_to_all(flattened, ("row", "col"), split_axis=1, concat_axis=1, tiled=True)
    fields = arrived.reshape(3, tile_blocks * columns * band_rows, tile_cols)
    bed_fine = expand(lookup(bathy_index[0], bed_levels))
    wetness = expand(wet_mask[0].astype(F32))
    stacked = jnp.concatenate([fields, bed_fine[None], wetness[None]], axis=0)
    padded_all = padded_2(stacked, (("row", 1), ("col", 2)), 1)
    updated = advance(padded_all[:3], padded_all[3], padded_all[4])
    restricted = restrict(updated)
    coarse_rows = restricted.shape[1]
    coarse_cols = restricted.shape[2]
    contribution = jnp.concatenate(
        [restricted, jnp.ones((1, coarse_rows, coarse_cols), F32)], axis=0
    )
    nest_index = lax.axis_index("nest")
    corner = lax.dynamic_index_in_dim(anchor, nest_index, 0, keepdims=False)
    canvas = lax.dynamic_update_slice(
        jnp.zeros((4, 2 * coarse_rows, 2 * coarse_cols), F32),
        contribution,
        (jnp.int32(0), corner[0], corner[1]),
    )
    spilled = passed_along(canvas[:, :, coarse_cols:], "col", 1)
    merged = canvas[:, :, :coarse_cols] + spilled
    lowered = passed_along(merged[:, coarse_rows:], ("nest", "row"), 1)
    received_sum = merged[:, :coarse_rows] + lowered
    coarse_next = (coarse + received_sum[:3]) / (1.0 + received_sum[3])
    return (updated[None], coarse_next)


def halo_rows(dims, d):
    return d // dims[2] != dims[0] - 1


def message_rows(dims, d):
    blocks, band, columns, lane_blocks = dims
    return 3 * lane_blocks * band + (16 if halo_rows(dims, d) else 8)


def half_rows(row):
    return pltpu.roll(row, 64, 1), row


def from_half_rows(block, at, lane):
    upper = block[at : at + 1]
    return jnp.where(lane < 64, pltpu.roll(upper, 64, 1), block[at + 1 : at + 2])


def pack_body(dims, ds, after, strips_hbm, wet_hbm, class_hbm, levels_hbm, *rest):
    blocks, band, columns, lane_blocks = dims
    rest = rest[after:]
    outs = rest[: len(ds)]
    strips, tiles, wet_ref, class_ref, levels_ref, sems, small = rest[len(ds) :]
    tile_cols = lane_blocks * 128
    me = lax.axis_index(("row", "col")).astype(jnp.int32)
    my_row = me // columns
    my_col = me % columns
    loads = [
        pltpu.make_async_copy(wet_hbm, wet_ref, small.at[0]),
        pltpu.make_async_copy(class_hbm, class_ref, small.at[1]),
        pltpu.make_async_copy(levels_hbm, levels_ref, small.at[2]),
    ]
    for c in loads:
        c.start()
    first = me == 0
    groups = sorted({d // columns for d in ds})
    copies = []
    for n, r in enumerate(groups):
        j = my_row ^ r
        jj = jnp.clip(jnp.where(first, j + 1, j - 1), 0, blocks - 1)
        edge = pl.ds(pl.multiple_of(jnp.where(first, 0, band - 8), 8), 8)
        copies.append(
            (
                pltpu.make_async_copy(strips_hbm.at[0, :, j, 0], strips.at[n], sems.at[0, n]),
                pltpu.make_async_copy(strips_hbm.at[0, :, jj, 0, edge], tiles.at[n], sems.at[1, n]),
            )
        )
    for pair in copies:
        for c in pair:
            c.start()
    lane = lax.broadcasted_iota(jnp.int32, (8, 128), 1)
    sub = lax.broadcasted_iota(jnp.int32, (8, 128), 0)
    size = wet_ref.shape[1]
    diag = lax.broadcasted_iota(jnp.int32, (size, 128), 0) == lax.broadcasted_iota(
        jnp.int32, (size, 128), 1
    )
    for c in loads:
        c.wait()
    edges = []
    for ref in (wet_ref, class_ref):
        cells = ref[0].astype(F32)
        north = cells[0:1]
        south = cells[size - 1 : size]
        west = jnp.sum(jnp.where(diag, cells[:, 0:1], 0.0), axis=0, keepdims=True)
        east = jnp.sum(jnp.where(diag, cells[:, 127:128], 0.0), axis=0, keepdims=True)
        four = (north, south, west, east)
        if ref is class_ref:
            four = tuple(level_of(row, levels_ref) for row in four)
        edges.append(four)
    body_rows = 3 * lane_blocks * band
    waiting = list(groups)
    mixes = []
    for out, d in zip(outs, ds):
        n = groups.index(d // columns)
        if groups[n] in waiting:
            copies[n][0].wait()
            waiting.remove(groups[n])
        to = me ^ d
        j = to // columns
        c = to % columns
        base = pl.multiple_of(c * tile_cols, 128)
        for k in range(3):
            for q in range(lane_blocks):
                at = (k * lane_blocks + q) * band
                out[at : at + band] = strips[n, k, :, pl.ds(pl.multiple_of(base + q * 128, 128), 128)]
        west_at = pl.multiple_of(jnp.maximum(base - 128, 0), 128)
        east_at = pl.multiple_of(jnp.where(c == columns - 1, base, base + tile_cols), 128)
        mixed = jnp.zeros((8, 128), F32)
        for g in range(band // 8):
            for k in range(3):
                i = g * 3 + k
                west = strips[n, k, g * 8 : g * 8 + 8, pl.ds(west_at, 128)]
                east = strips[n, k, g * 8 : g * 8 + 8, pl.ds(east_at, 128)]
                both = pltpu.roll(jnp.where(lane == 127, west, east), 2 * i + 1, 1)
                mixed = jnp.where((lane == 2 * i) | (lane == 2 * i + 1), both, mixed)
        mixes.append(mixed)
    for pair in copies:
        pair[1].wait()
    for out, d, mixed in zip(outs, ds, mixes):
        n = groups.index(d // columns)
        to = me ^ d
        j = to // columns
        c = to % columns
        base = pl.multiple_of(c * tile_cols, 128)
        tucked = [jnp.zeros((1, 128), F32)]
        if halo_rows(dims, d):
            rows = []
            for k in range(3):
                for q in range(lane_blocks):
                    spot = pl.ds(pl.multiple_of(base + q * 128, 128), 128)
                    tile = tiles[n, k, :, spot]
                    rows.append(jnp.where(first, tile[0:1], tile[7:8]))
            halo = jnp.zeros((8, 128), F32)
            for i in range(8):
                halo = jnp.where(sub == i, rows[i], halo)
            out[body_rows + 8 : body_rows + 16] = halo
            tucked = [rows[8]]
        for north, south, west, east in edges:
            row = jnp.where(
                c == my_col,
                jnp.where(j > my_row, south, north),
                jnp.where(c > my_col, east, west),
            )
            tucked.append(row)
        for t, row in enumerate(tucked):
            low, high = half_rows(row)
            mixed = jnp.where((sub == 2 * t) & (lane >= 64), low, mixed)
            mixed = jnp.where((sub == 2 * t + 1) & (lane >= 64), high, mixed)
        out[body_rows : body_rows + 8] = mixed


def spread(rows, cols, width, offset=None):
    i = lax.broadcasted_iota(jnp.int32, (rows, cols), 0)
    m = lax.broadcasted_iota(jnp.int32, (rows, cols), 1)
    if offset is not None:
        m = m - offset
        m = jnp.where(m < 0, m + cols, m)
    low = m * width
    return jnp.where((i >= low) & (i < low + width), 1.0, 0.0)


def spread_t(rows, cols, width, offset=None):
    m = lax.broadcasted_iota(jnp.int32, (rows, cols), 0)
    i = lax.broadcasted_iota(jnp.int32, (rows, cols), 1)
    if offset is not None:
        m = m - offset
        m = jnp.where(m < 0, m + rows, m)
    low = m * width
    return jnp.where((i >= low) & (i < low + width), 1.0, 0.0)


def level_of(classes, levels_ref):
    out = jnp.zeros_like(classes)
    for n in range(levels_ref.shape[0]):
        out = jnp.where(classes == n, levels_ref[n], out)
    return out


def prep_body(columns, levels_ref, anchor_ref, wet_ref, class_ref, wet_out, bed_out, weights):
    lane_blocks, rows, _ = wet_out.shape
    size, width = wet_ref.shape[1], wet_ref.shape[2]
    wet = wet_ref[0].astype(F32)
    bed = level_of(class_ref[0].astype(F32), levels_ref)
    across = spread_t(width, lane_blocks * 128, 3)
    down = spread(rows, size, 3)
    for out, cells, parts in ((wet_out, wet, 1), (bed_out, bed, 3)):
        fine = mul_left(down, mul_right(cells, across, parts), parts)
        for q in range(lane_blocks):
            out[q] = fine[:, q * 128 : q * 128 + 128]
    nest = lax.axis_index("nest").astype(jnp.int32)
    row_at = lax.axis_index("row").astype(jnp.int32)
    col_at = lax.axis_index("col").astype(jnp.int32)
    up_nest = jnp.where(row_at == 0, jnp.maximum(nest - 1, 0), nest)
    i = lax.broadcasted_iota(jnp.int32, weights.shape[1:], 0)
    m = lax.broadcasted_iota(jnp.int32, weights.shape[1:], 1)
    has_left = jnp.where(col_at > 0, 1.0, 0.0)
    has_up = jnp.where((row_at > 0) | (nest > 0), 1.0, 0.0)
    own_rows = jnp.where(i >= anchor_ref[nest, 0], 1.0, 0.0)
    up_rows = jnp.where(i < anchor_ref[up_nest, 0], has_up, 0.0)
    own_cols = m >= anchor_ref[nest, 1]
    up_cols = m >= anchor_ref[up_nest, 1]
    shares = (
        jnp.where(own_cols, own_rows, 0.0),
        jnp.where(own_cols, 0.0, own_rows * has_left),
        jnp.where(up_cols, up_rows, 0.0),
        jnp.where(up_cols, 0.0, up_rows * has_left),
    )
    scale = 1.0 / (1.0 + shares[0] + shares[1] + shares[2] + shares[3])
    weights[0] = scale
    for n, share in enumerate(shares):
        weights[n + 1] = share * scale


def split(x, parts):
    out = []
    for n in range(parts):
        piece = x.astype(jnp.bfloat16)
        out.append(piece)
        if n + 1 < parts:
            x = x - piece.astype(F32)
    return out


def mul_left(matrix, x, parts):
    matrix = matrix.astype(jnp.bfloat16)
    return sum(jnp.dot(matrix, piece, preferred_element_type=F32) for piece in split(x, parts))


def mul_right(x, matrix, parts):
    matrix = matrix.astype(jnp.bfloat16)
    return sum(jnp.dot(piece, matrix, preferred_element_type=F32) for piece in split(x, parts))


def mul_left_t(matrix, x, parts):
    matrix = matrix.astype(jnp.bfloat16)
    return sum(
        lax.dot_general(matrix, piece, (((1,), (1,)), ((), ())), preferred_element_type=F32)
        for piece in split(x, parts)
    )


def unpack(dims, me, first_row, messages, ds, field, extra):
    blocks, band, columns, lane_blocks = dims
    body_rows = 3 * lane_blocks * band
    for message, d in zip(messages, ds):
        p = me ^ d
        top = pl.multiple_of(8 + p * band - first_row, 8)
        mixed = message[body_rows : body_rows + 8]
        for k in range(3):
            for q in range(lane_blocks):
                n = k * lane_blocks + q
                field[k, q, pl.ds(top, band)] = message[
                    n * band : n * band + band
                ]
            for g in range(band // 8):
                i = g * 3 + k
                at = pl.multiple_of(top + g * 8, 8)
                field[k, lane_blocks, pl.ds(at, 8)] = pltpu.roll(mixed, 127 - 2 * i, 1)
        extra[p, 0:8] = mixed
        if halo_rows(dims, d):
            extra[p, 8:16] = message[body_rows + 8 : body_rows + 16]


def edge_rows(dims, extra, source, inside):
    blocks, band, columns, lane_blocks = dims
    lane = lax.broadcasted_iota(jnp.int32, (1, 128), 1)
    block = extra[jnp.where(inside, source, 0), 0:8]
    wet_row = from_half_rows(block, 2, lane)
    bed_row = from_half_rows(block, 4, lane)
    return jnp.where(inside, wet_row, 0.0), jnp.where(inside, bed_row, 0.0)


def side_cells(dims, me, extra, wet_side, bed_side):
    columns = dims[2]
    my_col = me % columns
    west = edge_rows(dims, extra, me - 1, my_col > 0)
    east = edge_rows(dims, extra, me + 1, my_col < columns - 1)
    sub = lax.broadcasted_iota(jnp.int32, (128, 128), 0)
    pair = jnp.zeros((128, 128), F32)
    for n, row in ((0, east[0]), (127, west[0]), (64, east[1]), (63, west[1])):
        pair = jnp.where(sub == n, row, pair)
    sides = mul_left_t(spread(wet_side.shape[0], 128, 3), pair, 3)
    wet_side[...] = sides
    bed_side[...] = pltpu.roll(sides, 64, 1)


def slopes(lane_blocks, wet, bed, wet_side, bed_side, open_x, slope_x, rows):
    lane = lax.broadcasted_iota(jnp.int32, (8, 128), 1)
    sides = lane_blocks + 1

    def step(t, _):
        at = pl.ds(pl.multiple_of(t * 8, 8), 8)
        w = [wet[q, at] for q in range(lane_blocks)] + [wet_side[at]]
        z = [bed[q, at] for q in range(lane_blocks)] + [bed_side[at]]
        steps = []
        for q in range(sides):
            w2, z2 = (
                pltpu.roll(jnp.where(lane == 0, x[(q + 1) % sides], x[q]), 127, 1) for x in (w, z)
            )
            half = (0.5 * courant) * (w[q] * w2)
            open_x[q, at] = half
            steps.append(half * (z2 - z[q]))
        for q in range(lane_blocks):
            left = pltpu.roll(jnp.where(lane == 127, steps[q - 1], steps[q]), 1, 1)
            slope_x[q, at] = gravity * (steps[q] + left)
        return 0

    lax.fori_loop(0, rows // 8, step, 0, unroll=2)


def sweep(dims, field, wet, bed, wet_at, open_x, slope_x, open_at, more, made, fine, start, count, unroll):
    lane_blocks = dims[3]
    sides = lane_blocks + 1
    lane = lax.broadcasted_iota(jnp.int32, (8, 128), 1)
    sub = lax.broadcasted_iota(jnp.int32, (8, 128), 0)

    def rates(h, hu, hv):
        root = lax.rsqrt(h)
        inv = root * root
        u = hu * inv
        c = (gravity**0.5) * (h * root)
        p = (0.5 * gravity) * (h * h)
        return hu * u + p, hv * u, jnp.abs(u) + c, inv, c, p

    def cells(group, q):
        at = pl.ds(pl.multiple_of(8 + group * 8, 8), 8)
        h, hu, hv = (field[k, q, at] for k in range(3))
        f2, m, a, inv, c, p = rates(h, hu, hv)
        if q < lane_blocks:
            v = hv * inv
            more[0, q, at] = m
            more[1, q, at] = hv * v + p
            more[2, q, at] = jnp.abs(v) + c
        return h, hu, hv, f2, m, a

    def face(half, near, far):
        bound = half * jnp.maximum(near[6], far[6])
        return [half * (near[3 + k] + far[3 + k]) - bound * (far[k] - near[k]) for k in range(3)]

    def across(t, _):
        group = start + t
        spot = pl.ds(pl.multiple_of(group * 8, 8), 8)
        opened = pl.ds(pl.multiple_of(open_at + group * 8, 8), 8)
        blocks = [cells(group, q) for q in range(sides)]
        faces = []
        for q in range(sides):
            now, nxt = blocks[q], blocks[(q + 1) % sides]
            h, hu, hv, f2, m, a = now
            h2, hu2, hv2 = (
                pltpu.roll(jnp.where(lane == 0, y, x), 127, 1) for x, y in zip(now[:3], nxt[:3])
            )
            f22, m2, a2 = rates(h2, hu2, hv2)[:3]
            faces.append(
                face(open_x[q, opened], (h, hu, hv, hu, f2, m, a), (h2, hu2, hv2, hu2, f22, m2, a2))
            )
        for q in range(lane_blocks):
            right = faces[q]
            left = [
                pltpu.roll(jnp.where(lane == 127, y, x), 1, 1) for x, y in zip(right, faces[q - 1])
            ]
            h, hu, hv = blocks[q][:3]
            made[0, q, spot] = h - (right[0] - left[0])
            made[1, q, spot] = hu - (right[1] - left[1]) - h * slope_x[q, opened]
            made[2, q, spot] = hv - (right[2] - left[2])
        return 0

    def south_face(group, q):
        at = pl.multiple_of(8 + group * 8, 8)
        w_at = pl.multiple_of(wet_at + group * 8, 8)
        sides = []
        for step in range(2):
            rows = pl.ds(at + step, 8)
            h, hu, hv = (field[k, q, rows] for k in range(3))
            m, g3, b = (more[k, q, rows] for k in range(3))
            sides.append((h, hu, hv, hv, m, g3, b))
        half = (0.5 * courant) * (wet[q, pl.ds(w_at, 8)] * wet[q, pl.ds(w_at + 1, 8)])
        slope = half * (bed[q, pl.ds(w_at + 1, 8)] - bed[q, pl.ds(w_at, 8)])
        return face(half, *sides) + [slope]

    def down(t, above):
        group = start + t
        spot = pl.ds(pl.multiple_of(group * 8, 8), 8)
        new = []
        for q in range(lane_blocks):
            below = south_face(group, q)
            up = [
                pltpu.roll(jnp.where(sub == 7, y, x), 1, 0) for x, y in zip(below, above[q])
            ]
            h = field[0, q, pl.ds(pl.multiple_of(8 + group * 8, 8), 8)]
            done = [made[k, q, spot] - (below[k] - up[k]) for k in range(3)]
            done[2] = done[2] - gravity * h * (below[3] + up[3])
            for k in range(3):
                made[k, q, spot] = done[k]
                if fine is not None:
                    fine[0, k, spot, q * 128 : q * 128 + 128] = done[k]
            new.append(below)
        return new

    for q in range(lane_blocks):
        cells(start - 1, q)
        cells(start + count, q)
    if count == 1:
        across(0, 0)
        down(0, [south_face(start - 1, q) for q in range(lane_blocks)])
    else:
        lax.fori_loop(0, count, across, 0, unroll=unroll)
        above = [south_face(start - 1, q) for q in range(lane_blocks)]
        lax.fori_loop(0, count, down, above, unroll=unroll)


def half_body(dims, ds, wet_in, bed_in, *rest):
    blocks, band, columns, lane_blocks = dims
    owners = blocks * columns
    messages = rest[: len(ds)]
    made, open_x, slope_x, field, wet_side, bed_side, more, extra = rest[len(ds) :]
    rows = owners * band // 2
    me = lax.axis_index(("row", "col")).astype(jnp.int32)
    first_row = pl.multiple_of((me * 2 // owners) * rows, 8)
    unpack(dims, me, first_row, messages, ds, field, extra)
    side_cells(dims, me, extra, wet_side, bed_side)
    slopes(lane_blocks, wet_in, bed_in, wet_side, bed_side, open_x, slope_x, 2 * rows)
    for k in range(3):
        for q in range(lane_blocks):
            made[k, q, 0:8] = jnp.zeros((8, 128), F32)
            made[k, q, rows - 8 : rows] = jnp.zeros((8, 128), F32)
    sweep(
        dims, field, wet_in, bed_in, first_row, open_x, slope_x, first_row, more, made, None, 1, rows // 8 - 2, 2
    )


def main_body(dims, ds, anchor_hbm, wet_in, bed_in, half_in, open_x, slope_x, *rest):
    blocks, band, columns, lane_blocks = dims
    owners = blocks * columns
    messages = rest[:owners]
    fine_out, rolled_out = rest[owners : owners + 2]
    field, wet, bed, more, extra, made, anchor_ref, sem_in = rest[owners + 2 :]
    rows = owners * band
    cols = lane_blocks * 128
    me = lax.axis_index(("row", "col")).astype(jnp.int32)
    nest = lax.axis_index("nest").astype(jnp.int32)
    my_row = me // columns
    done_half = me * 2 // owners
    half_rows_at = pl.multiple_of(done_half * (rows // 2), 8)
    corners = pltpu.make_async_copy(anchor_hbm, anchor_ref, sem_in)
    corners.start()

    for k in range(3):
        for q in range(lane_blocks):
            made[k, q, pl.ds(half_rows_at, rows // 2)] = half_in[k, q]
            fine_out[0, k, pl.ds(half_rows_at, rows // 2), q * 128 : q * 128 + 128] = half_in[k, q]
    lane1 = lax.broadcasted_iota(jnp.int32, (1, 128), 1)
    for q in range(lane_blocks):
        wet[q, 8 : 8 + rows] = wet_in[q]
        bed[q, 8 : 8 + rows] = bed_in[q]
    unpack(dims, me, 0, messages, ds, field, extra)

    for source, at, inside, near in (
        (owners - 1, 0, my_row > 0, 8),
        (0, 8 + rows, my_row < blocks - 1, rows),
    ):
        last = from_half_rows(extra[source, 0:8], 0, lane1)
        for k in range(3):
            for q in range(lane_blocks):
                n = k * lane_blocks + q
                row = last if n == 8 else extra[source, 8 + n : 9 + n]
                row = jnp.broadcast_to(row, (8, 128))
                field[k, q, at : at + 8] = jnp.where(inside, row, field[k, q, near : near + 8])
    north = edge_rows(dims, extra, me - columns, my_row > 0)
    south = edge_rows(dims, extra, me + columns, my_row < blocks - 1)
    sub8 = lax.broadcasted_iota(jnp.int32, (8, 128), 0)
    stack = jnp.zeros((8, 128), F32)
    for n, row in enumerate((north[0], north[1], south[0], south[1])):
        stack = jnp.where(sub8 == n, row, stack)
    ends = mul_right(stack, spread_t(128, cols, 3), 3)
    for n, (ref, at) in enumerate(((wet, 0), (bed, 0), (wet, 8 + rows), (bed, 8 + rows))):
        for q in range(lane_blocks):
            ref[q, at : at + 8] = jnp.broadcast_to(ends[n : n + 1, q * 128 : q * 128 + 128], (8, 128))

    groups = rows // 8
    one = done_half * (groups - 1)
    along = (dims, field, wet, bed, 8, open_x, slope_x, 0, more, made, fine_out)
    sweep(*along, one, 1, 1)
    many = (1 - done_half) * (groups // 2 - 1)
    sweep(*along, many, groups // 2 + 1, 5)
    corners.wait()
    coarse_rows = rows // 3
    coarse_cols = cols // 3
    a0 = anchor_ref[nest, 0]
    a1 = anchor_ref[nest, 1]
    gather_cols = spread(cols, coarse_cols, 3, a1)
    for k in range(3):
        total = jnp.concatenate(
            [
                sum(made[k, q, pl.ds(n, coarse_rows, stride=3), :] for n in range(3))
                for q in range(lane_blocks)
            ],
            axis=1,
        )
        mean = mul_right(total, gather_cols, 2) * (1.0 / 9.0)
        rolled_out[k] = pltpu.roll(mean, a0, 0)


def finish_body(coarse, weights, left, diagonal, up, own, out):
    for k in range(3):
        out[k] = (
            coarse[k] * weights[0]
            + own[k] * weights[1]
            + left[k] * weights[2]
            + up[k] * weights[3]
            + diagonal[k] * weights[4]
        )


def in_vmem(x):
    return pltpu.with_memory_space_constraint(x, pltpu.VMEM)


def in_hbm(x):
    return pltpu.with_memory_space_constraint(x, pltpu.HBM)


SMEM = pl.BlockSpec(memory_space=pltpu.SMEM)
VMEM = pl.BlockSpec(memory_space=pltpu.VMEM)
HBM = pl.BlockSpec(memory_space=pltpu.HBM)


def half_call(dims, ds, wet_fine, bed_fine, messages):
    blocks, band, columns, lane_blocks = dims
    owners = blocks * columns
    rows = owners * band // 2
    return pl.pallas_call(
        lambda *refs: half_body(dims, ds, *refs),
        in_specs=[VMEM, VMEM] + [VMEM] * len(ds),
        out_specs=[VMEM] * 3,
        out_shape=[
            pltpu.VMEM((3, lane_blocks, rows, 128), F32),
            pltpu.VMEM((lane_blocks + 1, 2 * rows, 128), F32),
            pltpu.VMEM((lane_blocks, 2 * rows, 128), F32),
        ],
        scratch_shapes=[
            pltpu.VMEM((3, lane_blocks + 1, rows + 16, 128), F32),
            pltpu.VMEM((2 * rows, 128), F32),
            pltpu.VMEM((2 * rows, 128), F32),
            pltpu.VMEM((3, lane_blocks, rows + 16, 128), F32),
            pltpu.VMEM((owners, 16, 128), F32),
        ],
        name="half", compiler_params=pltpu.CompilerParams(vmem_limit_bytes=12 << 20),
    )(wet_fine, bed_fine, *messages)


def main_call(dims, ds, anchor, wet_fine, bed_fine, half, open_x, slope_x, messages):
    blocks, band, columns, lane_blocks = dims
    owners = blocks * columns
    rows = owners * band
    cols = lane_blocks * 128
    return pl.pallas_call(
        lambda *refs: main_body(dims, ds, *refs),
        in_specs=[HBM] + [VMEM] * (5 + owners),
        out_specs=[VMEM, VMEM],
        out_shape=[
            pltpu.VMEM((1, 3, rows, cols), F32),
            pltpu.VMEM((3, rows // 3, cols // 3), F32),
        ],
        scratch_shapes=[
            pltpu.VMEM((3, lane_blocks + 1, rows + 16, 128), F32),
            pltpu.VMEM((lane_blocks, rows + 16, 128), F32),
            pltpu.VMEM((lane_blocks, rows + 16, 128), F32),
            pltpu.VMEM((3, lane_blocks, rows + 16, 128), F32),
            pltpu.VMEM((owners, 16, 128), F32),
            pltpu.VMEM((3, lane_blocks, rows, 128), F32),
            pltpu.SMEM((2, 2), jnp.int32),
            pltpu.SemaphoreType.DMA,
        ],
        name="main", compiler_params=pltpu.CompilerParams(vmem_limit_bytes=20 << 20),
    )(anchor, wet_fine, bed_fine, half, open_x, slope_x, *messages)


def local_packed(strips, anchor, wet_mask, bathy_index, bed_levels, coarse):
    blocks, band, full_cols = strips.shape[2], strips.shape[4], strips.shape[5]
    columns = lax.axis_size("col")
    owners = blocks * columns
    cols = full_cols // columns
    lane_blocks = cols // 128
    rows = owners * band
    dims = (blocks, band, columns, lane_blocks)
    half_owners = owners // 2

    def rank(d):
        r, c = d // columns, d % columns
        return (d >= half_owners, c * 2 < columns, r, c)

    wanted = sorted(range(1, owners), key=rank)
    opening = [d for d in wanted if d < columns and d * 2 >= columns]
    rest = [d for d in range(half_owners) if d not in opening]
    messages = {}
    after = []
    for ds in (opening, rest, list(range(half_owners, owners))):
        count = len({d // columns for d in ds})
        made = pl.pallas_call(
            lambda *refs, ds=ds, after=len(after): pack_body(dims, ds, after, *refs),
            in_specs=[HBM] * 4 + [VMEM] * len(after),
            out_specs=[VMEM] * len(ds),
            out_shape=[pltpu.VMEM((message_rows(dims, d), 128), F32) for d in ds],
            scratch_shapes=[
                pltpu.VMEM((count, 3, band, full_cols), F32),
                pltpu.VMEM((count, 3, 8, full_cols), F32),
                pltpu.VMEM(wet_mask.shape, jnp.int32),
                pltpu.VMEM(bathy_index.shape, jnp.int32),
                pltpu.SMEM(bed_levels.shape, F32),
                pltpu.SemaphoreType.DMA((2, count)),
                pltpu.SemaphoreType.DMA((3,)),
            ],
            name="pack",
            compiler_params=pltpu.CompilerParams(vmem_limit_bytes=10 << 20),
        )(
            in_hbm(strips),
            in_hbm(wet_mask),
            in_hbm(bathy_index),
            in_hbm(bed_levels),
            *after,
        )
        messages.update(zip(ds, (in_vmem(x) for x in made)))
        after = [messages[ds[0]]]

    arrived = {
        d: lax.ppermute(messages[d], ("row", "col"), [(i, i ^ d) for i in range(owners)])
        for d in wanted
    }
    arrived[0] = messages[0]
    arrived = {d: in_vmem(x) if d else x for d, x in arrived.items()}

    coarse_rows = rows // 3
    coarse_cols = cols // 3
    wet_fine, bed_fine, weights = pl.pallas_call(
        lambda *refs: prep_body(columns, *refs),
        in_specs=[SMEM, SMEM, VMEM, VMEM],
        out_specs=[VMEM] * 3,
        out_shape=[pltpu.VMEM((lane_blocks, rows, 128), F32)] * 2
        + [pltpu.VMEM((5, coarse_rows, coarse_cols), F32)],
        name="prep", compiler_params=pltpu.CompilerParams(vmem_limit_bytes=12 << 20),
    )(bed_levels, anchor, wet_mask, bathy_index)

    early = [0] + wanted[: half_owners - 1]
    order = [0] + wanted
    wet_fine, bed_fine, weights = in_vmem(wet_fine), in_vmem(bed_fine), in_vmem(weights)
    half, open_x, slope_x = half_call(dims, early, wet_fine, bed_fine, [arrived[d] for d in early])
    half, open_x, slope_x = in_vmem(half), in_vmem(open_x), in_vmem(slope_x)
    fine, rolled = main_call(
        dims,
        order,
        in_hbm(anchor),
        wet_fine,
        bed_fine,
        half,
        open_x,
        slope_x,
        [arrived[d] for d in order],
    )
    rolled = in_vmem(rolled)

    lines = lax.axis_size("nest") * lax.axis_size("row")
    rights = [(c, c + 1) for c in range(columns - 1)]
    downs = [(l, l + 1) for l in range(lines - 1)]
    both = [(l * columns + c, l2 * columns + c2) for l, l2 in downs for c, c2 in rights]
    diagonal = lax.ppermute(rolled, ("nest", "row", "col"), both)
    from_left = lax.ppermute(rolled, "col", rights)
    from_up = lax.ppermute(rolled, ("nest", "row"), downs)

    coarse_next = pl.pallas_call(
        finish_body,
        in_specs=[VMEM] * 6,
        out_specs=VMEM,
        out_shape=jax.ShapeDtypeStruct(coarse.shape, F32),
        name="finish", compiler_params=pltpu.CompilerParams(vmem_limit_bytes=4 << 20),
    )(
        in_vmem(coarse),
        weights,
        in_vmem(from_left),
        in_vmem(diagonal),
        in_vmem(from_up),
        rolled,
    )
    return (fine, coarse_next)


def local(strips, anchor, wet_mask, bathy_index, bed_levels, coarse):
    columns = lax.axis_size("col")
    owners = strips.shape[2] * columns
    cols = strips.shape[5] // columns
    band = strips.shape[4]
    fits = (
        owners & (owners - 1) == 0
        and 2 <= owners <= 16
        and strips.shape[2] == lax.axis_size("row")
        and band == 24
        and cols == 384
        and owners * band == 384
        and wet_mask.shape[1:] == (128, 128)
    )
    run = local_packed if fits else local_general
    return run(strips, anchor, wet_mask, bathy_index, bed_levels, coarse)


def solution(mesh):
    return jax.shard_map(
        local,
        mesh=mesh,
        in_specs=(
            P("nest", None, None, ("row", "col"), None, None),
            P(),
            P("nest", "row", "col"),
            P("nest", "row", "col"),
            P(),
            P(None, ("nest", "row"), "col"),
        ),
        out_specs=(P("nest", None, "row", "col"), P(None, ("nest", "row"), "col")),
        check_vma=False,
    )
```

```python
import jax
import jax.numpy as jnp
from jax import lax
from jax.experimental import pallas as pl
from jax.experimental.pallas import tpu as pltpu
from jax.sharding import PartitionSpec as P


gravity = 1.0
courant = 0.2
F32 = jnp.float32


def padded_2(cells, sides, width):
    for axis, dim in sides:
        count = lax.axis_size(axis)
        ends = count - 1
        head = lax.slice_in_dim(cells, 0, width, axis=dim)
        tail = lax.slice_in_dim(cells, cells.shape[dim] - width, cells.shape[dim], axis=dim)
        cells = jnp.concatenate(
            [
                lax.ppermute(tail, axis, [(i, (i + 1) % count) for i in range(ends)]),
                cells,
                lax.ppermute(head, axis, [((i + 1) % count, i) for i in range(ends)]),
            ],
            axis=dim,
        )
    return cells


def passed_along(block, axis, distance):
    devices = range(lax.axis_size(axis))
    route = [(i - distance, i) for i in devices if i - distance in devices]
    return lax.ppermute(block, axis, route)


def advance(padded, bed_pad, wet_pad):
    depth_now = padded[0]
    flow_u = padded[1]
    flow_v = padded[2]
    depth_safe = jnp.where(wet_pad > 0.5, depth_now, 1.0)
    speed_u = flow_u / depth_safe
    speed_v = flow_v / depth_safe
    celerity = jnp.sqrt(gravity * depth_safe)
    pressure = 0.5 * gravity * depth_safe * depth_safe
    fluxes_x = (flow_u, flow_u * speed_u + pressure, flow_v * speed_u)
    fluxes_y = (flow_v, flow_u * speed_v, flow_v * speed_v + pressure)
    reach_x = jnp.abs(speed_u) + celerity
    reach_y = jnp.abs(speed_v) + celerity
    open_x = wet_pad[1:-1, :-1] * wet_pad[1:-1, 1:]
    open_y = wet_pad[:-1, 1:-1] * wet_pad[1:, 1:-1]
    bound_x = jnp.maximum(reach_x[1:-1, :-1], reach_x[1:-1, 1:])
    bound_y = jnp.maximum(reach_y[:-1, 1:-1], reach_y[1:, 1:-1])
    slope_x = (bed_pad[1:-1, 1:] - bed_pad[1:-1, :-1]) * open_x
    slope_y = (bed_pad[1:, 1:-1] - bed_pad[:-1, 1:-1]) * open_y
    centre = depth_now[1:-1, 1:-1]
    sources = (
        None,
        -0.5 * gravity * centre * (slope_x[:, 1:] + slope_x[:, :-1]),
        -0.5 * gravity * centre * (slope_y[1:] + slope_y[:-1]),
    )
    results = []
    for plane in range(3):
        state = padded[plane]
        flux_col = fluxes_x[plane]
        flux_row = fluxes_y[plane]
        face_x = (
            0.5 * (flux_col[1:-1, :-1] + flux_col[1:-1, 1:])
            - 0.5 * bound_x * (state[1:-1, 1:] - state[1:-1, :-1])
        ) * open_x
        face_y = (
            0.5 * (flux_row[:-1, 1:-1] + flux_row[1:, 1:-1])
            - 0.5 * bound_y * (state[1:, 1:-1] - state[:-1, 1:-1])
        ) * open_y
        value = (
            state[1:-1, 1:-1]
            - courant * (face_x[:, 1:] - face_x[:, :-1])
            - courant * (face_y[1:] - face_y[:-1])
        )
        if plane > 0:
            value = value + courant * sources[plane]
        results.append(value)
    return jnp.stack(results)


def expand(cells):
    return jnp.repeat(jnp.repeat(cells, 3, axis=-2), 3, axis=-1)


def lookup(classes, levels):
    ladder = jnp.arange(levels.shape[0], dtype=jnp.int32)
    matches = classes[None] == ladder[:, None, None]
    return jnp.sum(jnp.where(matches, levels[:, None, None], 0.0), axis=0)


def restrict(updated):
    planes, row_count, col_count = updated.shape
    return updated.reshape(planes, row_count // 3, 3, col_count // 3, 3).sum(axis=(2, 4)) / 9.0


def local_general(strips, anchor, wet_mask, bathy_index, bed_levels, coarse):
    tile_blocks = strips.shape[2]
    band_rows = strips.shape[4]
    full_cols = strips.shape[5]
    columns = lax.axis_size("col")
    tile_cols = full_cols // columns
    layered = (
        strips[0, :, :, 0]
        .reshape(3, tile_blocks, band_rows, columns, tile_cols)
        .transpose(0, 1, 3, 2, 4)
    )
    flattened = layered.reshape(3, tile_blocks * columns, band_rows, tile_cols)
    arrived = lax.all_to_all(flattened, ("row", "col"), split_axis=1, concat_axis=1, tiled=True)
    fields = arrived.reshape(3, tile_blocks * columns * band_rows, tile_cols)
    bed_fine = expand(lookup(bathy_index[0], bed_levels))
    wetness = expand(wet_mask[0].astype(F32))
    stacked = jnp.concatenate([fields, bed_fine[None], wetness[None]], axis=0)
    padded_all = padded_2(stacked, (("row", 1), ("col", 2)), 1)
    updated = advance(padded_all[:3], padded_all[3], padded_all[4])
    restricted = restrict(updated)
    coarse_rows = restricted.shape[1]
    coarse_cols = restricted.shape[2]
    contribution = jnp.concatenate(
        [restricted, jnp.ones((1, coarse_rows, coarse_cols), F32)], axis=0
    )
    nest_index = lax.axis_index("nest")
    corner = lax.dynamic_index_in_dim(anchor, nest_index, 0, keepdims=False)
    canvas = lax.dynamic_update_slice(
        jnp.zeros((4, 2 * coarse_rows, 2 * coarse_cols), F32),
        contribution,
        (jnp.int32(0), corner[0], corner[1]),
    )
    spilled = passed_along(canvas[:, :, coarse_cols:], "col", 1)
    merged = canvas[:, :, :coarse_cols] + spilled
    lowered = passed_along(merged[:, coarse_rows:], ("nest", "row"), 1)
    received_sum = merged[:, :coarse_rows] + lowered
    coarse_next = (coarse + received_sum[:3]) / (1.0 + received_sum[3])
    return (updated[None], coarse_next)


def halo_rows(dims, d):
    return d // dims[2] != dims[0] - 1


def message_rows(dims, d):
    blocks, band, columns, lane_blocks = dims
    return 3 * lane_blocks * band + (16 if halo_rows(dims, d) else 8)


def half_rows(row):
    return pltpu.roll(row, 64, 1), row


def from_half_rows(block, at, lane):
    upper = block[at : at + 1]
    return jnp.where(lane < 64, pltpu.roll(upper, 64, 1), block[at + 1 : at + 2])


def pack_body(dims, ds, after, strips_hbm, wet_hbm, class_hbm, levels_hbm, *rest):
    blocks, band, columns, lane_blocks = dims
    rest = rest[after:]
    outs = rest[: len(ds)]
    strips, tiles, wet_ref, class_ref, levels_ref, sems, small = rest[len(ds) :]
    tile_cols = lane_blocks * 128
    me = lax.axis_index(("row", "col")).astype(jnp.int32)
    my_row = me // columns
    my_col = me % columns
    loads = [
        pltpu.make_async_copy(wet_hbm, wet_ref, small.at[0]),
        pltpu.make_async_copy(class_hbm, class_ref, small.at[1]),
        pltpu.make_async_copy(levels_hbm, levels_ref, small.at[2]),
    ]
    for c in loads:
        c.start()
    first = me == 0
    groups = sorted({d // columns for d in ds})
    copies = []
    for n, r in enumerate(groups):
        j = my_row ^ r
        jj = jnp.clip(jnp.where(first, j + 1, j - 1), 0, blocks - 1)
        edge = pl.ds(pl.multiple_of(jnp.where(first, 0, band - 8), 8), 8)
        copies.append(
            (
                pltpu.make_async_copy(strips_hbm.at[0, :, j, 0], strips.at[n], sems.at[0, n]),
                pltpu.make_async_copy(strips_hbm.at[0, :, jj, 0, edge], tiles.at[n], sems.at[1, n]),
            )
        )
    for pair in copies:
        for c in pair:
            c.start()
    lane = lax.broadcasted_iota(jnp.int32, (8, 128), 1)
    sub = lax.broadcasted_iota(jnp.int32, (8, 128), 0)
    size = wet_ref.shape[1]
    diag = lax.broadcasted_iota(jnp.int32, (size, 128), 0) == lax.broadcasted_iota(
        jnp.int32, (size, 128), 1
    )
    for c in loads:
        c.wait()
    edges = []
    for ref in (wet_ref, class_ref):
        cells = ref[0].astype(F32)
        north = cells[0:1]
        south = cells[size - 1 : size]
        west = jnp.sum(jnp.where(diag, cells[:, 0:1], 0.0), axis=0, keepdims=True)
        east = jnp.sum(jnp.where(diag, cells[:, 127:128], 0.0), axis=0, keepdims=True)
        four = (north, south, west, east)
        if ref is class_ref:
            four = tuple(level_of(row, levels_ref) for row in four)
        edges.append(four)
    body_rows = 3 * lane_blocks * band
    waiting = list(groups)
    mixes = []
    for out, d in zip(outs, ds):
        n = groups.index(d // columns)
        if groups[n] in waiting:
            copies[n][0].wait()
            waiting.remove(groups[n])
        to = me ^ d
        j = to // columns
        c = to % columns
        base = pl.multiple_of(c * tile_cols, 128)
        for k in range(3):
            for q in range(lane_blocks):
                at = (k * lane_blocks + q) * band
                out[at : at + band] = strips[n, k, :, pl.ds(pl.multiple_of(base + q * 128, 128), 128)]
        west_at = pl.multiple_of(jnp.maximum(base - 128, 0), 128)
        east_at = pl.multiple_of(jnp.where(c == columns - 1, base, base + tile_cols), 128)
        mixed = jnp.zeros((8, 128), F32)
        for g in range(band // 8):
            for k in range(3):
                i = g * 3 + k
                west = strips[n, k, g * 8 : g * 8 + 8, pl.ds(west_at, 128)]
                east = strips[n, k, g * 8 : g * 8 + 8, pl.ds(east_at, 128)]
                both = pltpu.roll(jnp.where(lane == 127, west, east), 2 * i + 1, 1)
                mixed = jnp.where((lane == 2 * i) | (lane == 2 * i + 1), both, mixed)
        mixes.append(mixed)
    for pair in copies:
        pair[1].wait()
    for out, d, mixed in zip(outs, ds, mixes):
        n = groups.index(d // columns)
        to = me ^ d
        j = to // columns
        c = to % columns
        base = pl.multiple_of(c * tile_cols, 128)
        tucked = [jnp.zeros((1, 128), F32)]
        if halo_rows(dims, d):
            rows = []
            for k in range(3):
                for q in range(lane_blocks):
                    spot = pl.ds(pl.multiple_of(base + q * 128, 128), 128)
                    tile = tiles[n, k, :, spot]
                    rows.append(jnp.where(first, tile[0:1], tile[7:8]))
            halo = jnp.zeros((8, 128), F32)
            for i in range(8):
                halo = jnp.where(sub == i, rows[i], halo)
            out[body_rows + 8 : body_rows + 16] = halo
            tucked = [rows[8]]
        for north, south, west, east in edges:
            row = jnp.where(
                c == my_col,
                jnp.where(j > my_row, south, north),
                jnp.where(c > my_col, east, west),
            )
            tucked.append(row)
        for t, row in enumerate(tucked):
            low, high = half_rows(row)
            mixed = jnp.where((sub == 2 * t) & (lane >= 64), low, mixed)
            mixed = jnp.where((sub == 2 * t + 1) & (lane >= 64), high, mixed)
        out[body_rows : body_rows + 8] = mixed


def spread(rows, cols, width, offset=None):
    i = lax.broadcasted_iota(jnp.int32, (rows, cols), 0)
    m = lax.broadcasted_iota(jnp.int32, (rows, cols), 1)
    if offset is not None:
        m = m - offset
        m = jnp.where(m < 0, m + cols, m)
    low = m * width
    return jnp.where((i >= low) & (i < low + width), 1.0, 0.0)


def spread_t(rows, cols, width, offset=None):
    m = lax.broadcasted_iota(jnp.int32, (rows, cols), 0)
    i = lax.broadcasted_iota(jnp.int32, (rows, cols), 1)
    if offset is not None:
        m = m - offset
        m = jnp.where(m < 0, m + rows, m)
    low = m * width
    return jnp.where((i >= low) & (i < low + width), 1.0, 0.0)


def level_of(classes, levels_ref):
    out = jnp.zeros_like(classes)
    for n in range(levels_ref.shape[0]):
        out = jnp.where(classes == n, levels_ref[n], out)
    return out


def prep_body(columns, levels_ref, anchor_ref, wet_ref, class_ref, wet_out, bed_out, weights):
    lane_blocks, rows, _ = wet_out.shape
    size, width = wet_ref.shape[1], wet_ref.shape[2]
    wet = wet_ref[0].astype(F32)
    bed = level_of(class_ref[0].astype(F32), levels_ref)
    across = spread_t(width, lane_blocks * 128, 3)
    down = spread(rows, size, 3)
    for out, cells, parts in ((wet_out, wet, 1), (bed_out, bed, 3)):
        fine = mul_left(down, mul_right(cells, across, parts), parts)
        for q in range(lane_blocks):
            out[q] = fine[:, q * 128 : q * 128 + 128]
    nest = lax.axis_index("nest").astype(jnp.int32)
    row_at = lax.axis_index("row").astype(jnp.int32)
    col_at = lax.axis_index("col").astype(jnp.int32)
    up_nest = jnp.where(row_at == 0, jnp.maximum(nest - 1, 0), nest)
    i = lax.broadcasted_iota(jnp.int32, weights.shape[1:], 0)
    m = lax.broadcasted_iota(jnp.int32, weights.shape[1:], 1)
    has_left = jnp.where(col_at > 0, 1.0, 0.0)
    has_up = jnp.where((row_at > 0) | (nest > 0), 1.0, 0.0)
    own_rows = jnp.where(i >= anchor_ref[nest, 0], 1.0, 0.0)
    up_rows = jnp.where(i < anchor_ref[up_nest, 0], has_up, 0.0)
    own_cols = m >= anchor_ref[nest, 1]
    up_cols = m >= anchor_ref[up_nest, 1]
    shares = (
        jnp.where(own_cols, own_rows, 0.0),
        jnp.where(own_cols, 0.0, own_rows * has_left),
        jnp.where(up_cols, up_rows, 0.0),
        jnp.where(up_cols, 0.0, up_rows * has_left),
    )
    scale = 1.0 / (1.0 + shares[0] + shares[1] + shares[2] + shares[3])
    weights[0] = scale
    for n, share in enumerate(shares):
        weights[n + 1] = share * scale


def split(x, parts):
    out = []
    for n in range(parts):
        piece = x.astype(jnp.bfloat16)
        out.append(piece)
        if n + 1 < parts:
            x = x - piece.astype(F32)
    return out


def mul_left(matrix, x, parts):
    matrix = matrix.astype(jnp.bfloat16)
    return sum(jnp.dot(matrix, piece, preferred_element_type=F32) for piece in split(x, parts))


def mul_right(x, matrix, parts):
    matrix = matrix.astype(jnp.bfloat16)
    return sum(jnp.dot(piece, matrix, preferred_element_type=F32) for piece in split(x, parts))


def mul_left_t(matrix, x, parts):
    matrix = matrix.astype(jnp.bfloat16)
    return sum(
        lax.dot_general(matrix, piece, (((1,), (1,)), ((), ())), preferred_element_type=F32)
        for piece in split(x, parts)
    )


def unpack(dims, me, first_row, messages, ds, field, extra):
    blocks, band, columns, lane_blocks = dims
    body_rows = 3 * lane_blocks * band
    for message, d in zip(messages, ds):
        p = me ^ d
        top = pl.multiple_of(8 + p * band - first_row, 8)
        mixed = message[body_rows : body_rows + 8]
        for k in range(3):
            for q in range(lane_blocks):
                n = k * lane_blocks + q
                field[k, q, pl.ds(top, band)] = message[
                    n * band : n * band + band
                ]
            for g in range(band // 8):
                i = g * 3 + k
                at = pl.multiple_of(top + g * 8, 8)
                field[k, lane_blocks, pl.ds(at, 8)] = pltpu.roll(mixed, 127 - 2 * i, 1)
        extra[p, 0:8] = mixed
        if halo_rows(dims, d):
            extra[p, 8:16] = message[body_rows + 8 : body_rows + 16]


def edge_rows(dims, extra, source, inside):
    blocks, band, columns, lane_blocks = dims
    lane = lax.broadcasted_iota(jnp.int32, (1, 128), 1)
    block = extra[jnp.where(inside, source, 0), 0:8]
    wet_row = from_half_rows(block, 2, lane)
    bed_row = from_half_rows(block, 4, lane)
    return jnp.where(inside, wet_row, 0.0), jnp.where(inside, bed_row, 0.0)


def side_cells(dims, me, extra, wet_side, bed_side):
    columns = dims[2]
    my_col = me % columns
    west = edge_rows(dims, extra, me - 1, my_col > 0)
    east = edge_rows(dims, extra, me + 1, my_col < columns - 1)
    sub = lax.broadcasted_iota(jnp.int32, (128, 128), 0)
    pair = jnp.zeros((128, 128), F32)
    for n, row in ((0, east[0]), (127, west[0]), (64, east[1]), (63, west[1])):
        pair = jnp.where(sub == n, row, pair)
    sides = mul_left_t(spread(wet_side.shape[0], 128, 3), pair, 3)
    wet_side[...] = sides
    bed_side[...] = pltpu.roll(sides, 64, 1)


def slopes(lane_blocks, wet, bed, wet_side, bed_side, open_x, slope_x, rows):
    lane = lax.broadcasted_iota(jnp.int32, (8, 128), 1)
    sides = lane_blocks + 1

    def step(t, _):
        at = pl.ds(pl.multiple_of(t * 8, 8), 8)
        w = [wet[q, at] for q in range(lane_blocks)] + [wet_side[at]]
        z = [bed[q, at] for q in range(lane_blocks)] + [bed_side[at]]
        steps = []
        for q in range(sides):
            w2, z2 = (
                pltpu.roll(jnp.where(lane == 0, x[(q + 1) % sides], x[q]), 127, 1) for x in (w, z)
            )
            half = (0.5 * courant) * (w[q] * w2)
            open_x[q, at] = half
            steps.append(half * (z2 - z[q]))
        for q in range(lane_blocks):
            left = pltpu.roll(jnp.where(lane == 127, steps[q - 1], steps[q]), 1, 1)
            slope_x[q, at] = gravity * (steps[q] + left)
        return 0

    lax.fori_loop(0, rows // 8, step, 0, unroll=2)


def sweep(dims, field, wet, bed, wet_at, open_x, slope_x, open_at, more, made, fine, start, count, unroll):
    lane_blocks = dims[3]
    sides = lane_blocks + 1
    lane = lax.broadcasted_iota(jnp.int32, (8, 128), 1)
    sub = lax.broadcasted_iota(jnp.int32, (8, 128), 0)

    def rates(h, hu, hv):
        root = lax.rsqrt(h)
        inv = root * root
        u = hu * inv
        c = (gravity**0.5) * (h * root)
        p = (0.5 * gravity) * (h * h)
        return hu * u + p, hv * u, jnp.abs(u) + c, inv, c, p

    def cells(group, q):
        at = pl.ds(pl.multiple_of(8 + group * 8, 8), 8)
        h, hu, hv = (field[k, q, at] for k in range(3))
        f2, m, a, inv, c, p = rates(h, hu, hv)
        if q < lane_blocks:
            v = hv * inv
            more[0, q, at] = m
            more[1, q, at] = hv * v + p
            more[2, q, at] = jnp.abs(v) + c
        return h, hu, hv, f2, m, a

    def face(half, near, far):
        bound = half * jnp.maximum(near[6], far[6])
        return [half * (near[3 + k] + far[3 + k]) - bound * (far[k] - near[k]) for k in range(3)]

    def across(t, _):
        group = start + t
        spot = pl.ds(pl.multiple_of(group * 8, 8), 8)
        opened = pl.ds(pl.multiple_of(open_at + group * 8, 8), 8)
        blocks = [cells(group, q) for q in range(sides)]
        faces = []
        for q in range(sides):
            now, nxt = blocks[q], blocks[(q + 1) % sides]
            h, hu, hv, f2, m, a = now
            h2, hu2, hv2 = (
                pltpu.roll(jnp.where(lane == 0, y, x), 127, 1) for x, y in zip(now[:3], nxt[:3])
            )
            f22, m2, a2 = rates(h2, hu2, hv2)[:3]
            faces.append(
                face(open_x[q, opened], (h, hu, hv, hu, f2, m, a), (h2, hu2, hv2, hu2, f22, m2, a2))
            )
        for q in range(lane_blocks):
            right = faces[q]
            left = [
                pltpu.roll(jnp.where(lane == 127, y, x), 1, 1) for x, y in zip(right, faces[q - 1])
            ]
            h, hu, hv = blocks[q][:3]
            made[0, q, spot] = h - (right[0] - left[0])
            made[1, q, spot] = hu - (right[1] - left[1]) - h * slope_x[q, opened]
            made[2, q, spot] = hv - (right[2] - left[2])
        return 0

    def south_face(group, q):
        at = pl.multiple_of(8 + group * 8, 8)
        w_at = pl.multiple_of(wet_at + group * 8, 8)
        sides = []
        for step in range(2):
            rows = pl.ds(at + step, 8)
            h, hu, hv = (field[k, q, rows] for k in range(3))
            m, g3, b = (more[k, q, rows] for k in range(3))
            sides.append((h, hu, hv, hv, m, g3, b))
        half = (0.5 * courant) * (wet[q, pl.ds(w_at, 8)] * wet[q, pl.ds(w_at + 1, 8)])
        slope = half * (bed[q, pl.ds(w_at + 1, 8)] - bed[q, pl.ds(w_at, 8)])
        return face(half, *sides) + [slope]

    def down(t, above):
        group = start + t
        spot = pl.ds(pl.multiple_of(group * 8, 8), 8)
        new = []
        for q in range(lane_blocks):
            below = south_face(group, q)
            up = [
                pltpu.roll(jnp.where(sub == 7, y, x), 1, 0) for x, y in zip(below, above[q])
            ]
            h = field[0, q, pl.ds(pl.multiple_of(8 + group * 8, 8), 8)]
            done = [made[k, q, spot] - (below[k] - up[k]) for k in range(3)]
            done[2] = done[2] - gravity * h * (below[3] + up[3])
            for k in range(3):
                made[k, q, spot] = done[k]
                if fine is not None:
                    fine[0, k, spot, q * 128 : q * 128 + 128] = done[k]
            new.append(below)
        return new

    for q in range(lane_blocks):
        cells(start - 1, q)
        cells(start + count, q)
    if count == 1:
        across(0, 0)
        down(0, [south_face(start - 1, q) for q in range(lane_blocks)])
    else:
        lax.fori_loop(0, count, across, 0, unroll=unroll)
        above = [south_face(start - 1, q) for q in range(lane_blocks)]
        lax.fori_loop(0, count, down, above, unroll=unroll)


def half_body(dims, ds, wet_in, bed_in, *rest):
    blocks, band, columns, lane_blocks = dims
    owners = blocks * columns
    messages = rest[: len(ds)]
    made, open_x, slope_x, field, wet_side, bed_side, more, extra = rest[len(ds) :]
    rows = owners * band // 2
    me = lax.axis_index(("row", "col")).astype(jnp.int32)
    first_row = pl.multiple_of((me * 2 // owners) * rows, 8)
    unpack(dims, me, first_row, messages, ds, field, extra)
    side_cells(dims, me, extra, wet_side, bed_side)
    slopes(lane_blocks, wet_in, bed_in, wet_side, bed_side, open_x, slope_x, 2 * rows)
    for k in range(3):
        for q in range(lane_blocks):
            made[k, q, 0:8] = jnp.zeros((8, 128), F32)
            made[k, q, rows - 8 : rows] = jnp.zeros((8, 128), F32)
    sweep(
        dims, field, wet_in, bed_in, first_row, open_x, slope_x, first_row, more, made, None, 1, rows // 8 - 2, 2
    )


def main_body(dims, ds, anchor_hbm, wet_in, bed_in, half_in, open_x, slope_x, *rest):
    blocks, band, columns, lane_blocks = dims
    owners = blocks * columns
    messages = rest[:owners]
    fine_out, rolled_out = rest[owners : owners + 2]
    field, wet, bed, more, extra, made, anchor_ref, sem_in = rest[owners + 2 :]
    rows = owners * band
    cols = lane_blocks * 128
    me = lax.axis_index(("row", "col")).astype(jnp.int32)
    nest = lax.axis_index("nest").astype(jnp.int32)
    my_row = me // columns
    done_half = me * 2 // owners
    half_rows_at = pl.multiple_of(done_half * (rows // 2), 8)
    corners = pltpu.make_async_copy(anchor_hbm, anchor_ref, sem_in)
    corners.start()

    for k in range(3):
        for q in range(lane_blocks):
            made[k, q, pl.ds(half_rows_at, rows // 2)] = half_in[k, q]
            fine_out[0, k, pl.ds(half_rows_at, rows // 2), q * 128 : q * 128 + 128] = half_in[k, q]
    lane1 = lax.broadcasted_iota(jnp.int32, (1, 128), 1)
    for q in range(lane_blocks):
        for top, count in (
            ((1 - done_half) * (rows // 2 - 16), rows // 2 + 16),
            (done_half * (rows - 16), 16),
        ):
            at = pl.multiple_of(top, 8)
            to = pl.ds(pl.multiple_of(at + 8, 8), count)
            wet[q, to] = wet_in[q, pl.ds(at, count)]
            bed[q, to] = bed_in[q, pl.ds(at, count)]
    unpack(dims, me, 0, messages, ds, field, extra)

    for source, at, inside, near in (
        (owners - 1, 0, my_row > 0, 8),
        (0, 8 + rows, my_row < blocks - 1, rows),
    ):
        last = from_half_rows(extra[source, 0:8], 0, lane1)
        for k in range(3):
            for q in range(lane_blocks):
                n = k * lane_blocks + q
                row = last if n == 8 else extra[source, 8 + n : 9 + n]
                row = jnp.broadcast_to(row, (8, 128))
                field[k, q, at : at + 8] = jnp.where(inside, row, field[k, q, near : near + 8])
    north = edge_rows(dims, extra, me - columns, my_row > 0)
    south = edge_rows(dims, extra, me + columns, my_row < blocks - 1)
    sub8 = lax.broadcasted_iota(jnp.int32, (8, 128), 0)
    stack = jnp.zeros((8, 128), F32)
    for n, row in enumerate((north[0], north[1], south[0], south[1])):
        stack = jnp.where(sub8 == n, row, stack)
    ends = mul_right(stack, spread_t(128, cols, 3), 3)
    for n, (ref, at) in enumerate(((wet, 0), (bed, 0), (wet, 8 + rows), (bed, 8 + rows))):
        for q in range(lane_blocks):
            ref[q, at : at + 8] = jnp.broadcast_to(ends[n : n + 1, q * 128 : q * 128 + 128], (8, 128))

    groups = rows // 8
    one = done_half * (groups - 1)
    along = (dims, field, wet, bed, 8, open_x, slope_x, 0, more, made, fine_out)
    sweep(*along, one, 1, 1)
    many = (1 - done_half) * (groups // 2 - 1)
    sweep(*along, many, groups // 2 + 1, 5)
    corners.wait()
    coarse_rows = rows // 3
    coarse_cols = cols // 3
    a0 = anchor_ref[nest, 0]
    a1 = anchor_ref[nest, 1]
    gather_cols = spread(cols, coarse_cols, 3, a1)
    totals = [
        jnp.concatenate(
            [
                sum(made[k, q, pl.ds(n, coarse_rows, stride=3), :] for n in range(3))
                for q in range(lane_blocks)
            ],
            axis=1,
        )
        for k in range(3)
    ]
    means = mul_right(jnp.concatenate(totals, axis=0), gather_cols, 2) * (1.0 / 9.0)
    for k in range(3):
        rolled_out[k] = pltpu.roll(means[k * coarse_rows : (k + 1) * coarse_rows], a0, 0)


def finish_body(coarse, weights, left, up, diagonal, own, out):
    for k in range(3):
        out[k] = (
            coarse[k] * weights[0]
            + own[k] * weights[1]
            + left[k] * weights[2]
            + up[k] * weights[3]
            + diagonal[k] * weights[4]
        )


def in_vmem(x):
    return pltpu.with_memory_space_constraint(x, pltpu.VMEM)


def in_hbm(x):
    return pltpu.with_memory_space_constraint(x, pltpu.HBM)


SMEM = pl.BlockSpec(memory_space=pltpu.SMEM)
VMEM = pl.BlockSpec(memory_space=pltpu.VMEM)
HBM = pl.BlockSpec(memory_space=pltpu.HBM)


def half_call(dims, ds, wet_fine, bed_fine, messages):
    blocks, band, columns, lane_blocks = dims
    owners = blocks * columns
    rows = owners * band // 2
    return pl.pallas_call(
        lambda *refs: half_body(dims, ds, *refs),
        in_specs=[VMEM, VMEM] + [VMEM] * len(ds),
        out_specs=[VMEM] * 3,
        out_shape=[
            pltpu.VMEM((3, lane_blocks, rows, 128), F32),
            pltpu.VMEM((lane_blocks + 1, 2 * rows, 128), F32),
            pltpu.VMEM((lane_blocks, 2 * rows, 128), F32),
        ],
        scratch_shapes=[
            pltpu.VMEM((3, lane_blocks + 1, rows + 16, 128), F32),
            pltpu.VMEM((2 * rows, 128), F32),
            pltpu.VMEM((2 * rows, 128), F32),
            pltpu.VMEM((3, lane_blocks, rows + 16, 128), F32),
            pltpu.VMEM((owners, 16, 128), F32),
        ],
        name="half", compiler_params=pltpu.CompilerParams(vmem_limit_bytes=12 << 20),
    )(wet_fine, bed_fine, *messages)


def main_call(dims, ds, anchor, wet_fine, bed_fine, half, open_x, slope_x, messages):
    blocks, band, columns, lane_blocks = dims
    owners = blocks * columns
    rows = owners * band
    cols = lane_blocks * 128
    return pl.pallas_call(
        lambda *refs: main_body(dims, ds, *refs),
        in_specs=[HBM] + [VMEM] * (5 + owners),
        out_specs=[VMEM, VMEM],
        out_shape=[
            pltpu.VMEM((1, 3, rows, cols), F32),
            pltpu.VMEM((3, rows // 3, cols // 3), F32),
        ],
        scratch_shapes=[
            pltpu.VMEM((3, lane_blocks + 1, rows + 16, 128), F32),
            pltpu.VMEM((lane_blocks, rows + 16, 128), F32),
            pltpu.VMEM((lane_blocks, rows + 16, 128), F32),
            pltpu.VMEM((3, lane_blocks, rows + 16, 128), F32),
            pltpu.VMEM((owners, 16, 128), F32),
            pltpu.VMEM((3, lane_blocks, rows, 128), F32),
            pltpu.SMEM((2, 2), jnp.int32),
            pltpu.SemaphoreType.DMA,
        ],
        name="main", compiler_params=pltpu.CompilerParams(vmem_limit_bytes=20 << 20),
    )(anchor, wet_fine, bed_fine, half, open_x, slope_x, *messages)


def local_packed(strips, anchor, wet_mask, bathy_index, bed_levels, coarse):
    blocks, band, full_cols = strips.shape[2], strips.shape[4], strips.shape[5]
    columns = lax.axis_size("col")
    owners = blocks * columns
    cols = full_cols // columns
    lane_blocks = cols // 128
    rows = owners * band
    dims = (blocks, band, columns, lane_blocks)
    half_owners = owners // 2

    def rank(d):
        r, c = d // columns, d % columns
        return (d >= half_owners, c * 2 < columns, r, c)

    wanted = sorted(range(1, owners), key=rank)
    opening = [d for d in wanted if d < columns and d * 2 >= columns]
    rest = [d for d in range(half_owners) if d not in opening]
    messages = {}
    after = []
    for ds in (opening, rest, list(range(half_owners, owners))):
        count = len({d // columns for d in ds})
        made = pl.pallas_call(
            lambda *refs, ds=ds, after=len(after): pack_body(dims, ds, after, *refs),
            in_specs=[HBM] * 4 + [VMEM] * len(after),
            out_specs=[VMEM] * len(ds),
            out_shape=[pltpu.VMEM((message_rows(dims, d), 128), F32) for d in ds],
            scratch_shapes=[
                pltpu.VMEM((count, 3, band, full_cols), F32),
                pltpu.VMEM((count, 3, 8, full_cols), F32),
                pltpu.VMEM(wet_mask.shape, jnp.int32),
                pltpu.VMEM(bathy_index.shape, jnp.int32),
                pltpu.SMEM(bed_levels.shape, F32),
                pltpu.SemaphoreType.DMA((2, count)),
                pltpu.SemaphoreType.DMA((3,)),
            ],
            name="pack",
            compiler_params=pltpu.CompilerParams(vmem_limit_bytes=10 << 20),
        )(
            in_hbm(strips),
            in_hbm(wet_mask),
            in_hbm(bathy_index),
            in_hbm(bed_levels),
            *after,
        )
        messages.update(zip(ds, (in_vmem(x) for x in made)))
        after = [messages[ds[0]]]

    arrived = {
        d: lax.ppermute(messages[d], ("row", "col"), [(i, i ^ d) for i in range(owners)])
        for d in wanted
    }
    arrived[0] = messages[0]
    arrived = {d: in_vmem(x) if d else x for d, x in arrived.items()}

    coarse_rows = rows // 3
    coarse_cols = cols // 3
    wet_fine, bed_fine, weights = pl.pallas_call(
        lambda *refs: prep_body(columns, *refs),
        in_specs=[SMEM, SMEM, VMEM, VMEM],
        out_specs=[VMEM] * 3,
        out_shape=[pltpu.VMEM((lane_blocks, rows, 128), F32)] * 2
        + [pltpu.VMEM((5, coarse_rows, coarse_cols), F32)],
        name="prep", compiler_params=pltpu.CompilerParams(vmem_limit_bytes=12 << 20),
    )(bed_levels, anchor, wet_mask, bathy_index)

    early = [0] + wanted[: half_owners - 1]
    order = [0] + wanted
    wet_fine, bed_fine, weights = in_vmem(wet_fine), in_vmem(bed_fine), in_vmem(weights)
    half, open_x, slope_x = half_call(dims, early, wet_fine, bed_fine, [arrived[d] for d in early])
    half, open_x, slope_x = in_vmem(half), in_vmem(open_x), in_vmem(slope_x)
    fine, rolled = main_call(
        dims,
        order,
        in_hbm(anchor),
        wet_fine,
        bed_fine,
        half,
        open_x,
        slope_x,
        [arrived[d] for d in order],
    )
    rolled = in_vmem(rolled)

    lines = lax.axis_size("nest") * lax.axis_size("row")
    rights = [(c, c + 1) for c in range(columns - 1)]
    downs = [(l, l + 1) for l in range(lines - 1)]
    both = [(l * columns + c, l2 * columns + c2) for l, l2 in downs for c, c2 in rights]
    diagonal = lax.ppermute(rolled, ("nest", "row", "col"), both)
    from_left = lax.ppermute(rolled, "col", rights)
    from_up = lax.ppermute(rolled, ("nest", "row"), downs)

    coarse_next = pl.pallas_call(
        finish_body,
        in_specs=[VMEM] * 6,
        out_specs=VMEM,
        out_shape=jax.ShapeDtypeStruct(coarse.shape, F32),
        name="finish", compiler_params=pltpu.CompilerParams(vmem_limit_bytes=4 << 20),
    )(
        in_vmem(coarse),
        weights,
        in_vmem(from_left),
        in_vmem(from_up),
        in_vmem(diagonal),
        rolled,
    )
    return (fine, coarse_next)


def local(strips, anchor, wet_mask, bathy_index, bed_levels, coarse):
    columns = lax.axis_size("col")
    owners = strips.shape[2] * columns
    cols = strips.shape[5] // columns
    band = strips.shape[4]
    fits = (
        owners & (owners - 1) == 0
        and 2 <= owners <= 16
        and strips.shape[2] == lax.axis_size("row")
        and band == 24
        and cols == 384
        and owners * band == 384
        and wet_mask.shape[1:] == (128, 128)
    )
    run = local_packed if fits else local_general
    return run(strips, anchor, wet_mask, bathy_index, bed_levels, coarse)


def solution(mesh):
    return jax.shard_map(
        local,
        mesh=mesh,
        in_specs=(
            P("nest", None, None, ("row", "col"), None, None),
            P(),
            P("nest", "row", "col"),
            P("nest", "row", "col"),
            P(),
            P(None, ("nest", "row"), "col"),
        ),
        out_specs=(P("nest", None, "row", "col"), P(None, ("nest", "row"), "col")),
        check_vma=False,
    )
```
